32 devices in a mesh: dp: 4 (over z), tensor: 8 (over y, x, core).
Axes of the slice: x: 2, y: 2, z: 4, core: 2. Of those that a mesh axis runs over, the one named last changes fastest.
Arguments:
- residual: float32 [4096, 1536], P(('dp', 'tensor')), may hold values from -6 to 6
- cotangent: float32 [4096, 1536], P(('dp', 'tensor')), may hold values from -6 to 6
- segments: int32 [4, 1024], P('dp'), may hold values from 0 to 2, never falling along the last dimension, each value on 1 to 512 neighbouring positions
- norm_gain: float32 [2, 1536], replicated, may hold values from 0.1 to 1.9
- inner_weight: bfloat16 [2, 2, 1536, 3072], P(None, None, None, 'tensor'), may hold values from -0.15625 to 0.15625
- state_weight: bfloat16 [2, 1536, 256], replicated, may hold values from -0.15625 to 0.15625
- step_weight: bfloat16 [2, 1536, 48], P(None, None, 'tensor'), may hold values from -0.15625 to 0.15625
- step_bias: float32 [2, 48], P(None, 'tensor'), may hold values from -6.9 to -2.25
- decay_log: float32 [2, 48], P(None, 'tensor'), may hold values from 0 to 2.77
- skip_gain: float32 [2, 48], P(None, 'tensor'), may hold values from 0.5 to 1.5
- conv_weight: float32 [2, 4, 3072], P(None, None, 'tensor'), may hold values from -3 to 3
- conv_bias: float32 [2, 3072], P(None, 'tensor'), may hold values from -0.5 to 0.5
- state_conv_weight: float32 [2, 4, 256], replicated, may hold values from -3 to 3
- state_conv_bias: float32 [2, 256], replicated, may hold values from -0.5 to 0.5
- gate_gain: float32 [2, 3072], P(None, 'tensor'), may hold values from 0.1 to 1.9
- out_weight: bfloat16 [2, 3072, 1536], P(None, 'tensor'), may hold values from -0.109375 to 0.109375
Outputs:
- block_output: float32 [4096, 1536], P(('dp', 'tensor'))
- input_grad: float32 [4096, 1536], P(('dp', 'tensor'))
- grad_norm_gain: float32 [2, 1536], P(None, ('dp', 'tensor'))
- grad_inner_weight: float32 [2, 2, 1536, 3072], P(None, None, 'dp', 'tensor')
- grad_state_weight: float32 [2, 1536, 256], P(None, ('dp', 'tensor'))
- grad_step_weight: float32 [2, 1536, 48], P(None, 'dp', 'tensor')
- grad_step_bias: float32 [2, 48], P(None, 'tensor')
- grad_decay_log: float32 [2, 48], P(None, 'tensor')
- grad_skip_gain: float32 [2, 48], P(None, 'tensor')
- grad_conv_weight: float32 [2, 4, 3072], P(None, None, 'tensor')
- grad_conv_bias: float32 [2, 3072], P(None, 'tensor')
- grad_state_conv_weight: float32 [2, 4, 256], replicated
- grad_state_conv_bias: float32 [2, 256], replicated
- grad_gate_gain: float32 [2, 3072], P(None, 'tensor')
- grad_out_weight: float32 [2, 3072, 1536], P(None, 'tensor', 'dp')
The draws below stay inside these ranges and needn't reach their ends.
Inputs may be any that keep to these rules, and one draw needn't show every extreme that they name: `segments`: each row numbers its sequences from 0 in order, never falling; a sequence has 1 to 512 tokens, and one sequence of each row has exactly 512.
All inputs are finite; a program needn't handle non-finite values.
Results may differ from the reference program's by a relative error of at most 0.029.
Values may be sent and summed in bfloat16 or wider, within the bound.
A program may use at most 192 MiB of HBM per device.

```python
import math
import jax
import jax.numpy as jnp
import numpy as np
from jax import lax

D = 1536
HEADS = 48
INNER = 3072
NSTATE = 128
CONV = 4
SPAN = 256
MOST = 512
LAYERS = 2
TOK_DEV = 1024
SEQS = 3
GROUPS = 4
TOKENS = 4096


def steps_of(key, extent, cuts, low, top_value):
    level = 1.0
    for axis_at, blocks in cuts:
        draws = jax.random.uniform(jax.random.fold_in(jax.random.fold_in(key, 6), axis_at), (blocks,), jnp.float32, low / len(cuts), top_value / len(cuts))
        level = level * jnp.repeat(jnp.exp(draws), extent[axis_at] // blocks).reshape((-1,) + (1,) * (len(extent) - 1 - axis_at))
    return level


def profile(number_of, total, reach, lean):
    weights = [(1 << 20) // math.isqrt(standing ** lean) + 1 for standing in range(2, number_of + 1)]
    spare, counts = total - reach - (number_of - 1), [1] * (number_of - 1)
    while spare > 0:
        candidates = [i for i in range(number_of - 1) if counts[i] < reach]
        mass, remaining = sum([weights[i] for i in candidates]), spare
        for i in candidates:
            more = min(reach - counts[i], max(1, remaining * weights[i] // mass), spare)
            counts[i] = counts[i] + more
            spare = spare - more
    return np.array([reach] + counts)


def ragged(key, amount, total, most, slope):
    if amount == 2:
        one = jax.random.randint(key, (), max(1, total - most), min(most, total - 1) + 1)
        return jnp.stack([one, total - one])
    sizes = jnp.asarray(profile(amount, total, most, slope), jnp.int32)
    couples = (amount - 1) // 2
    donor, receiver = sizes[1:1 + 2 * couples:2], sizes[2:2 + 2 * couples:2]
    slack = jnp.minimum(donor - 1, most - receiver)
    moved = jax.random.randint(jax.random.fold_in(key, 1), (couples,), 0, 1 << 20) % (slack + 1)
    sizes = sizes.at[1:1 + 2 * couples:2].set(donor - moved).at[2:2 + 2 * couples:2].set(receiver + moved)
    return sizes[jax.random.permutation(jax.random.fold_in(key, 2), amount)]


def bell_draw(stream_key, dims, scale, limit, split=(), kind=jnp.bfloat16):
    values = jax.random.normal(stream_key, dims, jnp.float32) * scale
    if len(split) > 0:
        values = steps_of(stream_key, dims, split, -0.22, 0.18) * values
    return jnp.clip(values, min=-limit, max=limit).astype(kind)


def setup_inputs(seed: int = 0) -> dict:
    key_of = jax.random.split(jax.random.key(seed), 17)
    return {
        "residual": bell_draw(key_of[0], (TOKENS, D), 1.0, 6.0, ((0, 32),), jnp.float32),
        "cotangent": bell_draw(key_of[1], (TOKENS, D), 1.0, 6.0, ((0, 32),), jnp.float32),
        "segments": jax.vmap(lambda own: jnp.searchsorted(jnp.cumsum(ragged(own, SEQS, TOK_DEV, MOST, 2)), jnp.arange(TOK_DEV), side="right"))(jax.random.split(key_of[2], GROUPS)).reshape((GROUPS, TOK_DEV)).astype(jnp.int32),
        "norm_gain": jnp.clip(1.0 + 0.18 * jax.random.normal(key_of[3], (LAYERS, D), jnp.float32), 0.1, 1.9),
        "inner_weight": bell_draw(key_of[4], (LAYERS, 2, D, INNER), D ** -0.5, 0.15625, ((3, 8),)),
        "state_weight": bell_draw(key_of[5], (LAYERS, D, 2 * NSTATE), D ** -0.5, 0.15625),
        "step_weight": bell_draw(key_of[6], (LAYERS, D, HEADS), D ** -0.5, 0.15625, ((2, 8),)),
        "step_bias": jnp.clip(-6.9 + 4.65 * jax.random.uniform(key_of[7], (LAYERS, HEADS), jnp.float32) ** steps_of(key_of[7], (LAYERS, HEADS), ((1, 8),), -0.2, 0.2), -6.9, -2.25),
        "decay_log": jnp.clip(2.77 * jax.random.uniform(key_of[8], (LAYERS, HEADS), jnp.float32) ** steps_of(key_of[8], (LAYERS, HEADS), ((1, 8),), -0.2, 0.2), 0.0, 2.77),
        "skip_gain": jnp.clip(0.5 + 1.0 * jax.random.uniform(key_of[9], (LAYERS, HEADS), jnp.float32) ** steps_of(key_of[9], (LAYERS, HEADS), ((1, 8),), -0.2, 0.2), 0.5, 1.5),
        "conv_weight": bell_draw(key_of[10], (LAYERS, CONV, INNER), CONV ** -0.5, 3.0, ((2, 8),), jnp.float32),
        "conv_bias": jnp.clip(jax.random.uniform(key_of[11], (LAYERS, INNER), jnp.float32, -0.5, 0.5) * steps_of(key_of[11], (LAYERS, INNER), ((1, 8),), -0.4, 0.0), -0.5, 0.5),
        "state_conv_weight": bell_draw(key_of[12], (LAYERS, CONV, 2 * NSTATE), CONV ** -0.5, 3.0, (), jnp.float32),
        "state_conv_bias": jnp.clip(jax.random.uniform(key_of[13], (LAYERS, 2 * NSTATE), jnp.float32, -0.5, 0.5), -0.5, 0.5),
        "gate_gain": jnp.clip(1.0 + 0.18 * jax.random.normal(key_of[14], (LAYERS, INNER), jnp.float32), 0.1, 1.9),
        "out_weight": bell_draw(key_of[15], (LAYERS, INNER, D), INNER ** -0.5, 0.109375, ((1, 8),)),
    }


EPS = 1e-05
HIGH = lax.Precision.HIGHEST

def shifted(array, offset, fill):
    head = jnp.full((offset,) + array.shape[1:], fill, array.dtype)
    return jnp.concatenate([head, array[:-offset]], axis=0)

def causal_conv(values, kernel, bias, segment):
    result = bias[None, :] + kernel[0][None, :] * values
    for offset in range(1, kernel.shape[0]):
        keep = (shifted(segment, offset, -1) == segment).astype(values.dtype)
        result = result + kernel[offset][None, :] * shifted(values, offset, 0.0) * keep[:, None]
    return result

def state_scan(inputs, step_size, rate, in_state, out_state, skip_gain, segment):
    length, heads, width = inputs.shape
    count = length // SPAN
    half_width = in_state.shape[1]
    log_decay = -step_size * rate[None, :]
    cumul = jnp.cumsum(log_decay.reshape(count, SPAN, heads), axis=1)
    cumul_head = jnp.transpose(cumul, (0, 2, 1))
    seg_blocks = segment.reshape(count, SPAN)
    block_in = inputs.reshape(count, SPAN, heads, width)
    weighted = block_in * step_size.reshape(count, SPAN, heads)[..., None]
    in_blocks = in_state.reshape(count, SPAN, half_width)
    out_blocks = out_state.reshape(count, SPAN, half_width)
    causal = jnp.arange(SPAN)[:, None] >= jnp.arange(SPAN)[None, :]
    same = (seg_blocks[:, :, None] == seg_blocks[:, None, :]) & causal[None]
    keep_mask = same.astype(inputs.dtype)[:, None]
    differ = cumul_head[:, :, :, None] - cumul_head[:, :, None, :]
    decay_mat = jnp.exp(jnp.where(same[:, None], differ, 0.0)) * keep_mask
    scores = jnp.einsum('ctn,csn->cts', out_blocks, in_blocks, precision=HIGH)
    intra = jnp.einsum('chts,cshp->cthp', decay_mat * scores[:, None], weighted, precision=HIGH)
    last = cumul_head[:, :, -1]
    tail_keep = (seg_blocks == seg_blocks[:, -1:]).astype(inputs.dtype)
    to_end = jnp.exp(last[:, :, None] - cumul_head) * tail_keep[:, None, :]
    span_states = jnp.einsum('chs,cshp,csn->chpn', to_end, weighted, in_blocks, precision=HIGH)
    prev_seg = jnp.concatenate([jnp.full((1,), -1, segment.dtype), seg_blocks[:-1, -1]])
    carry_keep = (seg_blocks[:, -1] == prev_seg).astype(inputs.dtype)
    carry_decay = jnp.exp(last) * carry_keep[:, None]

    def advance(current, items):
        factor, fresh = items
        return (factor[:, None, None] * current + fresh, current)
    _, entering = lax.scan(advance, jnp.zeros((heads, width, half_width), inputs.dtype), (carry_decay, span_states))
    head_keep = (seg_blocks == prev_seg[:, None]).astype(inputs.dtype)
    from_state = jnp.exp(cumul_head) * head_keep[:, None, :]
    inter = jnp.einsum('chq,cqn,chpn->cqhp', from_state, out_blocks, entering, precision=HIGH)
    result = intra + inter + skip_gain[None, None, :, None] * block_in
    return result.reshape(length, heads * width)

def mixer_core(floats, segment):
    gate_in, value_in, state_in, step_in, conv_weight, conv_bias, state_conv_weight, state_conv_bias, step_bias, decay_log, skip_gain = floats
    heads = step_in.shape[1]
    length = value_in.shape[0]
    values = jax.nn.silu(causal_conv(value_in, conv_weight, conv_bias, segment))
    states = jax.nn.silu(causal_conv(state_in, state_conv_weight, state_conv_bias, segment))
    half_width = states.shape[1] // 2
    step_size = jax.nn.softplus(step_in + step_bias[None, :])
    scanned = state_scan(values.reshape(length, heads, values.shape[1] // heads), step_size, jnp.exp(decay_log), states[:, :half_width], states[:, half_width:], skip_gain, segment)
    return scanned * jax.nn.silu(gate_in)

def contract_rows(left, right):
    return lax.dot_general(left, right, (((0,), (0,)), ((), ())), preferred_element_type=jnp.float32)

def contract_cols(left, right):
    return lax.dot_general(left, right, (((1,), (1,)), ((), ())), preferred_element_type=jnp.float32)

def layer_forward(resid, segment, params):
    norm_gain, inner_weight, state_weight, step_weight, step_bias, decay_log, skip_gain, conv_weight, conv_bias, state_conv_weight, state_conv_bias, gate_gain, out_weight = params
    row_scale = lax.rsqrt(lax.optimization_barrier(jnp.mean(resid * resid, axis=1)) + EPS)
    normed = (resid * row_scale[:, None] * norm_gain[None, :]).astype(jnp.bfloat16)
    gate_in = jnp.dot(normed, inner_weight[0], preferred_element_type=jnp.float32)
    value_in = jnp.dot(normed, inner_weight[1], preferred_element_type=jnp.float32)
    state_in = jnp.dot(normed, state_weight, preferred_element_type=jnp.float32)
    step_in = jnp.dot(normed, step_weight, preferred_element_type=jnp.float32)
    floats = (gate_in, value_in, state_in, step_in, conv_weight, conv_bias, state_conv_weight, state_conv_bias, step_bias, decay_log, skip_gain)
    gated = mixer_core(floats, segment)
    gate_scale = lax.rsqrt(lax.optimization_barrier(jnp.mean(gated * gated, axis=1)) + EPS)
    scaled_in = (gated * gate_gain[None, :]).astype(jnp.bfloat16)
    mixed = gate_scale[:, None] * jnp.dot(scaled_in, out_weight, preferred_element_type=jnp.float32)
    saved = (resid, row_scale, normed, floats, gated, gate_scale, scaled_in, mixed)
    return (resid + mixed, saved)

def layer_backward(saved, grad_out, segment, params):
    norm_gain, inner_weight, state_weight, step_weight, step_bias, decay_log, skip_gain, conv_weight, conv_bias, state_conv_weight, state_conv_bias, gate_gain, out_weight = params
    resid, row_scale, normed, floats, gated, gate_scale, scaled_in, mixed = saved
    sent = (gate_scale[:, None] * grad_out).astype(jnp.bfloat16)
    mean_grad = -0.5 * gate_scale * gate_scale * lax.optimization_barrier(jnp.sum(mixed * grad_out, axis=1))
    grad_out_weight = contract_rows(scaled_in, sent)
    grad_scaled = contract_cols(sent, out_weight)
    grad_gate_gain = lax.optimization_barrier(jnp.sum(grad_scaled * gated, axis=0))
    grad_gated = grad_scaled * gate_gain[None, :] + 2.0 / INNER * mean_grad[:, None] * gated
    pullback = jax.vjp(lambda *items: mixer_core(items, segment), *floats)[1]
    grads = pullback(grad_gated)
    rounded_gate = grads[0].astype(jnp.bfloat16)
    rounded_value = grads[1].astype(jnp.bfloat16)
    rounded_state = grads[2].astype(jnp.bfloat16)
    rounded_step = grads[3].astype(jnp.bfloat16)
    grad_normed = contract_cols(rounded_gate, inner_weight[0]) + contract_cols(rounded_value, inner_weight[1]) + contract_cols(rounded_state, state_weight) + contract_cols(rounded_step, step_weight)
    grad_inner = jnp.stack([contract_rows(normed, rounded_gate), contract_rows(normed, rounded_value)])
    grad_state_weight = contract_rows(normed, rounded_state)
    grad_step_weight = contract_rows(normed, rounded_step)
    weighted = grad_normed * norm_gain[None, :]
    grad_norm_gain = lax.optimization_barrier(jnp.sum(grad_normed * resid * row_scale[:, None], axis=0))
    inner_sum = lax.optimization_barrier(jnp.sum(weighted * resid, axis=1))
    grad_resid = grad_out + row_scale[:, None] * weighted - resid * (row_scale * row_scale * row_scale * inner_sum / D)[:, None]
    layer_grads = (grad_norm_gain, grad_inner, grad_state_weight, grad_step_weight, grads[8], grads[9], grads[10], grads[4], grads[5], grads[6], grads[7], grad_gate_gain, grad_out_weight)
    return (grad_resid, layer_grads)

def reference(residual, cotangent, segments, norm_gain, inner_weight, state_weight, step_weight, step_bias, decay_log, skip_gain, conv_weight, conv_bias, state_conv_weight, state_conv_bias, gate_gain, out_weight):
    weights = (norm_gain, inner_weight, state_weight, step_weight, step_bias, decay_log, skip_gain, conv_weight, conv_bias, state_conv_weight, state_conv_bias, gate_gain, out_weight)

    def one_group(totals, items):
        resid, grad_out, segment = items
        hidden = resid
        saved_all = []
        for layer in range(LAYERS):
            hidden, saved = layer_forward(hidden, segment, tuple((item[layer] for item in weights)))
            saved_all.append(saved)
        grad_hidden = grad_out
        per_layer = [None] * LAYERS
        for layer in range(LAYERS - 1, -1, -1):
            grad_hidden, per_layer[layer] = layer_backward(saved_all[layer], grad_hidden, segment, tuple((item[layer] for item in weights)))
        totals = tuple((total + jnp.stack([per_layer[layer][field] for layer in range(LAYERS)]) for field, total in enumerate(totals)))
        return (totals, (hidden, grad_hidden))
    initial = tuple((jnp.zeros(item.shape, jnp.float32) for item in weights))
    totals, (outputs, grads) = lax.scan(one_group, initial, (residual.reshape(GROUPS, TOK_DEV, D), cotangent.reshape(GROUPS, TOK_DEV, D), segments))
    return (outputs.reshape(TOKENS, D), grads.reshape(TOKENS, D), totals[0], totals[1], totals[2], totals[3], totals[4], totals[5], totals[6], totals[7], totals[8], totals[9], totals[10], totals[11], totals[12])
```

```python
import functools
import jax
import jax.numpy as jnp
from jax import lax
from jax.experimental import pallas as pl
from jax.experimental.pallas import tpu as pltpu

from jax.sharding import PartitionSpec as P

EPS = 1e-05
HIGH = lax.Precision.HIGHEST
F32 = jnp.float32
BF = jnp.bfloat16
VM = 60 * 1024 * 1024


def dot(a, b):
    return lax.dot_general(a, b, (((1,), (0,)), ((), ())), preferred_element_type=F32)


def dot_t(a, b):
    return lax.dot_general(a, b, (((1,), (1,)), ((), ())), preferred_element_type=F32)


def t_dot(a, b):
    return lax.dot_general(a, b, (((0,), (0,)), ((), ())), preferred_element_type=F32)


def exact(a, b):
    return lax.dot_general(
        a, b, (((1,), (0,)), ((), ())), preferred_element_type=F32, precision=HIGH
    )


def sigmoid(x):
    return 1.0 / (1.0 + jnp.exp(-x))


def softplus(x):
    return jnp.maximum(x, 0.0) + jnp.log1p(jnp.exp(-jnp.abs(x)))


def tiles_of(inner, width):
    return [
        (start, min(128, inner - start), start // width, min(128, inner - start) // width)
        for start in range(0, inner, 128)
    ]


def expand(cols, inner, width):
    rows = cols.shape[0]
    parts = []
    for _, wide, first, number in tiles_of(inner, width):
        lane = lax.broadcasted_iota(jnp.int32, (rows, wide), 1)
        value = jnp.broadcast_to(cols[:, first : first + 1], (rows, wide))
        for j in range(1, number):
            value = jnp.where(lane >= j * width, cols[:, first + j : first + j + 1], value)
        parts.append(value)
    return parts[0] if len(parts) == 1 else jnp.concatenate(parts, axis=1)


def head_sum_matrix(inner, heads, width):
    row = lax.broadcasted_iota(jnp.int32, (inner, heads), 0)
    col = lax.broadcasted_iota(jnp.int32, (inner, heads), 1)
    return ((row >= col * width) & (row < (col + 1) * width)).astype(BF)


def head_sum(value, inner, heads, width):
    ones = head_sum_matrix(inner, heads, width)
    high = value.astype(BF)
    low = (value - high.astype(F32)).astype(BF)
    return dot(high, ones) + dot(low, ones)


def head_split(tile, width, number):
    if number == 1:
        return tile
    lane = lax.broadcasted_iota(jnp.int32, tile.shape, 1)
    zero = jnp.zeros_like(tile)
    return jnp.concatenate(
        [
            jnp.where((lane >= j * width) & (lane < (j + 1) * width), tile, zero)
            for j in range(number)
        ],
        axis=0,
    )


def pair_mask(seg_col, seg_row):
    rows, cols = seg_col.shape[0], seg_row.shape[1]
    row = lax.broadcasted_iota(jnp.int32, (rows, cols), 0)
    col = lax.broadcasted_iota(jnp.int32, (rows, cols), 1)
    return (row >= col) & (seg_col == seg_row)


def lower_ones(size):
    row = lax.broadcasted_iota(jnp.int32, (size, size), 0)
    col = lax.broadcasted_iota(jnp.int32, (size, size), 1)
    return (row >= col).astype(F32)


def turned(value):
    return jnp.transpose(value)


def column_of(tile):
    rows = tile.shape[1]
    return jnp.transpose(jnp.broadcast_to(tile[0:1, :], (rows, rows)))[:, 0:1]


def tile_of(column):
    rows = column.shape[0]
    return jnp.transpose(jnp.broadcast_to(column, (rows, rows)))[0:8, :]


def forward_kernel(
    layer, heads, width, inner_all,
    nb_ref, meta_ref, segrow_ref, win_ref, wst_ref, wstep_ref, wout_ref,
    cw_ref, cb_ref, scw_ref, scb_ref, sb_ref, dl_ref, sk_ref, gg_ref,
    g_ref, v_ref, pv_ref, s_ref, ps_ref, d_ref, y_ref, sp_ref, part_ref, psq_ref,
    state, vbuf, sbuf,
):
    size, inner = g_ref.shape
    half = s_ref.shape[1] // 2
    at = slice(layer, layer + 1)

    @pl.when(pl.program_id(0) == 0)
    def _():
        state[...] = jnp.zeros_like(state)
        vbuf[...] = jnp.zeros_like(vbuf)
        sbuf[...] = jnp.zeros_like(sbuf)

    nb = nb_ref[...]
    gate = dot(nb, win_ref[0])
    g_ref[...] = gate
    value = dot(nb, win_ref[1])
    v_ref[...] = value.astype(BF)
    raw = dot(nb, wst_ref[...])
    s_ref[...] = raw.astype(BF)
    step_in = dot(nb, wstep_ref[...])
    d_ref[...] = step_in

    meta = meta_ref[...]

    def conv(buf, now, w_ref, b_row):
        buf[8:, :] = now
        total = b_row + w_ref[0:1, :] * now
        for k in range(1, w_ref.shape[0]):
            total = total + w_ref[k : k + 1, :] * (buf[8 - k : 8 - k + size, :] * meta[:, k : k + 1])
        buf[0:8, :] = now[size - 8 :, :]
        return total

    pre_v = conv(vbuf, value, cw_ref, cb_ref[at, :])
    pv_ref[...] = pre_v
    pre_s = conv(sbuf, raw, scw_ref, scb_ref[at, :])
    ps_ref[...] = pre_s
    x = pre_v * sigmoid(pre_v)
    st = pre_s * sigmoid(pre_s)
    b_mat = st[:, :half].astype(BF)
    c_mat = st[:, half:].astype(BF)
    dt = softplus(step_in + sb_ref[at, :])
    log_decay = -dt * jnp.exp(dl_ref[at, :])
    cum = exact(lower_ones(size), log_decay)
    cum_t = turned(cum)
    last = cum[size - 1 : size, :]
    xt = (x * expand(dt, inner, width)).astype(BF)
    from_state = jnp.exp(cum) * meta[:, 4:5]
    to_end = jnp.exp(last - cum) * meta[:, 5:6]
    carry = jnp.exp(last) * meta[0:1, 6:7]
    before = state[...]
    before_b = before.astype(BF)
    sp_ref[...] = before_b
    scores = dot_t(c_mat, b_mat)
    mask = pair_mask(meta[:, 0:1], segrow_ref[0:1, :])
    parts = []
    for start, wide, first, number in tiles_of(inner, width):
        mats = []
        for h in range(first, first + number):
            differ = cum[:, h : h + 1] - cum_t[h : h + 1, :]
            mats.append((jnp.exp(jnp.where(mask, differ, -1e30)) * scores).astype(BF))
        left = mats[0] if number == 1 else jnp.concatenate(mats, axis=1)
        parts.append(dot(left, head_split(xt[:, start : start + wide], width, number)))
    intra = parts[0] if len(parts) == 1 else jnp.concatenate(parts, axis=1)
    inter = dot(c_mat, before_b) * expand(from_state, inner, width)
    y = intra + inter + expand(sk_ref[at, :], inner, width) * x
    y_ref[...] = y
    ended = (xt.astype(F32) * expand(to_end, inner, width)).astype(BF)
    state[...] = expand(carry, inner, width) * before + t_dot(b_mat, ended)
    gated = y * (gate * sigmoid(gate))
    square = jnp.sum(gated * gated, axis=1, keepdims=True)
    psq_ref[...] = tile_of(square)
    scaled = (gated * gg_ref[at, :]).astype(BF)
    part_ref[...] = dot(scaled, wout_ref[...]).astype(BF)


def layer_block(shape, layer, buffered=True):
    block = (None,) + tuple(shape[1:])
    return pl.BlockSpec(
        block, lambda c: (layer,) + (0,) * (len(shape) - 1), pipeline_mode=pl.Buffered(1)
    )


def whole_block(shape):
    return pl.BlockSpec(tuple(shape), lambda c: (0,) * len(shape), pipeline_mode=pl.Buffered(1))


def forward_compute(layer, size, normed, meta, segrow, w):
    tokens, depth = normed.shape
    inner = w["inner_weight"].shape[3]
    heads = w["step_weight"].shape[2]
    width = inner // heads
    both = w["state_weight"].shape[2]
    half = both // 2
    count = tokens // size
    rows = lambda wide: pl.BlockSpec((size, wide), lambda c: (c, 0))
    kernel = functools.partial(forward_kernel, layer, heads, width, None)
    out = lambda wide, kind: jax.ShapeDtypeStruct((tokens, wide), kind)
    return pl.pallas_call(
        kernel,
        grid=(count,),
        out_shape=(
            out(inner, F32), out(inner, BF), out(inner, F32), out(both, BF), out(both, F32),
            out(heads, F32), out(inner, F32),
            jax.ShapeDtypeStruct((count, half, inner), BF),
            out(depth, BF),
            jax.ShapeDtypeStruct((count * 8, size), F32),
        ),
        in_specs=[
            rows(depth), rows(8), pl.BlockSpec((8, size), lambda c: (0, c)),
            layer_block(w["inner_weight"].shape, layer),
            layer_block(w["state_weight"].shape, layer),
            layer_block(w["step_weight"].shape, layer),
            layer_block(w["out_weight"].shape, layer),
            layer_block(w["conv_weight"].shape, layer),
            whole_block(w["conv_bias"].shape),
            layer_block(w["state_conv_weight"].shape, layer),
            whole_block(w["state_conv_bias"].shape),
            whole_block(w["step_bias"].shape),
            whole_block(w["decay_log"].shape),
            whole_block(w["skip_gain"].shape),
            whole_block(w["gate_gain"].shape),
        ],
        out_specs=(
            rows(inner), rows(inner), rows(inner), rows(both), rows(both), rows(heads), rows(inner),
            pl.BlockSpec((None, half, inner), lambda c: (c, 0, 0)),
            rows(depth),
            pl.BlockSpec((8, size), lambda c: (c, 0)),
        ),
        scratch_shapes=[
            pltpu.VMEM((half, inner), F32),
            pltpu.VMEM((size + 8, inner), F32),
            pltpu.VMEM((size + 8, both), F32),
        ],
        compiler_params=pltpu.CompilerParams(vmem_limit_bytes=VM),
        name="forward_mix",
    )(
        normed, meta, segrow, w["inner_weight"], w["state_weight"], w["step_weight"], w["out_weight"],
        w["conv_weight"], w["conv_bias"], w["state_conv_weight"], w["state_conv_bias"],
        w["step_bias"], w["decay_log"], w["skip_gain"], w["gate_gain"],
    )


def token_meta(segment, size):
    tokens = segment.shape[0]
    seg = segment.astype(F32)

    def back(k):
        return jnp.concatenate([jnp.full((k,), -1.0, F32), seg[:-k]])

    blocks = seg.reshape(-1, size)
    gone = jnp.full((1,), -1.0, F32)
    before = jnp.concatenate([gone, blocks[:-1, -1]])
    after = jnp.concatenate([blocks[1:, 0], gone])
    per = lambda v: jnp.broadcast_to(v[:, None], blocks.shape)
    end = per(blocks[:, -1])
    columns = [
        seg,
        (back(1) == seg).astype(F32),
        (back(2) == seg).astype(F32),
        (back(3) == seg).astype(F32),
        (blocks == per(before)).astype(F32).reshape(-1),
        (blocks == end).astype(F32).reshape(-1),
        (end == per(before)).astype(F32).reshape(-1),
        (blocks == per(after)).astype(F32).reshape(-1),
    ]
    rows = jnp.stack(columns)
    return rows.T, rows


def backward_kernel(
    layer, heads, width, inner_all,
    sent_ref, mean_ref, meta_ref, segrow_ref, g_ref, v_ref, pv_ref, s_ref, ps_ref, d_ref, y_ref, sp_ref,
    win_ref, wst_ref, wstep_ref, wout_ref,
    cw_ref, scw_ref, sb_ref, dl_ref, sk_ref, gg_ref,
    rg_ref, rv_ref, rs_ref, rd_ref, sc_ref, part_ref,
    gcw_ref, gcb_ref, gscw_ref, gscb_ref, ggg_ref, gsk_ref, gsb_ref, gdl_ref,
    state, vbuf, sbuf,
):
    size, inner = g_ref.shape
    half = s_ref.shape[1] // 2
    at = slice(layer, layer + 1)

    @pl.when(pl.program_id(0) == 0)
    def _():
        for ref in (state, vbuf, sbuf, gcw_ref, gcb_ref, gscw_ref, gscb_ref, ggg_ref, gsk_ref, gsb_ref, gdl_ref):
            ref[...] = jnp.zeros_like(ref)

    meta = meta_ref[...]
    sent = sent_ref[...]
    gate, y = g_ref[...], y_ref[...]
    gate_sig = sigmoid(gate)
    silu_gate = gate * gate_sig
    gated = y * silu_gate
    gain = gg_ref[at, :]
    sc_ref[...] = (gated * gain).astype(BF)
    grad_scaled = dot_t(sent, wout_ref[...])
    ggg_ref[...] += jnp.sum(grad_scaled * gated, axis=0, keepdims=True)
    grad_gated = grad_scaled * gain + (2.0 / inner_all) * column_of(mean_ref[...]) * gated
    rg = (grad_gated * y * (gate_sig * (1.0 + gate * (1.0 - gate_sig)))).astype(BF)
    rg_ref[...] = rg
    dy = grad_gated * silu_gate
    pre_v, pre_s = pv_ref[...], ps_ref[...]
    sig_v, sig_s = sigmoid(pre_v), sigmoid(pre_s)
    x = pre_v * sig_v
    st = pre_s * sig_s
    b_mat = st[:, :half].astype(BF)
    c_mat = st[:, half:].astype(BF)
    raw_step = d_ref[...] + sb_ref[at, :]
    dt = softplus(raw_step)
    rate = jnp.exp(dl_ref[at, :])
    log_decay = -dt * rate
    cum = exact(lower_ones(size), log_decay)
    cum_t = turned(cum)
    last = cum[size - 1 : size, :]
    dt_all = expand(dt, inner, width)
    skip_all = expand(sk_ref[at, :], inner, width)
    xt = (x * dt_all).astype(BF)
    dy_b = dy.astype(BF)
    from_state = expand(jnp.exp(cum) * meta[:, 4:5], inner, width)
    to_end = expand(jnp.exp(last - cum) * meta[:, 5:6], inner, width)
    carry = expand(jnp.exp(last) * meta[0:1, 6:7], inner, width)
    gsk_ref[...] += jnp.sum(dy * x, axis=0, keepdims=True)
    scores = dot_t(c_mat, b_mat)
    mask = pair_mask(meta[:, 0:1], segrow_ref[0:1, :])
    d_scores = jnp.zeros((size, size), F32)
    parts = []
    for start, wide, first, number in tiles_of(inner, width):
        dy_split = head_split(dy_b[:, start : start + wide], width, number)
        d_mats = dot_t(dy_split, xt[:, start : start + wide])
        mats = []
        for j in range(number):
            h = first + j
            differ = cum[:, h : h + 1] - cum_t[h : h + 1, :]
            decay = jnp.exp(jnp.where(mask, differ, -1e30))
            mats.append((decay * scores).astype(BF))
            d_scores = d_scores + d_mats[j * size : (j + 1) * size, :] * decay
        left = mats[0] if number == 1 else jnp.concatenate(mats, axis=0)
        parts.append(t_dot(left, dy_split))
    intra = parts[0] if len(parts) == 1 else jnp.concatenate(parts, axis=1)
    d_scores = d_scores.astype(BF)
    before = sp_ref[...]
    after = state[...]
    after_b = after.astype(BF)
    dy_in = (dy * from_state).astype(BF)
    ended = (xt.astype(F32) * to_end).astype(BF)
    from_later = dot(b_mat, after_b) * to_end
    d_xt = intra + from_later
    d_c = dot(d_scores, b_mat) + dot_t(dy_in, before)
    d_b = t_dot(d_scores, c_mat) + dot_t(ended, after_b)
    across = carry * jnp.sum(before.astype(F32) * after, axis=0, keepdims=True)
    state[...] = carry * after + t_dot(c_mat, dy_in)
    xt_f = xt.astype(F32)
    sums = head_sum(
        jnp.concatenate(
            [
                dy_b.astype(F32) * (y - skip_all * x) - xt_f * intra,
                xt_f * from_later,
                x * d_xt,
                jnp.broadcast_to(across, (8, inner)),
            ],
            axis=0,
        ),
        inner, heads, width,
    )
    seg_col, seg_row = meta[:, 0:1], segrow_ref[0:1, :]
    d_log = (
        exact(later_ones(seg_col, seg_row), sums[0:size])
        + exact(earlier_ones(seg_col, seg_row), sums[size : 2 * size])
        + sums[3 * size : 3 * size + 1]
    )
    d_step = sums[2 * size : 3 * size] - rate * d_log
    gdl_ref[...] += jnp.sum(d_log * log_decay, axis=0, keepdims=True)
    d_raw = d_step * sigmoid(raw_step)
    gsb_ref[...] += jnp.sum(d_raw, axis=0, keepdims=True)
    rd = d_raw.astype(BF)
    rd_ref[...] = rd
    d_x = dy * skip_all + d_xt * dt_all
    d_pre_v = d_x * (sig_v * (1.0 + pre_v * (1.0 - sig_v)))
    d_st = jnp.concatenate([d_b, d_c], axis=1)
    d_pre_s = d_st * (sig_s * (1.0 + pre_s * (1.0 - sig_s)))

    def conv(buf, now, w_ref, value, gw_ref, gb_ref):
        taps = w_ref.shape[0]
        gb_ref[...] += jnp.sum(now, axis=0, keepdims=True)
        total = w_ref[0:1, :] * now
        gw_ref[0:1, :] += jnp.sum(now * value, axis=0, keepdims=True)
        for k in range(1, taps):
            kept = now * meta[:, k : k + 1]
            buf[k - 1, 0:size, :] = kept
            moved = buf[k - 1, k : k + size, :]
            buf[k - 1, size : size + 8, :] = kept[0:8, :]
            total = total + w_ref[k : k + 1, :] * moved
            gw_ref[k : k + 1, :] += jnp.sum(moved * value, axis=0, keepdims=True)
        return total

    rv = conv(vbuf, d_pre_v, cw_ref, v_ref[...].astype(F32), gcw_ref, gcb_ref).astype(BF)
    rv_ref[...] = rv
    rs = conv(sbuf, d_pre_s, scw_ref, s_ref[...].astype(F32), gscw_ref, gscb_ref).astype(BF)
    rs_ref[...] = rs
    total = dot_t(rg, win_ref[0]) + dot_t(rv, win_ref[1]) + dot_t(rs, wst_ref[...]) + dot_t(rd, wstep_ref[...])
    part_ref[...] = total.astype(BF)


def later_ones(seg_col, seg_row):
    rows, cols = seg_col.shape[0], seg_row.shape[1]
    row = lax.broadcasted_iota(jnp.int32, (rows, cols), 0)
    col = lax.broadcasted_iota(jnp.int32, (rows, cols), 1)
    return ((row <= col) & (seg_col == seg_row)).astype(F32)


def earlier_ones(seg_col, seg_row):
    rows, cols = seg_col.shape[0], seg_row.shape[1]
    row = lax.broadcasted_iota(jnp.int32, (rows, cols), 0)
    col = lax.broadcasted_iota(jnp.int32, (rows, cols), 1)
    return ((row > col) & (seg_col == seg_row)).astype(F32)


def backward_compute(layer, size, inner_all, sent, mean, meta, segrow, saved, w):
    g, v, pv, s, ps, d, y, sp = saved
    tokens, depth = sent.shape
    inner = w["inner_weight"].shape[3]
    heads = w["step_weight"].shape[2]
    width = inner // heads
    both = w["state_weight"].shape[2]
    half = both // 2
    taps = w["conv_weight"].shape[1]
    count = tokens // size
    rows = lambda wide: pl.BlockSpec((size, wide), lambda c: (count - 1 - c, 0))
    kernel = functools.partial(backward_kernel, layer, heads, width, inner_all)
    out = lambda wide, kind: jax.ShapeDtypeStruct((tokens, wide), kind)
    small = [(taps, inner), (1, inner), (taps, both), (1, both), (1, inner), (1, inner), (1, heads), (1, heads)]
    return pl.pallas_call(
        kernel,
        grid=(count,),
        out_shape=(
            out(inner, BF), out(inner, BF), out(both, BF), out(heads, BF), out(inner, BF), out(depth, BF),
            *[jax.ShapeDtypeStruct(shape, F32) for shape in small],
        ),
        in_specs=[
            rows(depth), pl.BlockSpec((8, size), lambda c: (count - 1 - c, 0)), rows(8),
            pl.BlockSpec((8, size), lambda c: (0, count - 1 - c)),
            rows(inner), rows(inner), rows(inner), rows(both), rows(both), rows(heads), rows(inner),
            pl.BlockSpec((None, half, inner), lambda c: (count - 1 - c, 0, 0)),
            layer_block(w["inner_weight"].shape, layer),
            layer_block(w["state_weight"].shape, layer),
            layer_block(w["step_weight"].shape, layer),
            layer_block(w["out_weight"].shape, layer),
            layer_block(w["conv_weight"].shape, layer),
            layer_block(w["state_conv_weight"].shape, layer),
            whole_block(w["step_bias"].shape),
            whole_block(w["decay_log"].shape),
            whole_block(w["skip_gain"].shape),
            whole_block(w["gate_gain"].shape),
        ],
        out_specs=(
            rows(inner), rows(inner), rows(both), rows(heads), rows(inner), rows(depth),
            *[pl.BlockSpec(shape, lambda c: (0, 0)) for shape in small],
        ),
        scratch_shapes=[
            pltpu.VMEM((half, inner), F32),
            pltpu.VMEM((taps - 1, size + 8, inner), F32),
            pltpu.VMEM((taps - 1, size + 8, both), F32),
        ],
        compiler_params=pltpu.CompilerParams(vmem_limit_bytes=VM),
        name="backward_mix",
    )(
        sent, mean, meta, segrow, g, v, pv, s, ps, d, y, sp,
        w["inner_weight"], w["state_weight"], w["step_weight"], w["out_weight"],
        w["conv_weight"], w["state_conv_weight"],
        w["step_bias"], w["decay_log"], w["skip_gain"], w["gate_gain"],
    )


def weight_kernel(normed_ref, sent_ref, sc_ref, rg_ref, rv_ref, rs_ref, rd_ref, gin_ref, gst_ref, gsd_ref, gout_ref):
    nb = normed_ref[...]
    gin_ref[0] = t_dot(nb, rg_ref[...]).astype(BF)
    gin_ref[1] = t_dot(nb, rv_ref[...]).astype(BF)
    gst_ref[...] = t_dot(nb, rs_ref[...]).astype(BF)
    gsd_ref[...] = t_dot(nb, rd_ref[...]).astype(BF)
    gout_ref[...] = t_dot(sc_ref[...], sent_ref[...]).astype(BF)


def weight_compute(normed, sent, sc, rg, rv, rs, rd):
    tokens, depth = normed.shape
    inner, both, heads = rg.shape[1], rs.shape[1], rd.shape[1]
    step = 256
    whole = lambda wide: pl.BlockSpec((tokens, wide), lambda i: (0, 0), pipeline_mode=pl.Buffered(1))
    cols = pl.BlockSpec((tokens, step), lambda i: (0, i))
    return pl.pallas_call(
        weight_kernel,
        grid=(depth // step,),
        out_shape=(
            jax.ShapeDtypeStruct((2, depth, inner), BF),
            jax.ShapeDtypeStruct((depth, both), BF),
            jax.ShapeDtypeStruct((depth, heads), BF),
            jax.ShapeDtypeStruct((inner, depth), BF),
        ),
        in_specs=[cols, cols, whole(inner), whole(inner), whole(inner), whole(both), whole(heads)],
        out_specs=(
            pl.BlockSpec((2, step, inner), lambda i: (0, i, 0)),
            pl.BlockSpec((step, both), lambda i: (i, 0)),
            pl.BlockSpec((step, heads), lambda i: (i, 0)),
            pl.BlockSpec((inner, step), lambda i: (0, i)),
        ),
        compiler_params=pltpu.CompilerParams(vmem_limit_bytes=VM),
        name="weight_grads",
    )(normed, sent, sc, rg, rv, rs, rd)


AXIS = "tensor"


def span_of(dims):
    found = [0]
    for d in dims:
        found = found + [r ^ d for r in found]
    return found


class Exchange:
    def __init__(self, size):
        self.size = size
        links = [1 << b for b in range(1, size.bit_length() - 1)]
        self.links = links
        self.orders = [links, links[::-1]]
        self.offsets = sorted(span_of(links), key=lambda r: -bin(r).count("1"))

    def reduce_steps(self, q):
        order = self.orders[q]
        steps = []
        for i, d in enumerate(order):
            for s in sorted(span_of(order[i + 1 :]), key=lambda r: -bin(r).count("1")):
                steps.append((i, d ^ s))
        return steps + [(len(order), 0)]

    def gather_dims(self, q):
        return self.orders[q] + [1]

    def gather_last(self, q, r):
        dims = self.gather_dims(q)
        return max([i for i, d in enumerate(dims) if r & d], default=-1)

    def gather_steps(self, q):
        dims = self.gather_dims(q)
        found = [r for r in range(1, self.size)]
        return sorted(found, key=lambda r: (self.gather_last(q, r), r & (r - 1) != 0))


def remote(src, dst, send, recv, target):
    return pltpu.make_async_remote_copy(
        src_ref=src, dst_ref=dst, send_sem=send, recv_sem=recv,
        device_id={AXIS: target}, device_id_type=pl.DeviceIdType.MESH,
    )


def greet(targets):
    barrier = pltpu.get_barrier_semaphore()
    for target in targets:
        pl.semaphore_signal(barrier, inc=1, device_id={AXIS: target}, device_id_type=pl.DeviceIdType.MESH)
    pl.semaphore_wait(barrier, len(targets))


def block_rows(block, rows, half, q):
    return pl.ds(pl.multiple_of(block * rows + q * half, half), half)


def comm_kernel(ex, rows, spec, middle, *refs):
    refs = list(refs)
    take = lambda k: [refs.pop(0) for _ in range(k)]
    part_ref = take(1)[0] if spec["reduce"] else None
    psq_ref = take(1)[0] if spec["squares"] else None
    ins = take(spec["n_in"])
    out_ref = take(1)[0] if spec["gather"] else None
    mean_out = take(1)[0] if spec["means"] else None
    outs = take(spec["n_out"])
    me = lax.axis_index(AXIS)
    n = ex.size
    half = rows // 2
    peers = [me ^ r for r in range(1, n)]
    partners = peers if (spec["squares"] or spec["means"]) else [me ^ d for d in ex.links + [1]]
    greet(partners)
    pending = []

    total = None
    if spec["reduce"]:
        own, pair, stage, got = take(4)
        load_sem, pair_send, pair_recv, link_send, link_recv = take(5)
        if spec["squares"]:
            sq_buf, sq_send, sq_recv = take(3)
        slot_of = {r: i for i, r in enumerate(ex.offsets)}
        loads = {}
        for r in ex.offsets:
            i = slot_of[r]
            loads[r] = pltpu.make_async_copy(
                part_ref.at[pl.ds(pl.multiple_of((me ^ r) * rows, rows), rows), :], own.at[i], load_sem.at[i]
            )
            loads[r].start()
        pairs = {}
        for r in ex.offsets:
            i = slot_of[r]
            pairs[r] = remote(
                part_ref.at[pl.ds(pl.multiple_of((me ^ r ^ 1) * rows, rows), rows), :], pair.at[i],
                pair_send.at[i], pair_recv.at[i], me ^ 1,
            )
            pairs[r].start()
        squares = []
        if spec["squares"]:
            for r in range(1, n):
                copy = remote(
                    psq_ref.at[pl.ds(pl.multiple_of((me ^ r) * 8, 8), 8), :], sq_buf.at[r],
                    sq_send.at[r], sq_recv.at[r], me ^ r,
                )
                copy.start()
                squares.append(copy)
        ready = set()
        index = {}
        for q in range(2):
            for i, r in ex.reduce_steps(q):
                for j in range(i):
                    index[(q, j, r)] = len(index)
        arrivals = {}
        steps = [ex.reduce_steps(q) for q in range(2)]
        final = [None, None]
        for k in range(len(steps[0])):
            for q in range(2):
                i, r = steps[q][k]
                if r not in ready:
                    loads[r].wait()
                    pairs[r].wait_recv()
                    ready.add(r)
                piece = pl.ds(q * half, half)
                value = own[slot_of[r], piece, :].astype(F32) + pair[slot_of[r], piece, :].astype(F32)
                for j in range(i):
                    arrivals[(q, j, r)].wait_recv()
                    value = value + got[index[(q, j, r)]].astype(F32)
                if r == 0:
                    final[q] = value
                    continue
                d = ex.orders[q][i]
                s = q * (n // 2) + slot_of[r]
                stage[s] = value.astype(BF)
                at = index[(q, i, r ^ d)]
                copy = remote(stage.at[s], got.at[at], link_send.at[s], link_recv.at[at], me ^ d)
                copy.start()
                arrivals[(q, i, r ^ d)] = copy
                pending.append(copy)
        total = jnp.concatenate(final, axis=0)
        pending.extend(pairs.values())
        square = None
        if spec["squares"]:
            square = psq_ref[pl.ds(pl.multiple_of(me * 8, 8), 8), :]
            for r, copy in enumerate(squares, 1):
                copy.wait_recv()
                square = square + sq_buf[r]
            pending.extend(squares)
    result = middle(total, column_of(square) if spec["squares"] else None, ins, outs)
    if spec["gather"]:
        row_buf, own_sem, send_sem, recv_sem = take(4)
        sent_rows, mean = result
        row_buf[...] = sent_rows
        copies = {}

        def forward(q, r):
            dims = ex.gather_dims(q)
            block = me ^ r
            place = block_rows(block, rows, half, q)
            src = row_buf.at[pl.ds(q * half, half), :] if r == 0 else out_ref.at[place, :]
            return [
                (i, remote(src, out_ref.at[place, :], send_sem.at[q, r ^ dims[i]], recv_sem.at[q, r ^ dims[i]], me ^ dims[i]), r ^ dims[i])
                for i in range(ex.gather_last(q, r) + 1, len(dims))
            ]

        first = [forward(q, 0) for q in range(2)]
        for i in range(len(first[0])):
            for q in range(2):
                _, copy, r = first[q][i]
                copy.start()
                copies[(q, r)] = copy
        local = pltpu.make_async_copy(
            row_buf, out_ref.at[pl.ds(pl.multiple_of(me * rows, rows), rows), :], own_sem
        )
        local.start()
        mean_copies = []
        if spec["means"]:
            mean_buf, mean_send, mean_recv = take(3)
            tile = tile_of(mean)
            mean_buf[...] = tile
            mine = pl.ds(pl.multiple_of(me * 8, 8), 8)
            for r in range(1, n):
                copy = remote(mean_buf, mean_out.at[mine, :], mean_send.at[r], mean_recv.at[r], me ^ r)
                copy.start()
                mean_copies.append(copy)
            mean_out[mine, :] = tile
        steps = [ex.gather_steps(q) for q in range(2)]
        for k in range(len(steps[0])):
            for q in range(2):
                r = steps[q][k]
                copies[(q, r)].wait_recv()
                for _, copy, beyond in forward(q, r):
                    copy.start()
                    copies[(q, beyond)] = copy
        for copy in mean_copies:
            copy.wait()
        local.wait()
        for copy in copies.values():
            copy.wait_send()
    for copy in pending:
        copy.wait_send()


def comm_call(name, collective, ex, middle, part=None, psq=None, ins=(), outs=(), gather=None, means=False):
    n = ex.size
    spec = dict(reduce=part is not None, squares=psq is not None, gather=gather is not None, means=means, n_in=len(ins), n_out=len(outs))
    vm = pl.BlockSpec(memory_space=pltpu.VMEM)
    anywhere = pl.BlockSpec(memory_space=pl.ANY)
    operands, in_specs, out_shape, out_specs, scratch = [], [], [], [], []
    if part is not None:
        rows, depth = part.shape[0] // n, part.shape[1]
        operands.append(part)
        in_specs.append(anywhere)
    else:
        rows, depth = ins[0].shape
    if psq is not None:
        operands.append(psq)
        in_specs.append(vm)
    operands.extend(ins)
    in_specs.extend([vm] * len(ins))
    half = rows // 2
    dma = pltpu.SemaphoreType.DMA
    if part is not None:
        slots = n // 2
        scratch += [
            pltpu.VMEM((slots, rows, depth), BF), pltpu.VMEM((slots, rows, depth), BF),
            pltpu.VMEM((2 * slots, half, depth), BF), pltpu.VMEM((2 * (slots - 1), half, depth), BF),
            dma((slots,)), dma((slots,)), dma((slots,)), dma((2 * slots,)), dma((2 * (slots - 1),)),
        ]
        if psq is not None:
            scratch += [pltpu.VMEM((n, 8, rows), F32), dma((n,)), dma((n,))]
    if gather is not None:
        out_shape.append(jax.ShapeDtypeStruct((n * rows, gather), BF))
        out_specs.append(anywhere)
        if means:
            out_shape.append(jax.ShapeDtypeStruct((n * 8, rows), F32))
            out_specs.append(vm)
        scratch += [pltpu.VMEM((rows, gather), BF), dma, dma((2, n)), dma((2, n))]
        if means:
            scratch += [pltpu.VMEM((8, rows), F32), dma((n,)), dma((n,))]
    out_shape.extend(outs)
    out_specs.extend([vm] * len(outs))
    return pl.pallas_call(
        functools.partial(comm_kernel, ex, rows, spec, middle),
        out_shape=tuple(out_shape),
        in_specs=in_specs,
        out_specs=tuple(out_specs),
        scratch_shapes=scratch,
        compiler_params=pltpu.CompilerParams(collective_id=collective, has_side_effects=True, vmem_limit_bytes=VM),
        name=name,
    )(*operands)


LAYERS = 2
SIZE = 128
NAMES = (
    "norm_gain", "inner_weight", "state_weight", "step_weight", "step_bias", "decay_log", "skip_gain",
    "conv_weight", "conv_bias", "state_conv_weight", "state_conv_bias", "gate_gain", "out_weight",
)


def shape_of(rows, depth):
    return jax.ShapeDtypeStruct((rows, depth), F32)


def row_scale_of(resid):
    return lax.rsqrt(jnp.mean(resid * resid, axis=1, keepdims=True) + EPS)


def retile(tiles, count):
    width = tiles.shape[1]
    if tiles.shape[0] == count * 8:
        return tiles
    flat = tiles.reshape(-1, 8, width)[:, 0, :].reshape(count, 1, -1)
    return jnp.broadcast_to(flat, (count, 8, flat.shape[2])).reshape(count * 8, -1)


def gate_of(square, inner_all):
    return lax.rsqrt(square / inner_all + EPS)


def start_middle(layer, total, square, ins, outs):
    resid, gain = ins[0][...], ins[1][layer : layer + 1, :]
    return (resid * row_scale_of(resid) * gain).astype(BF), None


def between_middle(layer, inner_all, total, square, ins, outs):
    gate = gate_of(square, inner_all)
    mixed = gate * total
    hidden = ins[0][...] + mixed
    outs[0][...] = hidden
    outs[1][...] = mixed
    outs[2][...] = gate
    return (hidden * row_scale_of(hidden) * ins[1][layer : layer + 1, :]).astype(BF), None


def turn_middle(inner_all, total, square, ins, outs):
    gate = gate_of(square, inner_all)
    mixed = gate * total
    grad = ins[1][...]
    outs[0][...] = ins[0][...] + mixed
    mean = -0.5 * gate * gate * jnp.sum(mixed * grad, axis=1, keepdims=True)
    return (gate * grad).astype(BF), mean


def norm_backward(layer, total, resid, grad, gain):
    scale = row_scale_of(resid)
    weighted = total * gain
    inner = jnp.sum(weighted * resid, axis=1, keepdims=True)
    gain_grad = jnp.sum(total * resid * scale, axis=0, keepdims=True)
    fresh = grad + scale * weighted - resid * (scale * scale * scale * inner / resid.shape[1])
    return fresh, gain_grad


def back_middle(layer, total, square, ins, outs):
    fresh, gain_grad = norm_backward(layer, total, ins[0][...], ins[1][...], ins[2][layer : layer + 1, :])
    outs[0][...] = fresh
    outs[1][...] = gain_grad
    mixed, gate = ins[3][...], ins[4][...]
    mean = -0.5 * gate * gate * jnp.sum(mixed * fresh, axis=1, keepdims=True)
    return (gate * fresh).astype(BF), mean


def end_middle(layer, total, square, ins, outs):
    fresh, gain_grad = norm_backward(layer, total, ins[0][...], ins[1][...], ins[2][layer : layer + 1, :])
    outs[0][...] = fresh
    outs[1][...] = gain_grad
    return None


def shards(ex, residual, cotangent, segments, *weights):
    w = dict(zip(NAMES, weights))
    rows, depth = residual.shape
    tokens = segments.shape[1]
    inner = w["inner_weight"].shape[3]
    heads = w["step_weight"].shape[2]
    inner_all = inner * ex.size
    count = tokens // SIZE
    gain = w["norm_gain"]
    meta, segrow = token_meta(segments[0], SIZE)
    ids = iter(range(100))
    resids, mixeds, gates, normeds, saved = [residual], [], [], [], []
    (normed,) = comm_call(
        "rows_start", next(ids), ex, functools.partial(start_middle, 0), ins=(residual, gain), gather=depth
    )
    hidden = residual
    for layer in range(LAYERS):
        normeds.append(normed)
        made = forward_compute(layer, SIZE, normed, meta, segrow, w)
        saved.append(made[:8])
        part, squares = made[8:]
        squares = retile(squares, ex.size)
        if layer + 1 < LAYERS:
            normed, hidden, mixed, gate = comm_call(
                "rows_between", next(ids), ex, functools.partial(between_middle, layer + 1, inner_all),
                part=part, psq=squares, ins=(hidden, gain),
                outs=(shape_of(rows, depth), shape_of(rows, depth), shape_of(rows, 1)), gather=depth,
            )
            resids.append(hidden)
            mixeds.append(mixed)
            gates.append(gate)
        else:
            sent, mean, block_output = comm_call(
                "rows_turn", next(ids), ex, functools.partial(turn_middle, inner_all),
                part=part, psq=squares, ins=(hidden, cotangent), outs=(shape_of(rows, depth),), gather=depth, means=True,
            )
    grad = cotangent
    big, small = [None] * LAYERS, [None] * LAYERS
    for layer in range(LAYERS - 1, -1, -1):
        made = backward_compute(layer, SIZE, inner_all, sent, retile(mean, count), meta, segrow, saved[layer], w)
        rg, rv, rs, rd, sc, part = made[:6]
        g_inner, g_state, g_step, g_out = weight_compute(normeds[layer], sent, sc, rg, rv, rs, rd)
        scatter = lambda v, dim: lax.psum_scatter(v, "dp", scatter_dimension=dim, tiled=True).astype(F32)
        big[layer] = (
            scatter(g_inner, 1),
            lax.psum_scatter(g_state, ("dp", "tensor"), scatter_dimension=0, tiled=True).astype(F32),
            scatter(g_step, 0),
            scatter(g_out, 1),
        )
        if layer:
            sent, mean, grad, g_gain = comm_call(
                "rows_back", next(ids), ex, functools.partial(back_middle, layer), part=part,
                ins=(resids[layer], grad, gain, mixeds[layer - 1], gates[layer - 1]),
                outs=(shape_of(rows, depth), shape_of(1, depth)), gather=depth, means=True,
            )
        else:
            grad, g_gain = comm_call(
                "rows_end", next(ids), ex, functools.partial(end_middle, layer), part=part,
                ins=(resids[layer], grad, gain), outs=(shape_of(rows, depth), shape_of(1, depth)),
            )
        small[layer] = (made[6:], g_gain)
    per_dp = lax.psum(
        jnp.stack([jnp.concatenate([m[0], m[1], m[4], m[5]], axis=0) for m, _ in small]), "dp"
    )
    per_head = lax.psum(jnp.stack([jnp.concatenate([m[6], m[7]], axis=0) for m, _ in small]), "dp")
    everywhere = lax.psum(jnp.stack([jnp.concatenate([m[2], m[3]], axis=0) for m, _ in small]), ("dp", "tensor"))
    g_norm = lax.psum_scatter(
        jnp.concatenate([g for _, g in small], axis=0), ("dp", "tensor"), scatter_dimension=1, tiled=True
    )
    taps = w["conv_weight"].shape[1]
    stack = lambda k: jnp.stack([big[layer][k] for layer in range(LAYERS)])
    return (
        block_output,
        grad,
        g_norm,
        stack(0),
        stack(1),
        stack(2),
        per_head[:, 0],
        per_head[:, 1],
        per_dp[:, taps + 2].reshape(LAYERS, heads, -1).sum(2),
        per_dp[:, :taps],
        per_dp[:, taps],
        everywhere[:, :taps],
        everywhere[:, taps],
        per_dp[:, taps + 1],
        stack(3),
    )


def solution(mesh):
    ex = Exchange(mesh.shape["tensor"])
    return jax.shard_map(
        functools.partial(shards, ex),
        mesh=mesh,
        in_specs=(
            P(("dp", "tensor"), None),
            P(("dp", "tensor"), None),
            P("dp", None),
            P(),
            P(None, None, None, "tensor"),
            P(),
            P(None, None, "tensor"),
            P(None, "tensor"),
            P(None, "tensor"),
            P(None, "tensor"),
            P(None, None, "tensor"),
            P(None, "tensor"),
            P(),
            P(),
            P(None, "tensor"),
            P(None, "tensor", None),
        ),
        out_specs=(
            P(("dp", "tensor"), None),
            P(("dp", "tensor"), None),
            P(None, ("dp", "tensor")),
            P(None, None, "dp", "tensor"),
            P(None, ("dp", "tensor"), None),
            P(None, "dp", "tensor"),
            P(None, "tensor"),
            P(None, "tensor"),
            P(None, "tensor"),
            P(None, None, "tensor"),
            P(None, "tensor"),
            P(),
            P(),
            P(None, "tensor"),
            P(None, "tensor", "dp"),
        ),
        check_vma=False,
    )
```

```python
import functools
from typing import Any, NamedTuple
import jax
import jax.numpy as jnp
from jax import lax
from jax.experimental import pallas as pl
from jax.experimental.pallas import tpu as pltpu

from jax.sharding import PartitionSpec as P

EPS = 1e-05
HIGH = lax.Precision.HIGHEST
F32 = jnp.float32
BF = jnp.bfloat16
VM = 60 * 1024 * 1024


def cost_of(flops, moved=1 << 24):
    return pl.CostEstimate(flops=flops, bytes_accessed=moved, transcendentals=0)


class Weights(NamedTuple):
    norm_gain: jax.Array
    inner_weight: jax.Array
    state_weight: jax.Array
    step_weight: jax.Array
    step_bias: jax.Array
    decay_log: jax.Array
    skip_gain: jax.Array
    conv_weight: jax.Array
    conv_bias: jax.Array
    state_conv_weight: jax.Array
    state_conv_bias: jax.Array
    gate_gain: jax.Array
    out_weight: jax.Array


def dot(a, b):
    return lax.dot_general(a, b, (((1,), (0,)), ((), ())), preferred_element_type=F32)


def dot_t(a, b):
    return lax.dot_general(a, b, (((1,), (1,)), ((), ())), preferred_element_type=F32)


def t_dot(a, b):
    return lax.dot_general(a, b, (((0,), (0,)), ((), ())), preferred_element_type=F32)


def exact(a, b):
    return lax.dot_general(
        a, b, (((1,), (0,)), ((), ())), preferred_element_type=F32, precision=HIGH
    )


def sigmoid(x):
    return 1.0 / (1.0 + jnp.exp(-x))


def softplus(x):
    return jnp.maximum(x, 0.0) + jnp.log1p(jnp.exp(-jnp.abs(x)))


def tiles_of(inner, width):
    return [
        (start, min(128, inner - start), start // width, min(128, inner - start) // width)
        for start in range(0, inner, 128)
    ]


def expand(cols, inner, width):
    rows = cols.shape[0]
    parts = []
    for _, wide, first, number in tiles_of(inner, width):
        lane = lax.broadcasted_iota(jnp.int32, (rows, wide), 1)
        value = jnp.broadcast_to(cols[:, first : first + 1], (rows, wide))
        for j in range(1, number):
            value = jnp.where(lane >= j * width, cols[:, first + j : first + j + 1], value)
        parts.append(value)
    return parts[0] if len(parts) == 1 else jnp.concatenate(parts, axis=1)


def head_sum_matrix(inner, heads, width):
    row = lax.broadcasted_iota(jnp.int32, (inner, heads), 0)
    col = lax.broadcasted_iota(jnp.int32, (inner, heads), 1)
    return ((row >= col * width) & (row < (col + 1) * width)).astype(BF)


def head_sum(value, inner, heads, width):
    ones = head_sum_matrix(inner, heads, width)
    high = value.astype(BF)
    low = (value - high.astype(F32)).astype(BF)
    return dot(high, ones) + dot(low, ones)


def head_split(tile, width, number):
    if number == 1:
        return tile
    lane = lax.broadcasted_iota(jnp.int32, tile.shape, 1)
    zero = jnp.zeros_like(tile)
    return jnp.concatenate(
        [
            jnp.where((lane >= j * width) & (lane < (j + 1) * width), tile, zero)
            for j in range(number)
        ],
        axis=0,
    )


def pair_mask(seg_col, seg_row):
    rows, cols = seg_col.shape[0], seg_row.shape[1]
    row = lax.broadcasted_iota(jnp.int32, (rows, cols), 0)
    col = lax.broadcasted_iota(jnp.int32, (rows, cols), 1)
    return (row >= col) & (seg_col == seg_row)


def lower_ones(size):
    row = lax.broadcasted_iota(jnp.int32, (size, size), 0)
    col = lax.broadcasted_iota(jnp.int32, (size, size), 1)
    return (row >= col).astype(F32)


def turned(value):
    return jnp.transpose(value)


def column_of(tile):
    rows = tile.shape[1]
    return jnp.transpose(jnp.broadcast_to(tile[0:1, :], (rows, rows)))[:, 0:1]


def tile_of(column):
    rows = column.shape[0]
    return jnp.transpose(jnp.broadcast_to(column, (rows, rows)))[0:8, :]


def forward_kernel(
    layer, heads, width, inner_all,
    nb_ref, meta_ref, segrow_ref, win_ref, wst_ref, wstep_ref, wout_ref,
    cw_ref, cb_ref, scw_ref, scb_ref, sb_ref, dl_ref, sk_ref, gg_ref,
    g_ref, v_ref, pv_ref, s_ref, ps_ref, d_ref, y_ref, sp_ref, part_ref, psq_ref,
    state, vbuf, sbuf,
):
    size, inner = g_ref.shape
    half = s_ref.shape[1] // 2
    at = slice(layer, layer + 1)

    @pl.when(pl.program_id(0) == 0)
    def _():
        state[...] = jnp.zeros_like(state)
        vbuf[...] = jnp.zeros_like(vbuf)
        sbuf[...] = jnp.zeros_like(sbuf)

    nb = nb_ref[...]
    gate = dot(nb, win_ref[0])
    g_ref[...] = gate
    value = dot(nb, win_ref[1])
    v_ref[...] = value.astype(BF)
    raw = dot(nb, wst_ref[...])
    s_ref[...] = raw.astype(BF)
    step_in = dot(nb, wstep_ref[...])
    d_ref[...] = step_in

    meta = meta_ref[...]

    def conv(buf, now, w_ref, b_row):
        buf[8:, :] = now
        total = b_row + w_ref[0:1, :] * now
        for k in range(1, w_ref.shape[0]):
            total = total + w_ref[k : k + 1, :] * (buf[8 - k : 8 - k + size, :] * meta[:, k : k + 1])
        buf[0:8, :] = now[size - 8 :, :]
        return total

    pre_v = conv(vbuf, value, cw_ref, cb_ref[at, :])
    pv_ref[...] = pre_v
    pre_s = conv(sbuf, raw, scw_ref, scb_ref[at, :])
    ps_ref[...] = pre_s
    x = pre_v * sigmoid(pre_v)
    st = pre_s * sigmoid(pre_s)
    b_mat = st[:, :half].astype(BF)
    c_mat = st[:, half:].astype(BF)
    dt = softplus(step_in + sb_ref[at, :])
    log_decay = -dt * jnp.exp(dl_ref[at, :])
    cum = exact(lower_ones(size), log_decay)
    cum_t = turned(cum)
    last = cum[size - 1 : size, :]
    xt = (x * expand(dt, inner, width)).astype(BF)
    from_state = jnp.exp(cum) * meta[:, 4:5]
    to_end = jnp.exp(last - cum) * meta[:, 5:6]
    carry = jnp.exp(last) * meta[0:1, 6:7]
    before = state[...]
    before_b = before.astype(BF)
    sp_ref[...] = before_b
    scores = dot_t(c_mat, b_mat)
    mask = pair_mask(meta[:, 0:1], segrow_ref[0:1, :])
    parts = []
    for start, wide, first, number in tiles_of(inner, width):
        mats = []
        for h in range(first, first + number):
            differ = cum[:, h : h + 1] - cum_t[h : h + 1, :]
            mats.append((jnp.exp(jnp.where(mask, differ, -1e30)) * scores).astype(BF))
        left = mats[0] if number == 1 else jnp.concatenate(mats, axis=1)
        parts.append(dot(left, head_split(xt[:, start : start + wide], width, number)))
    intra = parts[0] if len(parts) == 1 else jnp.concatenate(parts, axis=1)
    inter = dot(c_mat, before_b) * expand(from_state, inner, width)
    y = intra + inter + expand(sk_ref[at, :], inner, width) * x
    y_ref[...] = y
    ended = (xt.astype(F32) * expand(to_end, inner, width)).astype(BF)
    state[...] = expand(carry, inner, width) * before + t_dot(b_mat, ended)
    gated = y * (gate * sigmoid(gate))
    square = jnp.sum(gated * gated, axis=1, keepdims=True)
    psq_ref[...] = tile_of(square)
    scaled = (gated * gg_ref[at, :]).astype(BF)
    part_ref[...] = dot(scaled, wout_ref[...]).astype(BF)


def layer_block(shape, layer, buffered=True):
    block = (None,) + tuple(shape[1:])
    return pl.BlockSpec(
        block, lambda c: (layer,) + (0,) * (len(shape) - 1), pipeline_mode=pl.Buffered(1)
    )


def whole_block(shape):
    return pl.BlockSpec(tuple(shape), lambda c: (0,) * len(shape), pipeline_mode=pl.Buffered(1))


def forward_compute(layer, size, normed, meta, segrow, w):
    tokens, depth = normed.shape
    inner = w.inner_weight.shape[3]
    heads = w.step_weight.shape[2]
    width = inner // heads
    both = w.state_weight.shape[2]
    half = both // 2
    count = tokens // size
    rows = lambda wide: pl.BlockSpec((size, wide), lambda c: (c, 0))
    kernel = functools.partial(forward_kernel, layer, heads, width, None)
    out = lambda wide, kind: jax.ShapeDtypeStruct((tokens, wide), kind)
    return pl.pallas_call(
        kernel,
        grid=(count,),
        out_shape=(
            out(inner, F32), out(inner, BF), out(inner, F32), out(both, BF), out(both, F32),
            out(heads, F32), out(inner, F32),
            jax.ShapeDtypeStruct((count, half, inner), BF),
            out(depth, BF),
            jax.ShapeDtypeStruct((count * 8, size), F32),
        ),
        in_specs=[
            rows(depth), rows(8), pl.BlockSpec((8, size), lambda c: (0, c)),
            layer_block(w.inner_weight.shape, layer),
            layer_block(w.state_weight.shape, layer),
            layer_block(w.step_weight.shape, layer),
            layer_block(w.out_weight.shape, layer),
            layer_block(w.conv_weight.shape, layer),
            whole_block(w.conv_bias.shape),
            layer_block(w.state_conv_weight.shape, layer),
            whole_block(w.state_conv_bias.shape),
            whole_block(w.step_bias.shape),
            whole_block(w.decay_log.shape),
            whole_block(w.skip_gain.shape),
            whole_block(w.gate_gain.shape),
        ],
        out_specs=(
            rows(inner), rows(inner), rows(inner), rows(both), rows(both), rows(heads), rows(inner),
            pl.BlockSpec((None, half, inner), lambda c: (c, 0, 0)),
            rows(depth),
            pl.BlockSpec((8, size), lambda c: (c, 0)),
        ),
        scratch_shapes=[
            pltpu.VMEM((half, inner), F32),
            pltpu.VMEM((size + 8, inner), F32),
            pltpu.VMEM((size + 8, both), F32),
        ],
        compiler_params=pltpu.CompilerParams(vmem_limit_bytes=VM),
        cost_estimate=cost_of(10 * tokens * depth * inner),
        name="forward",
    )(
        normed, meta, segrow, w.inner_weight, w.state_weight, w.step_weight, w.out_weight,
        w.conv_weight, w.conv_bias, w.state_conv_weight, w.state_conv_bias,
        w.step_bias, w.decay_log, w.skip_gain, w.gate_gain,
    )


def token_meta(segment, size):
    tokens = segment.shape[0]
    seg = segment.astype(F32)

    def back(k):
        return jnp.concatenate([jnp.full((k,), -1.0, F32), seg[:-k]])

    blocks = seg.reshape(-1, size)
    gone = jnp.full((1,), -1.0, F32)
    before = jnp.concatenate([gone, blocks[:-1, -1]])
    after = jnp.concatenate([blocks[1:, 0], gone])
    per = lambda v: jnp.broadcast_to(v[:, None], blocks.shape)
    end = per(blocks[:, -1])
    columns = [
        seg,
        (back(1) == seg).astype(F32),
        (back(2) == seg).astype(F32),
        (back(3) == seg).astype(F32),
        (blocks == per(before)).astype(F32).reshape(-1),
        (blocks == end).astype(F32).reshape(-1),
        (end == per(before)).astype(F32).reshape(-1),
        (blocks == per(after)).astype(F32).reshape(-1),
    ]
    rows = jnp.stack(columns)
    return rows.T, rows


def backward_kernel(
    layer, heads, width, inner_all,
    sent_ref, mean_ref, meta_ref, segrow_ref, g_ref, v_ref, pv_ref, s_ref, ps_ref, d_ref, y_ref, sp_ref,
    win_ref, wst_ref, wstep_ref, wout_ref,
    cw_ref, scw_ref, sb_ref, dl_ref, sk_ref, gg_ref,
    rg_ref, rv_ref, rs_ref, rd_ref, sc_ref, part_ref,
    gcw_ref, gcb_ref, gscw_ref, gscb_ref, ggg_ref, gsk_ref, gsb_ref, gdl_ref,
    state, vbuf, sbuf,
):
    size, inner = g_ref.shape
    half = s_ref.shape[1] // 2
    at = slice(layer, layer + 1)

    @pl.when(pl.program_id(0) == 0)
    def _():
        for ref in (state, vbuf, sbuf, gcw_ref, gcb_ref, gscw_ref, gscb_ref, ggg_ref, gsk_ref, gsb_ref, gdl_ref):
            ref[...] = jnp.zeros_like(ref)

    meta = meta_ref[...]
    sent = sent_ref[...]
    gate, y = g_ref[...], y_ref[...]
    gate_sig = sigmoid(gate)
    silu_gate = gate * gate_sig
    gated = y * silu_gate
    gain = gg_ref[at, :]
    sc_ref[...] = (gated * gain).astype(BF)
    grad_scaled = dot_t(sent, wout_ref[...])
    ggg_ref[...] += jnp.sum(grad_scaled * gated, axis=0, keepdims=True)
    grad_gated = grad_scaled * gain + (2.0 / inner_all) * column_of(mean_ref[...]) * gated
    rg = (grad_gated * y * (gate_sig * (1.0 + gate * (1.0 - gate_sig)))).astype(BF)
    rg_ref[...] = rg
    dy = grad_gated * silu_gate
    pre_v, pre_s = pv_ref[...], ps_ref[...]
    sig_v, sig_s = sigmoid(pre_v), sigmoid(pre_s)
    x = pre_v * sig_v
    st = pre_s * sig_s
    b_mat = st[:, :half].astype(BF)
    c_mat = st[:, half:].astype(BF)
    raw_step = d_ref[...] + sb_ref[at, :]
    dt = softplus(raw_step)
    rate = jnp.exp(dl_ref[at, :])
    log_decay = -dt * rate
    cum = exact(lower_ones(size), log_decay)
    cum_t = turned(cum)
    last = cum[size - 1 : size, :]
    dt_all = expand(dt, inner, width)
    skip_all = expand(sk_ref[at, :], inner, width)
    xt = (x * dt_all).astype(BF)
    dy_b = dy.astype(BF)
    from_state = expand(jnp.exp(cum) * meta[:, 4:5], inner, width)
    to_end = expand(jnp.exp(last - cum) * meta[:, 5:6], inner, width)
    carry = expand(jnp.exp(last) * meta[0:1, 6:7], inner, width)
    gsk_ref[...] += jnp.sum(dy * x, axis=0, keepdims=True)
    scores = dot_t(c_mat, b_mat)
    mask = pair_mask(meta[:, 0:1], segrow_ref[0:1, :])
    d_scores = jnp.zeros((size, size), F32)
    parts = []
    for start, wide, first, number in tiles_of(inner, width):
        dy_split = head_split(dy_b[:, start : start + wide], width, number)
        d_mats = dot_t(dy_split, xt[:, start : start + wide])
        mats = []
        for j in range(number):
            h = first + j
            differ = cum[:, h : h + 1] - cum_t[h : h + 1, :]
            decay = jnp.exp(jnp.where(mask, differ, -1e30))
            mats.append((decay * scores).astype(BF))
            d_scores = d_scores + d_mats[j * size : (j + 1) * size, :] * decay
        left = mats[0] if number == 1 else jnp.concatenate(mats, axis=0)
        parts.append(t_dot(left, dy_split))
    intra = parts[0] if len(parts) == 1 else jnp.concatenate(parts, axis=1)
    d_scores = d_scores.astype(BF)
    before = sp_ref[...]
    after = state[...]
    after_b = after.astype(BF)
    dy_in = (dy * from_state).astype(BF)
    ended = (xt.astype(F32) * to_end).astype(BF)
    from_later = dot(b_mat, after_b) * to_end
    d_xt = intra + from_later
    d_c = dot(d_scores, b_mat) + dot_t(dy_in, before)
    d_b = t_dot(d_scores, c_mat) + dot_t(ended, after_b)
    across = carry * jnp.sum(before.astype(F32) * after, axis=0, keepdims=True)
    state[...] = carry * after + t_dot(c_mat, dy_in)
    xt_f = xt.astype(F32)
    sums = head_sum(
        jnp.concatenate(
            [
                dy_b.astype(F32) * (y - skip_all * x) - xt_f * intra,
                xt_f * from_later,
                x * d_xt,
                jnp.broadcast_to(across, (8, inner)),
            ],
            axis=0,
        ),
        inner, heads, width,
    )
    seg_col, seg_row = meta[:, 0:1], segrow_ref[0:1, :]
    d_log = (
        exact(later_ones(seg_col, seg_row), sums[0:size])
        + exact(earlier_ones(seg_col, seg_row), sums[size : 2 * size])
        + sums[3 * size : 3 * size + 1]
    )
    d_step = sums[2 * size : 3 * size] - rate * d_log
    gdl_ref[...] += jnp.sum(d_log * log_decay, axis=0, keepdims=True)
    d_raw = d_step * sigmoid(raw_step)
    gsb_ref[...] += jnp.sum(d_raw, axis=0, keepdims=True)
    rd = d_raw.astype(BF)
    rd_ref[...] = rd
    d_x = dy * skip_all + d_xt * dt_all
    d_pre_v = d_x * (sig_v * (1.0 + pre_v * (1.0 - sig_v)))
    d_st = jnp.concatenate([d_b, d_c], axis=1)
    d_pre_s = d_st * (sig_s * (1.0 + pre_s * (1.0 - sig_s)))

    def conv(buf, now, w_ref, value, gw_ref, gb_ref):
        taps = w_ref.shape[0]
        gb_ref[...] += jnp.sum(now, axis=0, keepdims=True)
        total = w_ref[0:1, :] * now
        gw_ref[0:1, :] += jnp.sum(now * value, axis=0, keepdims=True)
        for k in range(1, taps):
            kept = now * meta[:, k : k + 1]
            buf[k - 1, 0:size, :] = kept
            moved = buf[k - 1, k : k + size, :]
            buf[k - 1, size : size + 8, :] = kept[0:8, :]
            total = total + w_ref[k : k + 1, :] * moved
            gw_ref[k : k + 1, :] += jnp.sum(moved * value, axis=0, keepdims=True)
        return total

    rv = conv(vbuf, d_pre_v, cw_ref, v_ref[...].astype(F32), gcw_ref, gcb_ref).astype(BF)
    rv_ref[...] = rv
    rs = conv(sbuf, d_pre_s, scw_ref, s_ref[...].astype(F32), gscw_ref, gscb_ref).astype(BF)
    rs_ref[...] = rs
    total = dot_t(rg, win_ref[0]) + dot_t(rv, win_ref[1]) + dot_t(rs, wst_ref[...]) + dot_t(rd, wstep_ref[...])
    part_ref[...] = total.astype(BF)


def later_ones(seg_col, seg_row):
    rows, cols = seg_col.shape[0], seg_row.shape[1]
    row = lax.broadcasted_iota(jnp.int32, (rows, cols), 0)
    col = lax.broadcasted_iota(jnp.int32, (rows, cols), 1)
    return ((row <= col) & (seg_col == seg_row)).astype(F32)


def earlier_ones(seg_col, seg_row):
    rows, cols = seg_col.shape[0], seg_row.shape[1]
    row = lax.broadcasted_iota(jnp.int32, (rows, cols), 0)
    col = lax.broadcasted_iota(jnp.int32, (rows, cols), 1)
    return ((row > col) & (seg_col == seg_row)).astype(F32)


def backward_compute(layer, size, inner_all, sent, mean, meta, segrow, saved, w):
    g, v, pv, s, ps, d, y, sp = saved
    tokens, depth = sent.shape
    inner = w.inner_weight.shape[3]
    heads = w.step_weight.shape[2]
    width = inner // heads
    both = w.state_weight.shape[2]
    half = both // 2
    taps = w.conv_weight.shape[1]
    count = tokens // size
    rows = lambda wide: pl.BlockSpec((size, wide), lambda c: (count - 1 - c, 0))
    kernel = functools.partial(backward_kernel, layer, heads, width, inner_all)
    out = lambda wide, kind: jax.ShapeDtypeStruct((tokens, wide), kind)
    small = [(taps, inner), (1, inner), (taps, both), (1, both), (1, inner), (1, inner), (1, heads), (1, heads)]
    return pl.pallas_call(
        kernel,
        grid=(count,),
        out_shape=(
            out(inner, BF), out(inner, BF), out(both, BF), out(heads, BF), out(inner, BF), out(depth, BF),
            *[jax.ShapeDtypeStruct(shape, F32) for shape in small],
        ),
        in_specs=[
            rows(depth), pl.BlockSpec((8, size), lambda c: (count - 1 - c, 0)), rows(8),
            pl.BlockSpec((8, size), lambda c: (0, count - 1 - c)),
            rows(inner), rows(inner), rows(inner), rows(both), rows(both), rows(heads), rows(inner),
            pl.BlockSpec((None, half, inner), lambda c: (count - 1 - c, 0, 0)),
            layer_block(w.inner_weight.shape, layer),
            layer_block(w.state_weight.shape, layer),
            layer_block(w.step_weight.shape, layer),
            layer_block(w.out_weight.shape, layer),
            layer_block(w.conv_weight.shape, layer),
            layer_block(w.state_conv_weight.shape, layer),
            whole_block(w.step_bias.shape),
            whole_block(w.decay_log.shape),
            whole_block(w.skip_gain.shape),
            whole_block(w.gate_gain.shape),
        ],
        out_specs=(
            rows(inner), rows(inner), rows(both), rows(heads), rows(inner), rows(depth),
            *[pl.BlockSpec(shape, lambda c: (0, 0)) for shape in small],
        ),
        scratch_shapes=[
            pltpu.VMEM((half, inner), F32),
            pltpu.VMEM((taps - 1, size + 8, inner), F32),
            pltpu.VMEM((taps - 1, size + 8, both), F32),
        ],
        compiler_params=pltpu.CompilerParams(vmem_limit_bytes=VM),
        cost_estimate=cost_of(20 * tokens * depth * inner),
        name="backward",
    )(
        sent, mean, meta, segrow, g, v, pv, s, ps, d, y, sp,
        w.inner_weight, w.state_weight, w.step_weight, w.out_weight,
        w.conv_weight, w.state_conv_weight,
        w.step_bias, w.decay_log, w.skip_gain, w.gate_gain,
    )


def weight_kernel(steps, normed_ref, sent_ref, sc_ref, rg_ref, rv_ref, rs_ref, rd_ref, gin_ref, gst_ref, gsd_ref, gout_ref):
    cols = normed_ref.shape[1] // steps
    for i in range(steps):
        here = slice(i * cols, (i + 1) * cols)
        nb = normed_ref[:, here]
        turned_nb = jnp.transpose(nb)
        gin_ref[i, 0] = dot(turned_nb, rg_ref[...]).astype(BF)
        gin_ref[i, 1] = dot(turned_nb, rv_ref[...]).astype(BF)
        gst_ref[here, :] = dot(turned_nb, rs_ref[...]).astype(BF)
        gsd_ref[:, here] = t_dot(rd_ref[...], nb)
        gout_ref[i] = t_dot(sc_ref[...], sent_ref[:, here]).astype(BF)


def weight_compute(across, normed, sent, sc, rg, rv, rs, rd):
    tokens, depth = normed.shape
    inner, both, heads = rg.shape[1], rs.shape[1], rd.shape[1]
    share = depth // across
    steps = 1 if share % 128 == 0 else across
    wide = share * steps
    whole = lambda wide: pl.BlockSpec((tokens, wide), lambda i: (0, 0), pipeline_mode=pl.Buffered(1))
    cols = pl.BlockSpec((tokens, wide), lambda i: (0, i))
    return pl.pallas_call(
        functools.partial(weight_kernel, steps),
        grid=(depth // wide,),
        out_shape=(
            jax.ShapeDtypeStruct((across, 2, share, inner), BF),
            jax.ShapeDtypeStruct((depth, both), BF),
            jax.ShapeDtypeStruct((heads, depth), F32),
            jax.ShapeDtypeStruct((across, inner, share), BF),
        ),
        in_specs=[cols, cols, whole(inner), whole(inner), whole(inner), whole(both), whole(heads)],
        out_specs=(
            pl.BlockSpec((steps, 2, share, inner), lambda i: (i, 0, 0, 0)),
            pl.BlockSpec((wide, both), lambda i: (i, 0)),
            pl.BlockSpec((heads, wide), lambda i: (0, i)),
            pl.BlockSpec((steps, inner, share), lambda i: (i, 0, 0)),
        ),
        compiler_params=pltpu.CompilerParams(vmem_limit_bytes=VM),
        cost_estimate=cost_of(2 * tokens * depth * (3 * inner + both)),
        name="weights",
    )(normed, sent, sc, rg, rv, rs, rd)


AXIS = "tensor"
DATA = "dp"


def span_of(dims):
    found = [0]
    for d in dims:
        found = found + [r ^ d for r in found]
    return found


class Exchange:
    def __init__(self, size):
        self.size = size
        links = [1 << b for b in range(1, size.bit_length() - 1)]
        self.links = links
        self.orders = [links, links[::-1]]
        self.offsets = sorted(span_of(links), key=lambda r: -bin(r).count("1"))

    def reduce_steps(self, q):
        order = self.orders[q]
        steps = []
        for i, d in enumerate(order):
            for s in sorted(span_of(order[i + 1 :]), key=lambda r: -bin(r).count("1")):
                steps.append((i, d ^ s))
        return steps + [(len(order), 0)]

    def gather_dims(self, q):
        return self.orders[q] + [1]

    def gather_last(self, q, r):
        dims = self.gather_dims(q)
        return max([i for i, d in enumerate(dims) if r & d], default=-1)

    def gather_steps(self, q):
        dims = self.gather_dims(q)
        found = [r for r in range(1, self.size)]
        return sorted(found, key=lambda r: (self.gather_last(q, r), r & (r - 1) != 0))


def remote(src, dst, send, recv, target, axis=AXIS):
    return pltpu.make_async_remote_copy(
        src_ref=src, dst_ref=dst, send_sem=send, recv_sem=recv,
        device_id={axis: target}, device_id_type=pl.DeviceIdType.MESH,
    )


def greet(targets, across=()):
    barrier = pltpu.get_barrier_semaphore()
    for axis, group in ((AXIS, targets), (DATA, across)):
        for target in group:
            pl.semaphore_signal(barrier, inc=1, device_id={axis: target}, device_id_type=pl.DeviceIdType.MESH)
    pl.semaphore_wait(barrier, len(targets) + len(across))


def block_rows(block, rows, half, q):
    return pl.ds(pl.multiple_of(block * rows + q * half, half), half)


class Spec(NamedTuple):
    reduce: bool
    squares: bool
    gather: bool
    means: bool
    n_in: int
    n_out: int


def reduce_scratch(ex, rows, depth):
    slots, half = ex.size // 2, rows // 2
    dma = pltpu.SemaphoreType.DMA
    return [
        pltpu.VMEM((slots, rows, depth), BF), pltpu.VMEM((slots, rows, depth), BF),
        pltpu.VMEM((2 * slots, half, depth), BF), pltpu.VMEM((2 * (slots - 1), half, depth), BF),
        dma((slots,)), dma((slots,)), dma((slots,)), dma((2 * slots,)), dma((2 * (slots - 1),)),
    ]


def reduce_start(ex, part_ref, rows, bufs):
    own, pair, _, _, load_sem, pair_send, pair_recv, _, _ = bufs
    me = lax.axis_index(AXIS)
    block = lambda b: part_ref.at[pl.ds(pl.multiple_of(b * rows, rows), rows), :]
    loads, pairs = {}, {}
    for i, r in enumerate(ex.offsets):
        loads[r] = pltpu.make_async_copy(block(me ^ r), own.at[i], load_sem.at[i])
        loads[r].start()
    for i, r in enumerate(ex.offsets):
        pairs[r] = remote(block(me ^ r ^ 1), pair.at[i], pair_send.at[i], pair_recv.at[i], me ^ 1)
        pairs[r].start()
    return loads, pairs


def reduce_finish(ex, rows, bufs, loads, pairs, pending):
    own, pair, stage, got, _, _, _, link_send, link_recv = bufs
    me = lax.axis_index(AXIS)
    n, half = ex.size, rows // 2
    slot_of = {r: i for i, r in enumerate(ex.offsets)}
    steps = [ex.reduce_steps(q) for q in range(2)]
    index = {}
    for q in range(2):
        for i, r in steps[q]:
            for j in range(i):
                index[(q, j, r)] = len(index)
    ready, arrivals, final = set(), {}, [None, None]
    for k in range(len(steps[0])):
        for q in range(2):
            i, r = steps[q][k]
            if r not in ready:
                loads[r].wait()
                pairs[r].wait_recv()
                ready.add(r)
            piece = pl.ds(q * half, half)
            value = own[slot_of[r], piece, :].astype(F32) + pair[slot_of[r], piece, :].astype(F32)
            for j in range(i):
                arrivals[(q, j, r)].wait_recv()
                value = value + got[index[(q, j, r)]].astype(F32)
            if r == 0:
                final[q] = value
                continue
            d = ex.orders[q][i]
            s = q * (n // 2) + slot_of[r]
            stage[s] = value.astype(BF)
            at = index[(q, i, r ^ d)]
            copy = remote(stage.at[s], got.at[at], link_send.at[s], link_recv.at[at], me ^ d)
            copy.start()
            arrivals[(q, i, r ^ d)] = copy
            pending.append(copy)
    pending.extend(pairs.values())
    return jnp.concatenate(final, axis=0)


def comm_kernel(ex, rows, spec, middle, *refs):
    refs = list(refs)
    take = lambda k: [refs.pop(0) for _ in range(k)]
    part_ref = take(1)[0] if spec.reduce else None
    psq_ref = take(1)[0] if spec.squares else None
    ins = take(spec.n_in)
    out_ref = take(1)[0] if spec.gather else None
    mean_out = take(1)[0] if spec.means else None
    outs = take(spec.n_out)
    me = lax.axis_index(AXIS)
    n = ex.size
    half = rows // 2
    peers = [me ^ r for r in range(1, n)]
    partners = peers if (spec.squares or spec.means) else [me ^ d for d in ex.links + [1]]
    greet(partners)
    pending = []

    total = None
    square = None
    if spec.reduce:
        bufs = take(9)
        loads, pairs = reduce_start(ex, part_ref, rows, bufs)
        squares = []
        if spec.squares:
            sq_buf, sq_send, sq_recv = take(3)
            for r in range(1, n):
                copy = remote(
                    psq_ref.at[pl.ds(pl.multiple_of((me ^ r) * 8, 8), 8), :], sq_buf.at[r],
                    sq_send.at[r], sq_recv.at[r], me ^ r,
                )
                copy.start()
                squares.append(copy)
        total = reduce_finish(ex, rows, bufs, loads, pairs, pending)
        if spec.squares:
            square = psq_ref[pl.ds(pl.multiple_of(me * 8, 8), 8), :]
            for r, copy in enumerate(squares, 1):
                copy.wait_recv()
                square = square + sq_buf[r]
            square = column_of(square)
            pending.extend(squares)
    result = middle(total, square, ins, outs)
    if spec.gather:
        row_buf, own_sem, send_sem, recv_sem = take(4)
        sent_rows, mean = result
        row_buf[...] = sent_rows
        copies = {}

        def forward(q, r):
            dims = ex.gather_dims(q)
            block = me ^ r
            place = block_rows(block, rows, half, q)
            src = row_buf.at[pl.ds(q * half, half), :] if r == 0 else out_ref.at[place, :]
            return [
                (i, remote(src, out_ref.at[place, :], send_sem.at[q, r ^ dims[i]], recv_sem.at[q, r ^ dims[i]], me ^ dims[i]), r ^ dims[i])
                for i in range(ex.gather_last(q, r) + 1, len(dims))
            ]

        first = [forward(q, 0) for q in range(2)]
        for i in range(len(first[0])):
            for q in range(2):
                _, copy, r = first[q][i]
                copy.start()
                copies[(q, r)] = copy
        local = pltpu.make_async_copy(
            row_buf, out_ref.at[pl.ds(pl.multiple_of(me * rows, rows), rows), :], own_sem
        )
        local.start()
        mean_copies = []
        if spec.means:
            mean_buf, mean_send, mean_recv = take(3)
            tile = tile_of(mean)
            mean_buf[...] = tile
            mine = pl.ds(pl.multiple_of(me * 8, 8), 8)
            for r in range(1, n):
                copy = remote(mean_buf, mean_out.at[mine, :], mean_send.at[r], mean_recv.at[r], me ^ r)
                copy.start()
                mean_copies.append(copy)
            mean_out[mine, :] = tile
        steps = [ex.gather_steps(q) for q in range(2)]
        for k in range(len(steps[0])):
            for q in range(2):
                r = steps[q][k]
                copies[(q, r)].wait_recv()
                for _, copy, beyond in forward(q, r):
                    copy.start()
                    copies[(q, beyond)] = copy
        for copy in mean_copies:
            copy.wait()
        local.wait()
        for copy in copies.values():
            copy.wait_send()
    for copy in pending:
        copy.wait_send()


def comm_call(name, collective, ex, middle, part=None, psq=None, ins=(), outs=(), gather=None, means=False):
    n = ex.size
    spec = Spec(part is not None, psq is not None, gather is not None, means, len(ins), len(outs))
    vm = pl.BlockSpec(memory_space=pltpu.VMEM)
    anywhere = pl.BlockSpec(memory_space=pl.ANY)
    operands, in_specs, out_shape, out_specs, scratch = [], [], [], [], []
    if part is not None:
        rows, depth = part.shape[0] // n, part.shape[1]
        operands.append(part)
        in_specs.append(anywhere)
    else:
        rows, depth = ins[0].shape
    if psq is not None:
        operands.append(psq)
        in_specs.append(vm)
    operands.extend(ins)
    in_specs.extend([vm] * len(ins))
    half = rows // 2
    dma = pltpu.SemaphoreType.DMA
    if part is not None:
        scratch += reduce_scratch(ex, rows, depth)
        if psq is not None:
            scratch += [pltpu.VMEM((n, 8, rows), F32), dma((n,)), dma((n,))]
    if gather is not None:
        out_shape.append(jax.ShapeDtypeStruct((n * rows, gather), BF))
        out_specs.append(anywhere)
        if means:
            out_shape.append(jax.ShapeDtypeStruct((n * 8, rows), F32))
            out_specs.append(vm)
        scratch += [pltpu.VMEM((rows, gather), BF), dma, dma((2, n)), dma((2, n))]
        if means:
            scratch += [pltpu.VMEM((8, rows), F32), dma((n,)), dma((n,))]
    out_shape.extend(outs)
    out_specs.extend([vm] * len(outs))
    return pl.pallas_call(
        functools.partial(comm_kernel, ex, rows, spec, middle),
        out_shape=tuple(out_shape),
        in_specs=in_specs,
        out_specs=tuple(out_specs),
        scratch_shapes=scratch,
        compiler_params=pltpu.CompilerParams(collective_id=collective, has_side_effects=True, vmem_limit_bytes=VM),
        cost_estimate=cost_of(1 << 33),
        name=name,
    )(*operands)


def sums_kernel(ex, across, state_ref, small_ref, wide_ref, state_out, small_out, wide_out, *refs):
    refs = list(refs)
    take = lambda k: [refs.pop(0) for _ in range(k)]
    bufs = take(9)
    small_buf, wide_buf, mid_buf, all_buf, cell_buf, cell_got = take(6)
    small_send, small_recv, wide_send, wide_recv, all_send, all_recv, cell_send, cell_recv = take(8)
    me, row = lax.axis_index(AXIS), lax.axis_index(DATA)
    n = ex.size
    layers, cells = state_out.shape[0], state_out.shape[1]
    rows = state_ref.shape[0] // n
    greet([me ^ r for r in range(1, n)], [row ^ r for r in range(1, across)])
    pending, small_copies, wide_copies = [], [], []
    for r in range(1, across):
        small_copies.append(remote(small_ref, small_buf.at[r], small_send.at[r], small_recv.at[r], row ^ r, DATA))
        wide_copies.append(remote(wide_ref, wide_buf.at[r], wide_send.at[r], wide_recv.at[r], row ^ r, DATA))
        small_copies[-1].start()
        wide_copies[-1].start()
    loads, pairs = reduce_start(ex, state_ref, rows, bufs)
    total, wide = small_ref[...], wide_ref[...]
    for r in range(1, across):
        small_copies[r - 1].wait_recv()
        total = total + small_buf[r]
        wide_copies[r - 1].wait_recv()
        wide = wide + wide_buf[r]
    small_out[...] = total
    mid_buf[...] = wide
    all_copies = []
    for r in range(1, n):
        all_copies.append(remote(mid_buf, all_buf.at[r], all_send.at[r], all_recv.at[r], me ^ r))
        all_copies[-1].start()
    state = reduce_finish(ex, rows, bufs, loads, pairs, pending)
    for k in range(layers * across):
        cell_buf[k] = state[k * cells : (k + 1) * cells, :]
    cell_copies = {}
    for r in range(1, across):
        for layer in range(layers):
            k = r * layers + layer
            cell_copies[k] = remote(
                cell_buf.at[layer * across + (row ^ r)], cell_got.at[k], cell_send.at[k], cell_recv.at[k], row ^ r, DATA
            )
            cell_copies[k].start()
    wide_out[0] = wide
    total = wide
    for r in range(1, n):
        all_copies[r - 1].wait_recv()
        total = total + all_buf[r]
    wide_out[1] = total
    for layer in range(layers):
        value = cell_buf[layer * across + row]
        for r in range(1, across):
            cell_copies[r * layers + layer].wait_recv()
            value = value + cell_got[r * layers + layer]
        state_out[layer] = value
    for copy in pending + small_copies + wide_copies + all_copies + list(cell_copies.values()):
        copy.wait_send()


def sums_call(collective, ex, across, layers, state, small, wide):
    rows, both = state.shape[0] // ex.size, state.shape[1]
    cells = rows // (layers * across)
    vm = pl.BlockSpec(memory_space=pltpu.VMEM)
    dma = pltpu.SemaphoreType.DMA
    n = ex.size
    return pl.pallas_call(
        functools.partial(sums_kernel, ex, across),
        out_shape=(
            jax.ShapeDtypeStruct((layers, cells, both), F32),
            jax.ShapeDtypeStruct(small.shape, F32),
            jax.ShapeDtypeStruct((2,) + wide.shape, F32),
        ),
        in_specs=[pl.BlockSpec(memory_space=pl.ANY), vm, vm],
        out_specs=(vm, vm, vm),
        scratch_shapes=reduce_scratch(ex, rows, both) + [
            pltpu.VMEM((across,) + small.shape, F32), pltpu.VMEM((across,) + wide.shape, F32),
            pltpu.VMEM(wide.shape, F32), pltpu.VMEM((n,) + wide.shape, F32),
            pltpu.VMEM((layers * across, cells, both), F32), pltpu.VMEM((layers * across, cells, both), F32),
            dma((across,)), dma((across,)), dma((across,)), dma((across,)), dma((n,)), dma((n,)),
            dma((layers * across,)), dma((layers * across,)),
        ],
        compiler_params=pltpu.CompilerParams(collective_id=collective, has_side_effects=True, vmem_limit_bytes=VM),
        cost_estimate=cost_of(1 << 33),
        name="sums",
    )(state, small, wide)


LAYERS = 2
SIZE = 128

def shape_of(rows, depth):
    return jax.ShapeDtypeStruct((rows, depth), F32)


def row_scale_of(resid):
    return lax.rsqrt(jnp.mean(resid * resid, axis=1, keepdims=True) + EPS)


def retile(tiles, count):
    width = tiles.shape[1]
    if tiles.shape[0] == count * 8:
        return tiles
    flat = tiles.reshape(-1, 8, width)[:, 0, :].reshape(count, 1, -1)
    return jnp.broadcast_to(flat, (count, 8, flat.shape[2])).reshape(count * 8, -1)


def scatter_all(*arrays):
    flat = [a.reshape(a.shape[0], -1, a.shape[-1]) for a in arrays]
    if len({f.shape[2] for f in flat}) > 1:
        return [lax.psum_scatter(a, DATA, scatter_dimension=0, tiled=True)[0].astype(F32) for a in arrays]
    both = lax.psum_scatter(jnp.concatenate(flat, axis=1), DATA, scatter_dimension=0, tiled=True)[0].astype(F32)
    ends = [sum(f.shape[1] for f in flat[:i]) for i in range(len(flat) + 1)]
    return [both[ends[i] : ends[i + 1]].reshape(a.shape[1:]) for i, a in enumerate(arrays)]


def gate_of(square, inner_all):
    return lax.rsqrt(square / inner_all + EPS)


def start_middle(layer, total, square, ins, outs):
    resid, gain = ins[0][...], ins[1][layer : layer + 1, :]
    return (resid * row_scale_of(resid) * gain).astype(BF), None


def between_middle(layer, inner_all, total, square, ins, outs):
    gate = gate_of(square, inner_all)
    mixed = gate * total
    hidden = ins[0][...] + mixed
    outs[0][...] = hidden
    outs[1][...] = mixed
    outs[2][...] = gate
    return (hidden * row_scale_of(hidden) * ins[1][layer : layer + 1, :]).astype(BF), None


def turn_middle(inner_all, total, square, ins, outs):
    gate = gate_of(square, inner_all)
    mixed = gate * total
    grad = ins[1][...]
    outs[0][...] = ins[0][...] + mixed
    mean = -0.5 * gate * gate * jnp.sum(mixed * grad, axis=1, keepdims=True)
    return (gate * grad).astype(BF), mean


def norm_backward(layer, total, resid, grad, gain):
    scale = row_scale_of(resid)
    weighted = total * gain
    inner = jnp.sum(weighted * resid, axis=1, keepdims=True)
    gain_grad = jnp.sum(total * resid * scale, axis=0, keepdims=True)
    fresh = grad + scale * weighted - resid * (scale * scale * scale * inner / resid.shape[1])
    return fresh, gain_grad


def back_middle(layer, total, square, ins, outs):
    fresh, gain_grad = norm_backward(layer, total, ins[0][...], ins[1][...], ins[2][layer : layer + 1, :])
    outs[0][...] = fresh
    outs[1][...] = gain_grad
    mixed, gate = ins[3][...], ins[4][...]
    mean = -0.5 * gate * gate * jnp.sum(mixed * fresh, axis=1, keepdims=True)
    return (gate * fresh).astype(BF), mean


def end_middle(layer, total, square, ins, outs):
    fresh, gain_grad = norm_backward(layer, total, ins[0][...], ins[1][...], ins[2][layer : layer + 1, :])
    outs[0][...] = fresh
    outs[1][...] = gain_grad
    return None


def shards(ex, across, residual, cotangent, segments, *weights):
    w = Weights(*weights)
    rows, depth = residual.shape
    tokens = segments.shape[1]
    inner = w.inner_weight.shape[3]
    heads = w.step_weight.shape[2]
    inner_all = inner * ex.size
    count = tokens // SIZE
    gain = w.norm_gain
    meta, segrow = token_meta(segments[0], SIZE)
    ids = iter(range(100))
    resids, mixeds, gates, normeds, saved = [residual], [], [], [], []
    (normed,) = comm_call(
        "start", next(ids), ex, functools.partial(start_middle, 0), ins=(residual, gain), gather=depth
    )
    hidden = residual
    for layer in range(LAYERS):
        normeds.append(normed)
        made = forward_compute(layer, SIZE, normed, meta, segrow, w)
        saved.append(made[:8])
        part, squares = made[8:]
        squares = retile(squares, ex.size)
        if layer + 1 < LAYERS:
            normed, hidden, mixed, gate = comm_call(
                "between", next(ids), ex, functools.partial(between_middle, layer + 1, inner_all),
                part=part, psq=squares, ins=(hidden, gain),
                outs=(shape_of(rows, depth), shape_of(rows, depth), shape_of(rows, 1)), gather=depth,
            )
            resids.append(hidden)
            mixeds.append(mixed)
            gates.append(gate)
        else:
            sent, mean, block_output = comm_call(
                "turn", next(ids), ex, functools.partial(turn_middle, inner_all),
                part=part, psq=squares, ins=(hidden, cotangent), outs=(shape_of(rows, depth),), gather=depth, means=True,
            )
    grad = cotangent
    big, small = [None] * LAYERS, [None] * LAYERS
    for layer in range(LAYERS - 1, -1, -1):
        made = backward_compute(layer, SIZE, inner_all, sent, retile(mean, count), meta, segrow, saved[layer], w)
        rg, rv, rs, rd, sc, part = made[:6]
        g_inner, g_state, g_step, g_out = weight_compute(across, normeds[layer], sent, sc, rg, rv, rs, rd)
        part, g_inner, g_out = lax.optimization_barrier((part, g_inner, g_out))
        big[layer] = scatter_all(g_inner, g_out)
        if layer:
            sent, mean, grad, g_gain = comm_call(
                "back", next(ids), ex, functools.partial(back_middle, layer), part=part,
                ins=(resids[layer], grad, gain, mixeds[layer - 1], gates[layer - 1]),
                outs=(shape_of(rows, depth), shape_of(1, depth)), gather=depth, means=True,
            )
        else:
            grad, g_gain = comm_call(
                "end", next(ids), ex, functools.partial(end_middle, layer), part=part,
                ins=(resids[layer], grad, gain), outs=(shape_of(rows, depth), shape_of(1, depth)),
            )
        small[layer] = (made[6:], g_gain, g_state, g_step)
    taps = w.conv_weight.shape[1]
    both = w.state_weight.shape[2]
    cells = depth // (ex.size * across)

    def narrow(m):
        pad = jnp.zeros((1, inner - heads), F32)
        return jnp.concatenate(
            [m[0], m[1], m[4], m[5], jnp.concatenate([m[6], pad], axis=1), jnp.concatenate([m[7], pad], axis=1)], axis=0
        )

    def wide(item):
        m, g_gain, _, g_step = item
        pad = jnp.zeros((taps, depth - both), F32)
        return jnp.concatenate(
            [g_step, g_gain, jnp.concatenate([m[2], pad], axis=1), jnp.concatenate([m[3], pad[:1]], axis=1)], axis=0
        )

    state = jnp.stack([item[2].reshape(across, ex.size, cells, both) for item in small])
    state = jnp.transpose(state, (2, 0, 1, 3, 4)).reshape(-1, both)
    g_state, narrow_sum, wide_sum = sums_call(
        next(ids), ex, across, LAYERS, state,
        jnp.stack([narrow(item[0]) for item in small]), jnp.stack([wide(item) for item in small]),
    )
    per_dp = wide_sum[0, :, :heads]
    everywhere = wide_sum[1, :, heads:]
    own = lax.axis_index(DATA)
    step_cols = depth // across
    g_step = jnp.transpose(lax.dynamic_slice_in_dim(per_dp, own * step_cols, step_cols, 2), (0, 2, 1))
    device = own * ex.size + lax.axis_index(AXIS)
    g_norm = lax.dynamic_slice_in_dim(everywhere[:, 0], device * cells, cells, 1)
    return (
        block_output,
        grad,
        g_norm,
        jnp.stack([item[0] for item in big]),
        g_state,
        g_step,
        narrow_sum[:, taps + 3, :heads],
        narrow_sum[:, taps + 4, :heads],
        narrow_sum[:, taps + 2].reshape(LAYERS, heads, -1).sum(2),
        narrow_sum[:, :taps],
        narrow_sum[:, taps],
        everywhere[:, 1 : taps + 1, :both],
        everywhere[:, taps + 1, :both],
        narrow_sum[:, taps + 1],
        jnp.stack([item[1] for item in big]),
    )


def solution(mesh):
    ex = Exchange(mesh.shape[AXIS])
    both, rest = (DATA, AXIS), None
    return jax.shard_map(
        functools.partial(shards, ex, mesh.shape[DATA]),
        mesh=mesh,
        in_specs=(
            P(both, rest),
            P(both, rest),
            P(DATA, rest),
            P(),
            P(rest, rest, rest, AXIS),
            P(),
            P(rest, rest, AXIS),
            P(rest, AXIS),
            P(rest, AXIS),
            P(rest, AXIS),
            P(rest, rest, AXIS),
            P(rest, AXIS),
            P(),
            P(),
            P(rest, AXIS),
            P(rest, AXIS, rest),
        ),
        out_specs=(
            P(both, rest),
            P(both, rest),
            P(rest, both),
            P(rest, rest, DATA, AXIS),
            P(rest, both, rest),
            P(rest, DATA, AXIS),
            P(rest, AXIS),
            P(rest, AXIS),
            P(rest, AXIS),
            P(rest, rest, AXIS),
            P(rest, AXIS),
            P(),
            P(),
            P(rest, AXIS),
            P(rest, AXIS, DATA),
        ),
        check_vma=False,
    )
```

```python
import functools
from types import SimpleNamespace
from typing import NamedTuple

import jax
import jax.numpy as jnp
from jax import lax
from jax.experimental import pallas as pl
from jax.experimental.pallas import tpu as pltpu
from jax.sharding import PartitionSpec as P

LAYERS = 2
SIZE = 128
AXIS = "tensor"
DATA = "dp"
EPS = 1e-05
HIGH = lax.Precision.HIGHEST
F32 = jnp.float32
BF = jnp.bfloat16
VM = 67_000_000


def cost_of(flops, moved=1 << 24):
    return pl.CostEstimate(flops=flops, bytes_accessed=moved, transcendentals=0)


class Weights(NamedTuple):
    norm_gain: jax.Array
    inner_weight: jax.Array
    state_weight: jax.Array
    step_weight: jax.Array
    step_bias: jax.Array
    decay_log: jax.Array
    skip_gain: jax.Array
    conv_weight: jax.Array
    conv_bias: jax.Array
    state_conv_weight: jax.Array
    state_conv_bias: jax.Array
    gate_gain: jax.Array
    out_weight: jax.Array


def dot(a, b):
    return lax.dot_general(a, b, (((1,), (0,)), ((), ())), preferred_element_type=F32)


def dot_t(a, b):
    return lax.dot_general(a, b, (((1,), (1,)), ((), ())), preferred_element_type=F32)


def t_dot(a, b):
    return lax.dot_general(a, b, (((0,), (0,)), ((), ())), preferred_element_type=F32)


def exact(a, b):
    return lax.dot_general(
        a, b, (((1,), (0,)), ((), ())), preferred_element_type=F32, precision=HIGH
    )


def sigmoid(x):
    return 1.0 / (1.0 + jnp.exp(-x))


def softplus(x):
    return jnp.maximum(x, 0.0) + jnp.log1p(jnp.exp(-jnp.abs(x)))


def tiles_of(inner, width):
    return [
        (start, min(128, inner - start), start // width, min(128, inner - start) // width)
        for start in range(0, inner, 128)
    ]


def expand(cols, inner, width):
    rows = cols.shape[0]
    parts = []
    for _, wide, first, number in tiles_of(inner, width):
        lane = lax.broadcasted_iota(jnp.int32, (rows, wide), 1)
        value = jnp.broadcast_to(cols[:, first : first + 1], (rows, wide))
        for j in range(1, number):
            value = jnp.where(lane >= j * width, cols[:, first + j : first + j + 1], value)
        parts.append(value)
    return parts[0] if len(parts) == 1 else jnp.concatenate(parts, axis=1)


def head_sum_matrix(inner, heads, width):
    row = lax.broadcasted_iota(jnp.int32, (inner, heads), 0)
    col = lax.broadcasted_iota(jnp.int32, (inner, heads), 1)
    return ((row >= col * width) & (row < (col + 1) * width)).astype(BF)


def head_sum(value, inner, heads, width):
    ones = head_sum_matrix(inner, heads, width)
    high = value.astype(BF)
    low = (value - high.astype(F32)).astype(BF)
    return dot(high, ones) + dot(low, ones)


def head_split(tile, width, number):
    if number == 1:
        return tile
    lane = lax.broadcasted_iota(jnp.int32, tile.shape, 1)
    zero = jnp.zeros_like(tile)
    return jnp.concatenate(
        [
            jnp.where((lane >= j * width) & (lane < (j + 1) * width), tile, zero)
            for j in range(number)
        ],
        axis=0,
    )


def pair_mask(seg_col, seg_row):
    rows, cols = seg_col.shape[0], seg_row.shape[1]
    row = lax.broadcasted_iota(jnp.int32, (rows, cols), 0)
    col = lax.broadcasted_iota(jnp.int32, (rows, cols), 1)
    return (row >= col) & (seg_col == seg_row)


def lower_ones(size):
    row = lax.broadcasted_iota(jnp.int32, (size, size), 0)
    col = lax.broadcasted_iota(jnp.int32, (size, size), 1)
    return (row >= col).astype(F32)


def turned(value):
    return jnp.transpose(value)


def column_of(tile):
    rows = tile.shape[1]
    return jnp.transpose(jnp.broadcast_to(tile[0:1, :], (rows, rows)))[:, 0:1]


def tile_of(column):
    rows = column.shape[0]
    return jnp.transpose(jnp.broadcast_to(column, (rows, rows)))[0:8, :]


def later_ones(seg_col, seg_row):
    rows, cols = seg_col.shape[0], seg_row.shape[1]
    row = lax.broadcasted_iota(jnp.int32, (rows, cols), 0)
    col = lax.broadcasted_iota(jnp.int32, (rows, cols), 1)
    return ((row <= col) & (seg_col == seg_row)).astype(F32)


def earlier_ones(seg_col, seg_row):
    rows, cols = seg_col.shape[0], seg_row.shape[1]
    row = lax.broadcasted_iota(jnp.int32, (rows, cols), 0)
    col = lax.broadcasted_iota(jnp.int32, (rows, cols), 1)
    return ((row > col) & (seg_col == seg_row)).astype(F32)


def token_meta(segment, size):
    tokens = segment.shape[0]
    seg = segment.astype(F32)

    def back(k):
        return jnp.concatenate([jnp.full((k,), -1.0, F32), seg[:-k]])

    blocks = seg.reshape(-1, size)
    gone = jnp.full((1,), -1.0, F32)
    before = jnp.concatenate([gone, blocks[:-1, -1]])
    after = jnp.concatenate([blocks[1:, 0], gone])
    per = lambda v: jnp.broadcast_to(v[:, None], blocks.shape)
    end = per(blocks[:, -1])
    columns = [
        seg,
        (back(1) == seg).astype(F32),
        (back(2) == seg).astype(F32),
        (back(3) == seg).astype(F32),
        (blocks == per(before)).astype(F32).reshape(-1),
        (blocks == end).astype(F32).reshape(-1),
        (end == per(before)).astype(F32).reshape(-1),
        (blocks == per(after)).astype(F32).reshape(-1),
    ]
    rows = jnp.stack(columns)
    return rows.T, rows


def span_of(dims):
    found = [0]
    for d in dims:
        found = found + [r ^ d for r in found]
    return found


def most_first(offsets):
    return sorted(offsets, key=lambda r: -bin(r).count("1"))


class Cube:
    def __init__(self, size):
        self.size = size
        self.links = [1 << b for b in range(1, size.bit_length() - 1)]
        self.orders = [self.links, self.links[::-1]]
        self.offsets = most_first(span_of(self.links))

    def gather_dims(self, q):
        return self.orders[q] + [1]

    def gather_last(self, q, r):
        return max([i for i, d in enumerate(self.gather_dims(q)) if r & d], default=-1)

    def gather_steps(self, q):
        found = [r for r in span_of(self.links) if r]
        return sorted(found, key=lambda r: (self.gather_last(q, r), r & (r - 1) != 0))


def reduce_steps(order):
    steps = []
    for i, d in enumerate(order):
        for s in most_first(span_of(order[i + 1 :])):
            steps.append((i, d ^ s))
    return steps + [(len(order), 0)]


def arrival_slots(order, first=0):
    found = {}
    for i, r in reduce_steps(order):
        for j in range(i):
            found[(j, r)] = first + len(found)
    return found


def remote(src, dst, send, recv, target, axis=AXIS):
    return pltpu.make_async_remote_copy(
        src_ref=src, dst_ref=dst, send_sem=send, recv_sem=recv,
        device_id={axis: target}, device_id_type=pl.DeviceIdType.MESH,
    )


def greet(targets, across=()):
    barrier = pltpu.get_barrier_semaphore()
    for axis, group in ((AXIS, targets), (DATA, across)):
        for target in group:
            pl.semaphore_signal(barrier, inc=1, device_id={axis: target}, device_id_type=pl.DeviceIdType.MESH)
    pl.semaphore_wait(barrier, len(targets) + len(across))


def rows_of(block, rows, many=1):
    return pl.ds(pl.multiple_of(block * rows, rows), rows * many)


def dma(*shape):
    return pltpu.SemaphoreType.DMA(shape)


def gather_sems(ex):
    return dma(2, ex.size), dma(2, ex.size)


def gather_rows(ex, rows, row_buf, out, sems, visit, ahead=None):
    me = lax.axis_index(AXIS)
    send_sem, recv_sem = sems
    half = rows // 2
    copies, arrived = {}, set()

    def forward(q, r):
        dims = ex.gather_dims(q)
        place = pl.ds(pl.multiple_of((me ^ r) * rows + q * half, half), half)
        src = row_buf.at[pl.ds(q * half, half), :] if r == 0 else out.at[place, :]
        for i in range(ex.gather_last(q, r) + 1, len(dims)):
            beyond = r ^ dims[i]
            yield beyond, remote(src, out.at[place, :], send_sem.at[q, beyond], recv_sem.at[q, beyond], me ^ dims[i])

    def need(q, r):
        if (q, r) not in arrived:
            copies[(q, r)].wait_recv()
            arrived.add((q, r))
            for beyond, copy in forward(q, r):
                copy.start()
                copies[(q, beyond)] = copy

    first = [list(forward(q, 0)) for q in range(2)]
    for i in range(len(first[0])):
        for q in range(2):
            beyond, copy = first[q][i]
            copy.start()
            copies[(q, beyond)] = copy
    out[rows_of(me, rows), :] = row_buf[...]
    if ahead is not None:
        ahead()
    steps = [ex.gather_steps(q) for q in range(2)]
    visits = sorted(span_of(ex.links), key=lambda g: (ex.gather_last(0, g), g & (g - 1) != 0))
    k = 0
    for g in visits:
        while g and not all((q, g) in arrived for q in range(2)):
            for q in range(2):
                need(q, steps[q][k])
            k += 1
        for q in range(2):
            need(q, g ^ 1)
        visit(g)
    return list(copies.values())


def reduce_scratch(ex, rows, depth):
    slots, half = ex.size // 2, rows // 2
    return dict(
        pair=pltpu.VMEM((slots, rows, depth), BF),
        stage=pltpu.VMEM((2 * slots, half, depth), BF),
        got=pltpu.VMEM((2 * (slots - 1), half, depth), BF),
    )


def reduce_sems(ex):
    slots = ex.size // 2
    return dma(slots), dma(slots), dma(2 * slots), dma(2 * (slots - 1))


def reduce_rows(ex, rows, part, pair, stage, got, sems, produce, pending):
    me = lax.axis_index(AXIS)
    pair_send, pair_recv, link_send, link_recv = sems
    n, half = ex.size, rows // 2
    slot_of = {r: i for i, r in enumerate(ex.offsets)}
    steps = [reduce_steps(order) for order in ex.orders]
    slots = [arrival_slots(order, q * (n // 2 - 1)) for q, order in enumerate(ex.orders)]
    waiting = list(ex.offsets)
    pairs, ready, arrivals, final = {}, set(), {}, [None, None]

    def advance():
        r = waiting.pop(0)
        produce(r)
        i = slot_of[r]
        pairs[r] = remote(part.at[rows_of(me ^ r ^ 1, rows), :], pair.at[i], pair_send.at[i], pair_recv.at[i], me ^ 1)
        pairs[r].start()

    advance()
    for k in range(len(steps[0])):
        if waiting:
            advance()
        for q in range(2):
            i, r = steps[q][k]
            while r not in pairs:
                advance()
            if r not in ready:
                pairs[r].wait_recv()
                ready.add(r)
            own = part[pl.ds(pl.multiple_of((me ^ r) * rows + q * half, half), half), :]
            value = own.astype(F32) + pair[slot_of[r], pl.ds(q * half, half), :].astype(F32)
            for j in range(i):
                arrivals[(q, j, r)].wait_recv()
                value = value + got[slots[q][(j, r)]].astype(F32)
            if r == 0:
                final[q] = value
                continue
            d = ex.orders[q][i]
            s = q * (n // 2) + slot_of[r]
            stage[s] = value.astype(BF)
            at = slots[q][(i, r ^ d)]
            copy = remote(stage.at[s], got.at[at], link_send.at[s], link_recv.at[at], me ^ d)
            copy.start()
            arrivals[(q, i, r ^ d)] = copy
            pending.append(copy)
    pending.extend(pairs.values())
    return jnp.concatenate(final, axis=0)


def row_scale_of(resid):
    return lax.rsqrt(jnp.mean(resid * resid, axis=1, keepdims=True) + EPS)


def group_rows(ex, g, rows):
    me = lax.axis_index(AXIS)
    return pl.ds(pl.multiple_of(((me ^ g) // 2) * (2 * rows), 2 * rows), 2 * rows)


class Sizes(NamedTuple):
    tokens: int
    rows: int
    depth: int
    inner: int
    heads: int
    both: int
    taps: int
    inner_all: int
    across: int

    @property
    def width(self):
        return self.inner // self.heads

    @property
    def half(self):
        return self.both // 2

    @property
    def count(self):
        return self.tokens // SIZE


def weight_scratch(z, layers):
    return dict(
        win=pltpu.VMEM((layers, 2, z.depth, z.inner), BF),
        wst=pltpu.VMEM((layers, z.depth, z.both), BF),
        wstep=pltpu.VMEM((layers, z.heads, z.depth), BF),
        wout=pltpu.VMEM((layers, z.inner, z.depth), BF),
        weight_sem=dma(LAYERS, 4),
    )


def weight_loads(s, a, layer, slot):
    return [
        pltpu.make_async_copy(src.at[layer], dst.at[slot], s.weight_sem.at[layer, i])
        for i, (src, dst) in enumerate(
            ((a.inner_weight, s.win), (a.state_weight, s.wst), (a.step_weight, s.wstep), (a.out_weight, s.wout))
        )
    ]


def saved_shapes(z):
    t, i = z.tokens, z.inner
    return dict(
        normed=((t, z.depth), BF), gate=((t, i), F32), pre_v=((t, i), F32), y=((t, i), F32), pre_s=((t, z.both), F32),
        step_in=((t, z.heads), F32), value=((t, i), BF), raw=((t, z.both), BF), scaled=((t, i), BF),
        entering=((z.count, z.half, i), BF),
    )


def mix_forward(z, layer, s, a, meta, segrow):
    at = slice(layer, layer + 1)
    inner, width, half = z.inner, z.width, z.half
    s.state[...] = jnp.zeros_like(s.state)
    group = 2 if z.count % 2 == 0 else 1

    def chunk(c, before):
        rows = pl.ds(pl.multiple_of(c * SIZE, SIZE), SIZE)
        window = pl.ds(pl.multiple_of(c * SIZE, SIZE), SIZE + 8)
        m = meta[rows, :]

        def conv(buf, w_ref, b_ref):
            win = buf[window, :]
            total = b_ref[at, :] + w_ref[layer, 0:1, :] * win[8:, :]
            for k in range(1, z.taps):
                total = total + w_ref[layer, k : k + 1, :] * (win[8 - k : 8 - k + SIZE, :] * m[:, k : k + 1])
            return total, win[8:, :]

        pre_v, value = conv(s.vbuf, a.conv_weight, a.conv_bias)
        pre_s, raw = conv(s.sbuf, a.state_conv_weight, a.state_conv_bias)
        s.value[rows, :] = value.astype(BF)
        s.raw[rows, :] = raw.astype(BF)
        s.pre_v[rows, :] = pre_v
        s.pre_s[rows, :] = pre_s
        x = pre_v * sigmoid(pre_v)
        st = pre_s * sigmoid(pre_s)
        b_mat = st[:, :half].astype(BF)
        c_mat = st[:, half:].astype(BF)
        dt = softplus(s.step_in[rows, :] + a.step_bias[at, :])
        log_decay = -dt * jnp.exp(a.decay_log[at, :])
        cum = exact(lower_ones(SIZE), log_decay)
        cum_t = turned(cum)
        last = cum[SIZE - 1 : SIZE, :]
        xt = (x * expand(dt, inner, width)).astype(BF)
        from_state = jnp.exp(cum) * m[:, 4:5]
        to_end = jnp.exp(last - cum) * m[:, 5:6]
        carry = jnp.exp(last) * m[0:1, 6:7]
        before_b = before.astype(BF)
        s.entering[c] = before_b
        scores = dot_t(c_mat, b_mat)
        mask = pair_mask(m[:, 0:1], segrow[0:1, rows])
        parts = []
        for start, wide, first, number in tiles_of(inner, width):
            mats = []
            for h in range(first, first + number):
                differ = cum[:, h : h + 1] - cum_t[h : h + 1, :]
                mats.append((jnp.exp(jnp.where(mask, differ, -1e30)) * scores).astype(BF))
            left = mats[0] if number == 1 else jnp.concatenate(mats, axis=1)
            parts.append(dot(left, head_split(xt[:, start : start + wide], width, number)))
        intra = parts[0] if len(parts) == 1 else jnp.concatenate(parts, axis=1)
        inter = dot(c_mat, before_b) * expand(from_state, inner, width)
        y = intra + inter + expand(a.skip_gain[at, :], inner, width) * x
        s.y[rows, :] = y
        ended = (xt.astype(F32) * expand(to_end, inner, width)).astype(BF)
        after = expand(carry, inner, width) * before + t_dot(b_mat, ended)
        gate = s.gate[rows, :]
        gated = y * (gate * sigmoid(gate))
        square = jnp.sum(gated * gated, axis=1, keepdims=True)
        tile = tile_of(square)
        per = SIZE // z.rows if SIZE > z.rows else 1
        wide = SIZE // per
        for k in range(per):
            s.squares[c * per + k] = tile[:, k * wide : (k + 1) * wide]
        s.scaled[rows, :] = (gated * a.gate_gain[at, :]).astype(BF)
        return after

    def body(i, carry):
        before = s.state[...]
        for k in range(group):
            before = chunk(i * group + k, before)
        s.state[...] = before
        return carry

    lax.fori_loop(0, z.count // group, body, 0)


def forward_kernel(ex, z, names_in, names_out, names_scratch, *refs):
    count_in, count_out = len(names_in), len(names_out)
    a = SimpleNamespace(**dict(zip(names_in, refs)))
    o = SimpleNamespace(**dict(zip(names_out, refs[count_in:])))
    s = SimpleNamespace(**dict(zip(names_scratch, refs[count_in + count_out :])))
    me = lax.axis_index(AXIS)
    n = ex.size
    greet([me ^ r for r in range(1, n)])
    loads = [weight_loads(s, a, layer, layer) for layer in range(LAYERS)]
    for copy in loads[0] + loads[1]:
        copy.start()
    s.vbuf[0:8, :] = jnp.zeros((8, z.inner), F32)
    s.sbuf[0:8, :] = jnp.zeros((8, z.both), F32)
    pending, saves = [], []
    hidden = a.residual[...]
    for layer in range(LAYERS):
        s.row_buf[...] = (hidden * row_scale_of(hidden) * a.norm_gain[layer : layer + 1, :]).astype(BF)
        normed = s.normed.at[layer]
        for copy in saves:
            copy.wait()
        saves = []

        def project(g, layer=layer, normed=normed):
            if g == 0:
                for copy in loads[layer]:
                    copy.wait()
            here = group_rows(ex, g, z.rows)
            beyond = pl.ds(pl.multiple_of(((me ^ g) // 2) * (2 * z.rows) + 8, 8), 2 * z.rows)
            nb = normed[here, :]
            s.gate[here, :] = dot(nb, s.win[layer, 0])
            s.vbuf[beyond, :] = dot(nb, s.win[layer, 1])
            s.sbuf[beyond, :] = dot(nb, s.wst[layer])
            s.step_in[here, :] = dot_t(nb, s.wstep[layer])

        sent = gather_rows(ex, z.rows, s.row_buf, normed, (s.gather_send.at[layer], s.gather_recv.at[layer]), project)
        mix_forward(z, layer, s, a, a.meta, a.segrow)
        for i, name in enumerate(names_out[: len(saved_shapes(z))]):
            src = normed if i == 0 else getattr(s, name)
            saves.append(pltpu.make_async_copy(src, getattr(o, name).at[layer], s.save_sem.at[layer, i]))
            saves[-1].start()
        for copy in sent:
            copy.wait_send()

        def produce(g, layer=layer):
            here = group_rows(ex, g, z.rows)
            s.part[here, :] = dot(s.scaled[here, :], s.wout[layer]).astype(BF)

        squares = []
        for r in range(1, n):
            squares.append(
                remote(s.squares.at[me ^ r], s.square_got.at[layer, r], s.square_send.at[layer, r], s.square_recv.at[layer, r], me ^ r)
            )
            squares[-1].start()
        links = []
        total = reduce_rows(
            ex, z.rows, s.part, s.pair, s.stage, s.got,
            (s.pair_send.at[layer], s.pair_recv.at[layer], s.link_send.at[layer], s.link_recv.at[layer]), produce, links,
        )
        square = s.squares[me]
        for r, copy in enumerate(squares, 1):
            copy.wait_recv()
            square = square + s.square_got[layer, r]
        gate = lax.rsqrt(column_of(square) / z.inner_all + EPS)
        mixed = gate * total
        hidden = hidden + mixed
        if layer + 1 < LAYERS:
            o.resids[layer] = hidden
            o.mixeds[layer] = mixed
            o.gates[layer] = gate
        for copy in links + squares:
            copy.wait_send()
    o.block_output[...] = hidden
    grad = a.cotangent[...]
    o.sent[...] = (gate * grad).astype(BF)
    o.mean[...] = tile_of(-0.5 * gate * gate * jnp.sum(mixed * grad, axis=1, keepdims=True))
    for copy in saves:
        copy.wait()


def run_kernel(kernel, ex, z, inputs, outputs, scratch, collective, name):
    vm, anywhere = pl.BlockSpec(memory_space=pltpu.VMEM), pl.BlockSpec(memory_space=pl.ANY)
    made = pl.pallas_call(
        functools.partial(kernel, ex, z, tuple(inputs), tuple(outputs), tuple(scratch)),
        out_shape=tuple(jax.ShapeDtypeStruct(shape, kind) for shape, kind, _ in outputs.values()),
        in_specs=[vm if inside else anywhere for _, inside in inputs.values()],
        out_specs=tuple(vm if inside else anywhere for _, _, inside in outputs.values()),
        scratch_shapes=list(scratch.values()),
        compiler_params=pltpu.CompilerParams(collective_id=collective, has_side_effects=True, vmem_limit_bytes=VM),
        cost_estimate=cost_of(1 << 35),
        name=name,
    )(*[array for array, _ in inputs.values()])
    return SimpleNamespace(**dict(zip(outputs, made)))


def small_inputs(w):
    return dict(
        norm_gain=(w.norm_gain, True), step_bias=(w.step_bias, True), decay_log=(w.decay_log, True),
        skip_gain=(w.skip_gain, True), conv_weight=(w.conv_weight, True), conv_bias=(w.conv_bias, True),
        state_conv_weight=(w.state_conv_weight, True), state_conv_bias=(w.state_conv_bias, True), gate_gain=(w.gate_gain, True),
        inner_weight=(w.inner_weight, False), state_weight=(w.state_weight, False), step_weight=(w.step_weight, False),
        out_weight=(w.out_weight, False),
    )


def forward_pass(ex, z, residual, cotangent, meta, segrow, w):
    n = ex.size
    saved = saved_shapes(z)
    inputs = dict(residual=(residual, True), cotangent=(cotangent, True), meta=(meta, True), segrow=(segrow, True), **small_inputs(w))
    rows = (z.rows, z.depth)
    outputs = {k: ((LAYERS,) + shape, kind, False) for k, (shape, kind) in saved.items()}
    outputs.update(
        resids=((LAYERS - 1,) + rows, F32, True), mixeds=((LAYERS - 1,) + rows, F32, True),
        gates=((LAYERS - 1, z.rows, 1), F32, True), block_output=(rows, F32, True),
        sent=(rows, BF, True), mean=((8, z.rows), F32, True),
    )
    scratch = {k: pltpu.VMEM(shape, kind) for k, (shape, kind) in saved.items()}
    scratch.update(normed=pltpu.VMEM((LAYERS, z.tokens, z.depth), BF))
    scratch.update(weight_scratch(z, LAYERS))
    scratch.update(reduce_scratch(ex, z.rows, z.depth))
    slots = n // 2
    scratch.update(
        vbuf=pltpu.VMEM((z.tokens + 8, z.inner), F32), sbuf=pltpu.VMEM((z.tokens + 8, z.both), F32),
        state=pltpu.VMEM((z.half, z.inner), F32), part=pltpu.VMEM((z.tokens, z.depth), BF), row_buf=pltpu.VMEM(rows, BF),
        squares=pltpu.VMEM((n, 8, z.rows), F32), square_got=pltpu.VMEM((LAYERS, n, 8, z.rows), F32),
        square_send=dma(LAYERS, n), square_recv=dma(LAYERS, n), save_sem=dma(LAYERS, len(saved)),
        gather_send=dma(LAYERS, 2, n), gather_recv=dma(LAYERS, 2, n), pair_send=dma(LAYERS, slots), pair_recv=dma(LAYERS, slots),
        link_send=dma(LAYERS, 2 * slots), link_recv=dma(LAYERS, 2 * (slots - 1)),
    )
    return run_kernel(forward_kernel, ex, z, inputs, outputs, scratch, 0, "forward")


class Piece:
    def __init__(self, across, own, stage, got, send, recv):
        self.order = [1 << b for b in range(across.bit_length() - 1)]
        self.own, self.stage, self.got, self.send, self.recv = own, stage, got, send, recv
        self.slots = arrival_slots(self.order)
        self.row = lax.axis_index(DATA)
        self.arrivals, self.sent = {}, []

    def value(self, i, r):
        total = self.own[self.row ^ r].astype(F32)
        for j in range(i):
            self.arrivals[(j, r)].wait_recv()
            total = total + self.got[self.slots[(j, r)]].astype(F32)
        return total

    def phase(self, k):
        for number, (i, r) in enumerate(reduce_steps(self.order)):
            if i != k or r == 0:
                continue
            src = self.own.at[self.row ^ r]
            if i:
                self.stage[number] = self.value(i, r).astype(BF)
                src = self.stage.at[number]
            d = self.order[i]
            at = self.slots[(i, r ^ d)]
            copy = remote(src, self.got.at[at], self.send.at[number], self.recv.at[at], self.row ^ d, DATA)
            copy.start()
            self.arrivals[(i, r ^ d)] = copy
            self.sent.append(copy)

    def last(self):
        total = self.value(len(self.order), 0)
        for copy in self.sent:
            copy.wait_send()
        return total


def mix_backward(z, layer, s, a, meta, segrow):
    at = slice(layer, layer + 1)
    inner, width, half, heads, taps = z.inner, z.width, z.half, z.heads, z.taps
    s.state[...] = jnp.zeros_like(s.state)
    group = 2 if z.count % 2 == 0 else 1

    def chunk(c, after):
        rows = pl.ds(pl.multiple_of(c * SIZE, SIZE), SIZE)
        m = meta[rows, :]
        y, dy = s.y[rows, :], s.dy[rows, :]
        pre_v, pre_s = s.pre_v[rows, :], s.pre_s[rows, :]
        sig_v, sig_s = sigmoid(pre_v), sigmoid(pre_s)
        x = pre_v * sig_v
        st = pre_s * sig_s
        b_mat = st[:, :half].astype(BF)
        c_mat = st[:, half:].astype(BF)
        raw_step = s.step_in[rows, :] + a.step_bias[at, :]
        dt = softplus(raw_step)
        rate = jnp.exp(a.decay_log[at, :])
        log_decay = -dt * rate
        cum = exact(lower_ones(SIZE), log_decay)
        cum_t = turned(cum)
        last = cum[SIZE - 1 : SIZE, :]
        dt_all = expand(dt, inner, width)
        skip_all = expand(a.skip_gain[at, :], inner, width)
        xt = (x * dt_all).astype(BF)
        dy_b = dy.astype(BF)
        from_state = expand(jnp.exp(cum) * m[:, 4:5], inner, width)
        to_end = expand(jnp.exp(last - cum) * m[:, 5:6], inner, width)
        carry = expand(jnp.exp(last) * m[0:1, 6:7], inner, width)
        scores = dot_t(c_mat, b_mat)
        mask = pair_mask(m[:, 0:1], segrow[0:1, rows])
        d_scores = jnp.zeros((SIZE, SIZE), F32)
        parts = []
        for start, wide, first, number in tiles_of(inner, width):
            dy_split = head_split(dy_b[:, start : start + wide], width, number)
            d_mats = dot_t(dy_split, xt[:, start : start + wide])
            mats = []
            for j in range(number):
                h = first + j
                differ = cum[:, h : h + 1] - cum_t[h : h + 1, :]
                decay = jnp.exp(jnp.where(mask, differ, -1e30))
                mats.append((decay * scores).astype(BF))
                d_scores = d_scores + d_mats[j * SIZE : (j + 1) * SIZE, :] * decay
            left = mats[0] if number == 1 else jnp.concatenate(mats, axis=0)
            parts.append(t_dot(left, dy_split))
        intra = parts[0] if len(parts) == 1 else jnp.concatenate(parts, axis=1)
        d_scores = d_scores.astype(BF)
        before = s.entering[c]
        after_b = after.astype(BF)
        dy_in = (dy * from_state).astype(BF)
        xt_f = xt.astype(F32)
        ended = (xt_f * to_end).astype(BF)
        from_later = dot(b_mat, after_b) * to_end
        d_xt = intra + from_later
        d_c = dot(d_scores, b_mat) + dot_t(dy_in, before)
        d_b = t_dot(d_scores, c_mat) + dot_t(ended, after_b)
        across = carry * jnp.sum(before.astype(F32) * after, axis=0, keepdims=True)
        fresh = carry * after + t_dot(c_mat, dy_in)
        sums = head_sum(
            jnp.concatenate(
                [
                    dy_b.astype(F32) * (y - skip_all * x) - xt_f * intra,
                    xt_f * from_later,
                    x * d_xt,
                    jnp.broadcast_to(across, (8, inner)),
                ],
                axis=0,
            ),
            inner, heads, width,
        )
        seg_col, seg_row = m[:, 0:1], segrow[0:1, rows]
        d_log = (
            exact(later_ones(seg_col, seg_row), sums[0:SIZE])
            + exact(earlier_ones(seg_col, seg_row), sums[SIZE : 2 * SIZE])
            + sums[3 * SIZE : 3 * SIZE + 1]
        )
        d_raw = (sums[2 * SIZE : 3 * SIZE] - rate * d_log) * sigmoid(raw_step)
        s.rd[rows, :] = d_raw.astype(BF)
        d_x = dy * skip_all + d_xt * dt_all
        s.d_pre_v[rows, :] = d_x * (sig_v * (1.0 + pre_v * (1.0 - sig_v)))
        d_st = jnp.concatenate([d_b, d_c], axis=1)
        s.d_pre_s[rows, :] = d_st * (sig_s * (1.0 + pre_s * (1.0 - sig_s)))
        total = lambda v: jnp.sum(v, axis=0, keepdims=True)
        return fresh, (total(dy * x), total(d_raw), total(d_log * log_decay))

    def body(i, sums):
        after = s.state[...]
        for k in range(group):
            after, more = chunk(z.count - 1 - (i * group + k), after)
            sums = tuple(u + v for u, v in zip(sums, more))
        s.state[...] = after
        return sums

    zero = lambda wide: jnp.zeros((1, wide), F32)
    skip, bias, decay = lax.fori_loop(0, z.count // group, body, (zero(inner), zero(heads), zero(heads)))
    s.narrow[layer, taps + 2 : taps + 3, :] = skip
    s.narrow[layer, taps + 3 : taps + 4, 0:heads] = bias
    s.narrow[layer, taps + 4 : taps + 5, 0:heads] = decay

    def conv_body(c, sums):
        rows = pl.ds(pl.multiple_of(c * SIZE, SIZE), SIZE)
        window = pl.ds(pl.multiple_of(c * SIZE, SIZE), SIZE + 8)
        m = meta[window, :]
        more = []
        for src, w_ref, value_ref, dst in ((s.d_pre_v, a.conv_weight, s.value, s.rv), (s.d_pre_s, a.state_conv_weight, s.raw, s.rs)):
            win = src[window, :]
            value = value_ref[rows, :].astype(F32)
            now = win[0:SIZE, :]
            total = w_ref[layer, 0:1, :] * now
            lines = [jnp.sum(now * value, axis=0, keepdims=True)]
            for k in range(1, taps):
                moved = win[k : k + SIZE, :] * m[k : k + SIZE, k : k + 1]
                total = total + w_ref[layer, k : k + 1, :] * moved
                lines.append(jnp.sum(moved * value, axis=0, keepdims=True))
            lines.append(jnp.sum(now, axis=0, keepdims=True))
            dst[rows, :] = total.astype(BF)
            more.extend(lines)
        return tuple(u + v for u, v in zip(sums, more))

    lines = lax.fori_loop(0, z.count, conv_body, (zero(inner),) * (taps + 1) + (zero(z.both),) * (taps + 1))
    for k in range(taps + 1):
        s.narrow[layer, k : k + 1, :] = lines[k]
        s.wide[layer, k : k + 1, :] = lines[taps + 1 + k]


def norm_backward(total, resid, grad, gain):
    scale = row_scale_of(resid)
    weighted = total * gain
    inner = jnp.sum(weighted * resid, axis=1, keepdims=True)
    gain_grad = jnp.sum(total * resid * scale, axis=0, keepdims=True)
    return grad + scale * weighted - resid * (scale * scale * scale * inner / resid.shape[1]), gain_grad


def exchange(src, got, send, recv, place, number, axis):
    copies = [remote(src, got.at[r], send.at[r], recv.at[r], place ^ r, axis) for r in range(1, number)]
    for copy in copies:
        copy.start()
    return copies


def collected(own, got, copies):
    total = own
    for r, copy in enumerate(copies, 1):
        copy.wait_recv()
        total = total + got[r]
    return total


def backward_kernel(ex, z, names_in, names_out, names_scratch, *refs):
    count_in, count_out = len(names_in), len(names_out)
    a = SimpleNamespace(**dict(zip(names_in, refs)))
    o = SimpleNamespace(**dict(zip(names_out, refs[count_in:])))
    s = SimpleNamespace(**dict(zip(names_scratch, refs[count_in + count_out :])))
    me, row = lax.axis_index(AXIS), lax.axis_index(DATA)
    n, across, taps, heads = ex.size, z.across, z.taps, z.heads
    share = z.depth // across
    cells = z.depth // (n * across)
    padded = padded_cells(z, n)
    greet([me ^ r for r in range(1, n)], [row ^ r for r in range(1, across)])
    saved = list(saved_shapes(z))

    def start_loads(layer):
        found = weight_loads(s, a, layer, 0)
        found += [pltpu.make_async_copy(getattr(a, k).at[layer], getattr(s, k), s.save_sem.at[layer, i]) for i, k in enumerate(saved)]
        for copy in found:
            copy.start()
        return found

    loads = start_loads(LAYERS - 1)
    for ref in (s.narrow, s.wide, s.gain):
        ref[...] = jnp.zeros_like(ref)
    s.d_pre_v[z.tokens :, :] = jnp.zeros((8, z.inner), F32)
    s.d_pre_s[z.tokens :, :] = jnp.zeros((8, z.both), F32)
    if padded != cells:
        s.state_part[...] = jnp.zeros_like(s.state_part)
    grad = a.cotangent[...]
    s.row_buf[...] = a.sent[...]
    tile = a.mean[...]
    narrow_copies, outs, older = [None] * LAYERS, [], None

    def finish(piece, k, layer):
        s.done[k] = piece.last()
        target = o.g_out.at[layer] if k == 0 else o.g_inner.at[layer, k - 1]
        copy = pltpu.make_async_copy(s.done.at[k], target, s.done_sem.at[layer, k])
        copy.start()
        return copy

    for layer in range(LAYERS - 1, -1, -1):
        s.mean_own[layer] = tile
        means = []

        def ahead(layer=layer, means=means):
            for r in range(1, n):
                means.append(
                    remote(s.mean_own.at[layer], s.mean_all.at[layer, me], s.mean_send.at[layer, r], s.mean_recv.at[layer, r], me ^ r)
                )
                means[-1].start()
            s.mean_all[layer, me] = s.mean_own[layer]

        def visit(g, layer=layer, means=means, loads=loads):
            if g == 0:
                for copy in loads:
                    copy.wait()
            here = group_rows(ex, g, z.rows)
            first = (me ^ g) // 2 * 2
            for r in (g, g ^ 1):
                if r:
                    means[r - 1].wait_recv()
            mean = jnp.concatenate([column_of(s.mean_all[layer, first]), column_of(s.mean_all[layer, first + 1])], axis=0)
            at = slice(layer, layer + 1)
            grad_scaled = dot_t(s.sent_all[here, :], s.wout[0])
            gate, y = s.gate[here, :], s.y[here, :]
            gate_sig = sigmoid(gate)
            silu_gate = gate * gate_sig
            gated = y * silu_gate
            s.narrow[layer, taps + 1 : taps + 2, :] += jnp.sum(grad_scaled * gated, axis=0, keepdims=True)
            grad_gated = grad_scaled * a.gate_gain[at, :] + (2.0 / z.inner_all) * mean * gated
            s.rg[here, :] = (grad_gated * y * (gate_sig * (1.0 + gate * (1.0 - gate_sig)))).astype(BF)
            s.dy[here, :] = grad_gated * silu_gate

        sent = gather_rows(ex, z.rows, s.row_buf, s.sent_all, (s.gather_send.at[layer], s.gather_recv.at[layer]), visit, ahead)
        pieces = [
            Piece(
                across, own, s.piece_stage.at[k], s.piece_got.at[layer, k], s.piece_send.at[layer, k], s.piece_recv.at[layer, k]
            )
            for k, own in enumerate((s.own_out, s.own_inner.at[0], s.own_inner.at[1]))
        ]
        if older is not None:
            older[2].phase(1)
            for copy in outs:
                copy.wait()
            outs.clear()
        for i in range(across):
            s.own_out[i] = t_dot(s.scaled[...], s.sent_all[:, i * share : (i + 1) * share]).astype(BF)
        pieces[0].phase(0)
        for i in range(across):
            s.own_inner[0, i] = t_dot(s.normed[:, i * share : (i + 1) * share], s.rg[...]).astype(BF)
        pieces[1].phase(0)
        mix_backward(z, layer, s, a, a.meta, a.segrow)
        if older is not None:
            for k in range(2, len(older[2].order)):
                older[2].phase(k)
            outs.append(finish(older[2], 2, layer + 1))
        pieces[0].phase(1)
        narrow_copies[layer] = exchange(
            s.narrow.at[layer], s.narrow_got.at[layer], s.narrow_send.at[layer], s.narrow_recv.at[layer], row, across, DATA
        )
        for i in range(across):
            s.own_inner[1, i] = t_dot(s.normed[:, i * share : (i + 1) * share], s.rv[...]).astype(BF)
        pieces[2].phase(0)

        def produce(g, layer=layer):
            here = group_rows(ex, g, z.rows)
            total = dot_t(s.rg[here, :], s.win[0, 0]) + dot_t(s.rv[here, :], s.win[0, 1])
            total = total + dot_t(s.rs[here, :], s.wst[0]) + dot(s.rd[here, :], s.wstep[0])
            s.part[here, :] = total.astype(BF)

        for copy in sent + means:
            copy.wait_send()
        links = []
        total = reduce_rows(
            ex, z.rows, s.part, s.pair, s.stage, s.got,
            (s.pair_send.at[layer], s.pair_recv.at[layer], s.link_send.at[layer], s.link_recv.at[layer]), produce, links,
        )
        pieces[1].phase(1)
        resid = a.residual[...] if layer == 0 else a.resids[layer - 1]
        grad, gain_grad = norm_backward(total, resid, grad, a.norm_gain[layer : layer + 1, :])
        eighth = z.depth // 8
        for k in range(8):
            s.gain[layer, k : k + 1, :] = gain_grad[:, k * eighth : (k + 1) * eighth]
        for copy in links:
            copy.wait_send()
        if layer:
            mixed, gate = a.mixeds[layer - 1], a.gates[layer - 1]
            s.row_buf[...] = (gate * grad).astype(BF)
            tile = tile_of(-0.5 * gate * gate * jnp.sum(mixed * grad, axis=1, keepdims=True))
        for i in range(across):
            here = slice(i * share, (i + 1) * share)
            state = t_dot(s.normed[:, here], s.rs[...])
            for j in range(n):
                to = ((j * LAYERS + layer) * across + i) * padded
                s.state_part[to : to + cells, :] = state[j * cells : (j + 1) * cells, :].astype(BF)
            s.step_part[layer, i, 0:heads, :] = t_dot(s.rd[...], s.normed[:, here])
        if layer:
            loads = start_loads(layer - 1)
            for piece, k in ((pieces[0], 0), (pieces[1], 1)):
                for j in range(2, len(piece.order)):
                    piece.phase(j)
                outs.append(finish(piece, k, layer))
            older = pieces
    o.input_grad[...] = grad
    gains = exchange(s.gain, s.gain_got, s.gain_send, s.gain_recv, me, n, AXIS)
    wides = exchange(s.wide, s.wide_got, s.wide_send, s.wide_recv, me, n, AXIS)
    pieces[2].phase(1)
    links = []
    cell_rows = LAYERS * across * padded
    state = reduce_rows(
        ex, cell_rows, s.state_part, s.state_pair, s.state_stage, s.state_got,
        (s.cell_pair_send, s.cell_pair_recv, s.cell_link_send, s.cell_link_recv), lambda g: None, links,
    )
    s.gain_mid[...] = collected(s.gain[...], s.gain_got, gains)
    s.wide_mid[...] = collected(s.wide[...], s.wide_got, wides)
    gains_two = exchange(s.gain_mid, s.gain_two, s.gain_send_two, s.gain_recv_two, row, across, DATA)
    wides_two = exchange(s.wide_mid, s.wide_two, s.wide_send_two, s.wide_recv_two, row, across, DATA)
    for layer in range(LAYERS):
        for i in range(across):
            at = (layer * across + i) * padded
            s.cell_own[i, layer * padded : (layer + 1) * padded, :] = state[at : at + padded, :].astype(BF)
            s.step_own[i, layer * 16 : layer * 16 + 8, :] = s.step_part[layer, i].astype(BF)
    cell = Piece(across, s.cell_own, s.cell_stage, s.cell_got, s.cell_send, s.cell_recv)
    step = Piece(across, s.step_own, s.step_stage, s.step_got, s.step_send, s.step_recv)
    for k in range(len(cell.order)):
        cell.phase(k)
        step.phase(k)
    for layer in range(LAYERS):
        o.narrow[layer] = collected(s.narrow[layer], s.narrow_got.at[layer], narrow_copies[layer])
    o.gain[...] = collected(s.gain_mid[...], s.gain_two, gains_two)
    o.wide[...] = collected(s.wide_mid[...], s.wide_two, wides_two)
    state, steps = cell.last(), step.last()
    for layer in range(LAYERS):
        o.g_state[layer] = state[layer * padded : layer * padded + cells, :]
        o.g_step[layer] = steps[layer * 16 : layer * 16 + 8, :]
    for copy in outs:
        copy.wait()
    for k, piece in enumerate(pieces):
        for j in range(2, len(piece.order)):
            piece.phase(j)
    last = [finish(piece, k, 0) for k, piece in enumerate(pieces)]
    for copy in links + gains + wides + gains_two + wides_two + [c for copies in narrow_copies for c in copies]:
        copy.wait_send()
    for copy in last:
        copy.wait()


def padded_cells(z, n):
    cells = z.depth // (n * z.across)
    return -(-cells // 16) * 16


def piece_slots(across):
    order = [1 << b for b in range(across.bit_length() - 1)]
    return len(reduce_steps(order)), len(arrival_slots(order))


def backward_pass(ex, z, forward, residual, cotangent, meta, segrow, w):
    n, across = ex.size, z.across
    share = z.depth // across
    if share != z.inner:
        raise ValueError(share)
    saved = saved_shapes(z)
    rows = (z.rows, z.depth)
    inputs = dict(
        residual=(residual, True), cotangent=(cotangent, True), sent=(forward.sent, True), mean=(forward.mean, True),
        resids=(forward.resids, True), mixeds=(forward.mixeds, True), gates=(forward.gates, True),
        meta=(meta, True), segrow=(segrow, True), **small_inputs(w),
    )
    for k in saved:
        inputs[k] = (getattr(forward, k), False)
    cells, padded = z.depth // (n * across), padded_cells(z, n)
    narrow, wide, gain = (LAYERS, 16, z.inner), (LAYERS, 8, z.both), (LAYERS, 8, z.depth // 8)
    outputs = dict(
        input_grad=(rows, F32, True),
        g_inner=((LAYERS, 2, share, z.inner), F32, False), g_out=((LAYERS, z.inner, share), F32, False),
        g_state=((LAYERS, cells, z.both), F32, True), g_step=((LAYERS, 8, share), F32, True),
        narrow=(narrow, F32, True), wide=(wide, F32, True), gain=(gain, F32, True),
    )
    scratch = {k: pltpu.VMEM(shape, kind) for k, (shape, kind) in saved.items()}
    scratch.update(weight_scratch(z, 1))
    scratch.update(reduce_scratch(ex, z.rows, z.depth))
    slots = n // 2
    stages, arrivals = piece_slots(across)
    cell_rows = LAYERS * across * padded
    state = {"state_" + k: v for k, v in reduce_scratch(ex, cell_rows, z.both).items()}
    scratch.update(
        state_part=pltpu.VMEM((n * cell_rows, z.both), BF), **state,
        sent_all=pltpu.VMEM((z.tokens, z.depth), BF), part=pltpu.VMEM((z.tokens, z.depth), BF), row_buf=pltpu.VMEM(rows, BF),
        dy=pltpu.VMEM((z.tokens, z.inner), F32), rg=pltpu.VMEM((z.tokens, z.inner), BF), rv=pltpu.VMEM((z.tokens, z.inner), BF),
        rs=pltpu.VMEM((z.tokens, z.both), BF), rd=pltpu.VMEM((z.tokens, z.heads), BF), state=pltpu.VMEM((z.half, z.inner), F32),
        d_pre_v=pltpu.VMEM((z.tokens + 8, z.inner), F32), d_pre_s=pltpu.VMEM((z.tokens + 8, z.both), F32),
        mean_own=pltpu.VMEM((LAYERS, 8, z.rows), F32), mean_all=pltpu.VMEM((LAYERS, n, 8, z.rows), F32),
        mean_send=dma(LAYERS, n), mean_recv=dma(LAYERS, n), save_sem=dma(LAYERS, len(saved)),
        own_out=pltpu.VMEM((across, z.inner, share), BF), own_inner=pltpu.VMEM((2, across, share, z.inner), BF),
        piece_stage=pltpu.VMEM((3, stages, share, z.inner), BF), piece_got=pltpu.VMEM((LAYERS, 3, arrivals, share, z.inner), BF),
        piece_send=dma(LAYERS, 3, stages), piece_recv=dma(LAYERS, 3, arrivals),
        done=pltpu.VMEM((3, share, z.inner), F32), done_sem=dma(LAYERS, 3),
        narrow=pltpu.VMEM(narrow, F32), narrow_got=pltpu.VMEM((LAYERS, across) + narrow[1:], F32),
        narrow_send=dma(LAYERS, across), narrow_recv=dma(LAYERS, across),
        wide=pltpu.VMEM(wide, F32), wide_mid=pltpu.VMEM(wide, F32),
        wide_got=pltpu.VMEM((n,) + wide, F32), wide_two=pltpu.VMEM((across,) + wide, F32),
        gain=pltpu.VMEM(gain, F32), gain_mid=pltpu.VMEM(gain, F32),
        gain_got=pltpu.VMEM((n,) + gain, F32), gain_two=pltpu.VMEM((across,) + gain, F32),
        wide_send=dma(n), wide_recv=dma(n), gain_send=dma(n), gain_recv=dma(n),
        wide_send_two=dma(across), wide_recv_two=dma(across), gain_send_two=dma(across), gain_recv_two=dma(across),
        step_part=pltpu.VMEM((LAYERS, across, 8, share), F32), step_own=pltpu.VMEM((across, LAYERS * 16, share), BF),
        step_stage=pltpu.VMEM((stages, LAYERS * 16, share), BF), step_got=pltpu.VMEM((arrivals, LAYERS * 16, share), BF),
        step_send=dma(stages), step_recv=dma(arrivals),
        cell_own=pltpu.VMEM((across, LAYERS * padded, z.both), BF),
        cell_stage=pltpu.VMEM((stages, LAYERS * padded, z.both), BF), cell_got=pltpu.VMEM((arrivals, LAYERS * padded, z.both), BF),
        cell_send=dma(stages), cell_recv=dma(arrivals),
        cell_pair_send=dma(slots), cell_pair_recv=dma(slots), cell_link_send=dma(2 * slots), cell_link_recv=dma(2 * (slots - 1)),
        gather_send=dma(LAYERS, 2, n), gather_recv=dma(LAYERS, 2, n), pair_send=dma(LAYERS, slots), pair_recv=dma(LAYERS, slots),
        link_send=dma(LAYERS, 2 * slots), link_recv=dma(LAYERS, 2 * (slots - 1)),
    )
    return run_kernel(backward_kernel, ex, z, inputs, outputs, scratch, 1, "backward")


def sizes_of(ex, across, residual, segments, w):
    inner = w.inner_weight.shape[3]
    return Sizes(
        segments.shape[1], residual.shape[0], residual.shape[1], inner, w.step_weight.shape[2], w.state_weight.shape[2],
        w.conv_weight.shape[1], inner * ex.size, across,
    )


def shards(ex, across, residual, cotangent, segments, *weights):
    w = Weights(*weights)
    z = sizes_of(ex, across, residual, segments, w)
    w = w._replace(step_weight=jnp.transpose(w.step_weight, (0, 2, 1)))
    meta, segrow = token_meta(segments[0], SIZE)
    meta = jnp.concatenate([meta, jnp.zeros((8, 8), F32)], axis=0)
    f = forward_pass(ex, z, residual, cotangent, meta, segrow, w)
    b = backward_pass(ex, z, f, residual, cotangent, meta, segrow, w)
    taps, heads = z.taps, z.heads
    cells = z.depth // (ex.size * across)
    device = lax.axis_index(DATA) * ex.size + lax.axis_index(AXIS)
    return (
        f.block_output,
        b.input_grad,
        lax.dynamic_slice_in_dim(b.gain.reshape(LAYERS, z.depth), device * cells, cells, 1),
        b.g_inner,
        b.g_state,
        jnp.transpose(b.g_step[:, :heads], (0, 2, 1)),
        b.narrow[:, taps + 3, :heads],
        b.narrow[:, taps + 4, :heads],
        b.narrow[:, taps + 2].reshape(LAYERS, heads, -1).sum(2),
        b.narrow[:, :taps],
        b.narrow[:, taps],
        b.wide[:, :taps],
        b.wide[:, taps],
        b.narrow[:, taps + 1],
        b.g_out,
    )


def solution(mesh):
    ex = Cube(mesh.shape[AXIS])
    both, rest = (DATA, AXIS), None
    return jax.shard_map(
        functools.partial(shards, ex, mesh.shape[DATA]),
        mesh=mesh,
        in_specs=(
            P(both, rest),
            P(both, rest),
            P(DATA, rest),
            P(),
            P(rest, rest, rest, AXIS),
            P(),
            P(rest, rest, AXIS),
            P(rest, AXIS),
            P(rest, AXIS),
            P(rest, AXIS),
            P(rest, rest, AXIS),
            P(rest, AXIS),
            P(),
            P(),
            P(rest, AXIS),
            P(rest, AXIS, rest),
        ),
        out_specs=(
            P(both, rest),
            P(both, rest),
            P(rest, both),
            P(rest, rest, DATA, AXIS),
            P(rest, both, rest),
            P(rest, DATA, AXIS),
            P(rest, AXIS),
            P(rest, AXIS),
            P(rest, AXIS),
            P(rest, rest, AXIS),
            P(rest, AXIS),
            P(),
            P(),
            P(rest, AXIS),
            P(rest, AXIS, DATA),
        ),
        check_vma=False,
    )
```

```python
import functools
from types import SimpleNamespace
from typing import NamedTuple

import jax
import jax.numpy as jnp
from jax import lax
from jax.experimental import pallas as pl
from jax.experimental.pallas import tpu as pltpu
from jax.sharding import PartitionSpec as P

LAYERS = 2
SIZE = 128
CHUNKS = 2
AXIS = "tensor"
DATA = "dp"
EPS = 1e-05
HIGH = lax.Precision.HIGHEST
F32 = jnp.float32
BF = jnp.bfloat16
VM = 67_000_000


def cost_of(flops, moved=1 << 24):
    return pl.CostEstimate(flops=flops, bytes_accessed=moved, transcendentals=0)


class Weights(NamedTuple):
    norm_gain: jax.Array
    inner_weight: jax.Array
    state_weight: jax.Array
    step_weight: jax.Array
    step_bias: jax.Array
    decay_log: jax.Array
    skip_gain: jax.Array
    conv_weight: jax.Array
    conv_bias: jax.Array
    state_conv_weight: jax.Array
    state_conv_bias: jax.Array
    gate_gain: jax.Array
    out_weight: jax.Array


def dot(a, b):
    return lax.dot_general(a, b, (((1,), (0,)), ((), ())), preferred_element_type=F32)


def dot_t(a, b):
    return lax.dot_general(a, b, (((1,), (1,)), ((), ())), preferred_element_type=F32)


def t_dot(a, b):
    return lax.dot_general(a, b, (((0,), (0,)), ((), ())), preferred_element_type=F32)


def exact(a, b):
    return lax.dot_general(
        a, b, (((1,), (0,)), ((), ())), preferred_element_type=F32, precision=HIGH
    )


def sigmoid(x):
    return 1.0 / (1.0 + jnp.exp(-x))


def softplus(x):
    return jnp.maximum(x, 0.0) + jnp.log1p(jnp.exp(-jnp.abs(x)))


def tiles_of(inner, width):
    return [
        (start, min(128, inner - start), start // width, min(128, inner - start) // width)
        for start in range(0, inner, 128)
    ]


def expand(cols, inner, width):
    rows = cols.shape[0]
    parts = []
    for _, wide, first, number in tiles_of(inner, width):
        lane = lax.broadcasted_iota(jnp.int32, (rows, wide), 1)
        value = jnp.broadcast_to(cols[:, first : first + 1], (rows, wide))
        for j in range(1, number):
            value = jnp.where(lane >= j * width, cols[:, first + j : first + j + 1], value)
        parts.append(value)
    return parts[0] if len(parts) == 1 else jnp.concatenate(parts, axis=1)


def head_sum_matrix(inner, heads, width):
    row = lax.broadcasted_iota(jnp.int32, (inner, heads), 0)
    col = lax.broadcasted_iota(jnp.int32, (inner, heads), 1)
    return ((row >= col * width) & (row < (col + 1) * width)).astype(BF)


def head_sum(value, inner, heads, width, parts=1):
    ones = head_sum_matrix(inner, heads, width)
    high = value.astype(BF)
    if parts == 1:
        return dot(high, ones)
    return dot(high, ones) + dot((value - high.astype(F32)).astype(BF), ones)


def head_split(tile, width, number):
    if number == 1:
        return tile
    lane = lax.broadcasted_iota(jnp.int32, tile.shape, 1)
    zero = jnp.zeros_like(tile)
    return jnp.concatenate(
        [
            jnp.where((lane >= j * width) & (lane < (j + 1) * width), tile, zero)
            for j in range(number)
        ],
        axis=0,
    )


def pair_mask(seg_col, seg_row):
    rows, cols = seg_col.shape[0], seg_row.shape[1]
    row = lax.broadcasted_iota(jnp.int32, (rows, cols), 0)
    col = lax.broadcasted_iota(jnp.int32, (rows, cols), 1)
    return (row >= col) & (seg_col == seg_row)


def lower_ones(size):
    row = lax.broadcasted_iota(jnp.int32, (size, size), 0)
    col = lax.broadcasted_iota(jnp.int32, (size, size), 1)
    return (row >= col).astype(F32)


def turned(value):
    return jnp.transpose(value)


def column_of(tile):
    rows = tile.shape[1]
    return jnp.transpose(jnp.broadcast_to(tile[0:1, :], (rows, rows)))[:, 0:1]


def tile_of(column):
    rows = column.shape[0]
    return jnp.transpose(jnp.broadcast_to(column, (rows, rows)))[0:8, :]


def later_ones(seg_col, seg_row):
    rows, cols = seg_col.shape[0], seg_row.shape[1]
    row = lax.broadcasted_iota(jnp.int32, (rows, cols), 0)
    col = lax.broadcasted_iota(jnp.int32, (rows, cols), 1)
    return ((row <= col) & (seg_col == seg_row)).astype(F32)


def earlier_ones(seg_col, seg_row):
    rows, cols = seg_col.shape[0], seg_row.shape[1]
    row = lax.broadcasted_iota(jnp.int32, (rows, cols), 0)
    col = lax.broadcasted_iota(jnp.int32, (rows, cols), 1)
    return ((row > col) & (seg_col == seg_row)).astype(F32)


def build_meta(count, seg_ref, column, meta, segrow):
    row = seg_ref[...].astype(F32)
    segrow[0:1, :] = row
    wide = column.shape[1]
    column[0:8, :] = jnp.full((8, wide), -1.0, F32)
    for c in range(count):
        part = row[:, c * SIZE : (c + 1) * SIZE]
        column[8 + c * SIZE : 8 + (c + 1) * SIZE, :] = jnp.transpose(jnp.broadcast_to(part, (SIZE, SIZE)))
    lane = lax.broadcasted_iota(jnp.int32, (SIZE, wide), 1)
    for c in range(count):
        first = 8 + c * SIZE
        now = column[first : first + SIZE, :]
        before = column[first - 1 : first, :]
        end = column[first + SIZE - 1 : first + SIZE, :]
        value = now
        for k in range(1, 4):
            kept = (column[first - k : first - k + SIZE, :] == now).astype(F32)
            value = jnp.where(lane == k, kept, value)
        value = jnp.where(lane == 4, (now == before).astype(F32), value)
        value = jnp.where(lane == 5, (now == end).astype(F32), value)
        value = jnp.where(lane == 6, jnp.broadcast_to((end == before).astype(F32), (SIZE, wide)), value)
        meta[c * SIZE : (c + 1) * SIZE, :] = value[:, 0:8]
    meta[count * SIZE :, :] = jnp.zeros((8, 8), F32)


def span_of(dims):
    found = [0]
    for d in dims:
        found = found + [r ^ d for r in found]
    return found


def most_first(offsets):
    return sorted(offsets, key=lambda r: -bin(r).count("1"))


class Cube:
    def __init__(self, size):
        self.size = size
        self.links = [1 << b for b in range(1, size.bit_length() - 1)]
        self.orders = [self.links, self.links[::-1]]
        self.offsets = most_first(span_of(self.links))

    def gather_dims(self, q):
        return self.orders[q % 2] + [1]

    def gather_last(self, q, r):
        return max([i for i, d in enumerate(self.gather_dims(q)) if r & d], default=-1)

    def gather_steps(self, q):
        found = [r for r in span_of(self.links) if r]
        return sorted(found, key=lambda r: (self.gather_last(q, r), r & (r - 1) != 0))


def reduce_steps(order):
    steps = []
    for i, d in enumerate(order):
        for s in most_first(span_of(order[i + 1 :])):
            steps.append((i, d ^ s))
    return steps + [(len(order), 0)]


def arrival_slots(order, first=0):
    found = {}
    for i, r in reduce_steps(order):
        for j in range(i):
            found[(j, r)] = first + len(found)
    return found


def remote(src, dst, send, recv, target, axis=AXIS):
    return pltpu.make_async_remote_copy(
        src_ref=src, dst_ref=dst, send_sem=send, recv_sem=recv,
        device_id={axis: target}, device_id_type=pl.DeviceIdType.MESH,
    )


def greet(targets, across=()):
    barrier = pltpu.get_barrier_semaphore()
    for axis, group in ((AXIS, targets), (DATA, across)):
        for target in group:
            pl.semaphore_signal(barrier, inc=1, device_id={axis: target}, device_id_type=pl.DeviceIdType.MESH)
    pl.semaphore_wait(barrier, len(targets) + len(across))


def rows_of(block, rows, many=1):
    return pl.ds(pl.multiple_of(block * rows, rows), rows * many)


def dma(*shape):
    return pltpu.SemaphoreType.DMA(shape)


class Gather:
    def __init__(self, ex, rows, row_buf, out, send_sem, recv_sem):
        self.ex, self.rows, self.row_buf, self.out = ex, rows, row_buf, out
        self.send_sem, self.recv_sem = send_sem, recv_sem
        self.me = lax.axis_index(AXIS)
        self.copies, self.arrived = {}, set()

    def hops(self, q, r):
        dims, part = self.ex.gather_dims(q), self.rows // CHUNKS
        place = pl.ds(pl.multiple_of((self.me ^ r) * self.rows + q * part, part), part)
        src = self.row_buf.at[pl.ds(q * part, part), :] if r == 0 else self.out.at[place, :]
        found = []
        for i in range(self.ex.gather_last(q, r) + 1, len(dims)):
            b = r ^ dims[i]
            found.append((b, remote(src, self.out.at[place, :], self.send_sem.at[q, b], self.recv_sem.at[q, b], self.me ^ dims[i])))
        return found

    def start(self, *pieces):
        part = self.rows // CHUNKS
        hops = [self.hops(q, 0) for q in pieces]
        for step in zip(*hops):
            for q, (b, copy) in zip(pieces, step):
                copy.start()
                self.copies[(q, b)] = copy
        for q in pieces:
            here = pl.ds(pl.multiple_of(self.me * self.rows + q * part, part), part)
            self.out[here, :] = self.row_buf[q * part : (q + 1) * part, :]

    def need(self, q, r):
        if (q, r) not in self.arrived:
            self.copies[(q, r)].wait_recv()
            self.arrived.add((q, r))
            for b, copy in self.hops(q, r):
                copy.start()
                self.copies[(q, b)] = copy

    def run(self, visit):
        ex = self.ex
        steps = [ex.gather_steps(q) for q in range(CHUNKS)]
        visits = sorted(span_of(ex.links), key=lambda g: (ex.gather_last(0, g), g & (g - 1) != 0))
        k = 0
        for g in visits:
            while g and not all((q, g) in self.arrived for q in range(CHUNKS)):
                for q in range(CHUNKS):
                    self.need(q, steps[q][k])
                k += 1
            for q in range(CHUNKS):
                self.need(q, g ^ 1)
            visit(g)
        return list(self.copies.values())


def reduce_scratch(ex, rows, depth):
    slots, part = ex.size // 2, rows // CHUNKS
    return dict(
        pair=pltpu.VMEM((slots, rows, depth), BF),
        stage=pltpu.VMEM((CHUNKS * slots, part, depth), BF),
        got=pltpu.VMEM((CHUNKS * (slots - 1), part, depth), BF),
    )


def reduce_rows(*args, idle=None):
    for t, _ in enumerate(reduce_steps_of(*args)):
        if idle is not None:
            idle(t)


def reduce_steps_of(ex, rows, part, pair, stage, got, sems, produce, final, pending):
    me = lax.axis_index(AXIS)
    pair_send, pair_recv, link_send, link_recv = sems
    n, size = ex.size, rows // CHUNKS
    slot_of = {r: i for i, r in enumerate(ex.offsets)}
    orders = [ex.orders[q % 2] for q in range(CHUNKS)]
    steps = [reduce_steps(order) for order in orders]
    slots = [arrival_slots(order, q * (n // 2 - 1)) for q, order in enumerate(orders)]
    waiting = list(ex.offsets)
    pairs, ready, arrivals = {}, set(), {}

    def advance():
        r = waiting.pop(0)
        produce(r)
        i = slot_of[r]
        pairs[r] = remote(part.at[rows_of(me ^ r ^ 1, rows), :], pair.at[i], pair_send.at[i], pair_recv.at[i], me ^ 1)
        pairs[r].start()

    def step(q, k):
        i, r = steps[q][k]
        while r not in pairs:
            advance()
        if r not in ready:
            pairs[r].wait_recv()
            ready.add(r)
        own = part[pl.ds(pl.multiple_of((me ^ r) * rows + q * size, size), size), :]
        value = own.astype(F32) + pair[slot_of[r], pl.ds(q * size, size), :].astype(F32)
        for j in range(i):
            arrivals[(q, j, r)].wait_recv()
            value = value + got[slots[q][(j, r)]].astype(F32)
        if r == 0:
            final(q, value)
            return
        d = orders[q][i]
        s = q * (n // 2) + slot_of[r]
        stage[s] = value.astype(BF)
        at = slots[q][(i, r ^ d)]
        copy = remote(stage.at[s], got.at[at], link_send.at[s], link_recv.at[at], me ^ d)
        copy.start()
        arrivals[(q, i, r ^ d)] = copy
        pending.append(copy)

    advance()
    waves = CHUNKS // 2
    for t in range(len(steps[0]) + waves - 1):
        if waiting:
            advance()
        for p in range(waves):
            if 0 <= t - p < len(steps[0]):
                step(2 * p, t - p)
                step(2 * p + 1, t - p)
        if t + 1 == len(steps[0]) + waves - 1:
            pending.extend(pairs.values())
        yield t


def row_scale_of(resid):
    return lax.rsqrt(jnp.mean(resid * resid, axis=1, keepdims=True) + EPS)


def group_rows(ex, g, rows):
    me = lax.axis_index(AXIS)
    return pl.ds(pl.multiple_of(((me ^ g) // 2) * (2 * rows), 2 * rows), 2 * rows)


class Sizes(NamedTuple):
    tokens: int
    rows: int
    depth: int
    inner: int
    heads: int
    both: int
    taps: int
    inner_all: int
    across: int

    @property
    def width(self):
        return self.inner // self.heads

    @property
    def half(self):
        return self.both // 2

    @property
    def count(self):
        return self.tokens // SIZE


def weight_scratch(z, layers):
    return dict(
        win=pltpu.VMEM((layers, 2, z.depth, z.inner), BF),
        wst=pltpu.VMEM((layers, z.depth, z.both), BF),
        wstep=pltpu.VMEM((layers, z.heads, z.depth), F32),
        wout=pltpu.VMEM((layers, z.inner, z.depth), BF),
        weight_sem=dma(LAYERS, 3),
    )


def step_rows(z, a, s, layer, slot):
    for h in range(z.heads):
        s.wstep[slot, h : h + 1, :] = a.step_weight[h, layer : layer + 1, :].astype(F32)


def meta_scratch(z):
    return dict(
        column=pltpu.VMEM((z.tokens + 8, SIZE), F32), meta=pltpu.VMEM((z.tokens + 8, 8), F32), segrow=pltpu.VMEM((8, z.tokens), F32)
    )


def weight_loads(s, a, layer, slot):
    return [
        pltpu.make_async_copy(src.at[layer], dst.at[slot], s.weight_sem.at[layer, i])
        for i, (src, dst) in enumerate(
            ((a.inner_weight, s.win), (a.state_weight, s.wst), (a.out_weight, s.wout))
        )
    ]


def saved_shapes(z):
    t, i = z.tokens, z.inner
    return dict(
        normed=((t, z.depth), BF), gate=((t, i), F32), pre_v=((t, i), F32), y=((t, i), F32), pre_s=((t, z.both), F32),
        step_in=((t, z.heads), F32), value=((t, i), BF), raw=((t, z.both), BF), scaled=((t, i), BF),
        entering=((z.count, z.half, i), BF),
    )


def mix_forward(z, layer, s, a, meta, segrow):
    at = slice(layer, layer + 1)
    inner, width, half = z.inner, z.width, z.half
    s.state[...] = jnp.zeros_like(s.state)
    group = 2 if z.count % 2 == 0 else 1

    def chunk(c, before):
        rows = pl.ds(pl.multiple_of(c * SIZE, SIZE), SIZE)
        window = pl.ds(pl.multiple_of(c * SIZE, SIZE), SIZE + 8)
        m = meta[rows, :]

        def conv(buf, w_ref, b_ref):
            win = buf[window, :]
            total = b_ref[at, :] + w_ref[layer, 0:1, :] * win[8:, :]
            for k in range(1, z.taps):
                total = total + w_ref[layer, k : k + 1, :] * (win[8 - k : 8 - k + SIZE, :] * m[:, k : k + 1])
            return total, win[8:, :]

        pre_v, value = conv(s.vbuf, a.conv_weight, a.conv_bias)
        pre_s, raw = conv(s.sbuf, a.state_conv_weight, a.state_conv_bias)
        s.value[rows, :] = value.astype(BF)
        s.raw[rows, :] = raw.astype(BF)
        s.pre_v[rows, :] = pre_v
        s.pre_s[rows, :] = pre_s
        x = pre_v * sigmoid(pre_v)
        st = pre_s * sigmoid(pre_s)
        b_mat = st[:, :half].astype(BF)
        c_mat = st[:, half:].astype(BF)
        dt = softplus(s.step_in[rows, :] + a.step_bias[at, :])
        log_decay = -dt * jnp.exp(a.decay_log[at, :])
        cum = exact(lower_ones(SIZE), log_decay)
        cum_t = turned(cum)
        last = cum[SIZE - 1 : SIZE, :]
        xt = (x * expand(dt, inner, width)).astype(BF)
        from_state = jnp.exp(cum) * m[:, 4:5]
        to_end = jnp.exp(last - cum) * m[:, 5:6]
        carry = jnp.exp(last) * m[0:1, 6:7]
        before_b = before.astype(BF)
        s.entering[c] = before_b
        scores = dot_t(c_mat, b_mat)
        mask = pair_mask(m[:, 0:1], segrow[0:1, rows])
        parts = []
        for start, wide, first, number in tiles_of(inner, width):
            mats = []
            for h in range(first, first + number):
                differ = cum[:, h : h + 1] - cum_t[h : h + 1, :]
                mats.append((jnp.exp(jnp.where(mask, differ, -1e30)) * scores).astype(BF))
            left = mats[0] if number == 1 else jnp.concatenate(mats, axis=1)
            parts.append(dot(left, head_split(xt[:, start : start + wide], width, number)))
        intra = parts[0] if len(parts) == 1 else jnp.concatenate(parts, axis=1)
        inter = dot(c_mat, before_b) * expand(from_state, inner, width)
        y = intra + inter + expand(a.skip_gain[at, :], inner, width) * x
        s.y[rows, :] = y
        ended = (xt.astype(F32) * expand(to_end, inner, width)).astype(BF)
        after = expand(carry, inner, width) * before + t_dot(b_mat, ended)
        gate = s.gate[rows, :]
        gated = y * (gate * sigmoid(gate))
        square = jnp.sum(gated * gated, axis=1, keepdims=True)
        tile = tile_of(square)
        per = SIZE // z.rows if SIZE > z.rows else 1
        wide = SIZE // per
        for k in range(per):
            s.squares[c * per + k] = tile[:, k * wide : (k + 1) * wide]
        s.scaled[rows, :] = (gated * a.gate_gain[at, :]).astype(BF)
        return after

    def body(i, carry):
        before = s.state[...]
        for k in range(group):
            before = chunk(i * group + k, before)
        s.state[...] = before
        return carry

    lax.fori_loop(0, z.count // group, body, 0)


def forward_kernel(ex, z, names_in, names_out, names_scratch, *refs):
    count_in, count_out = len(names_in), len(names_out)
    a = SimpleNamespace(**dict(zip(names_in, refs)))
    o = SimpleNamespace(**dict(zip(names_out, refs[count_in:])))
    s = SimpleNamespace(**dict(zip(names_scratch, refs[count_in + count_out :])))
    me = lax.axis_index(AXIS)
    n = ex.size
    greet([me ^ r for r in range(1, n)])
    loads = [weight_loads(s, a, layer, layer) for layer in range(LAYERS)]
    for copy in loads[0] + loads[1]:
        copy.start()
    s.vbuf[0:8, :] = jnp.zeros((8, z.inner), F32)
    s.sbuf[0:8, :] = jnp.zeros((8, z.both), F32)
    saves = []
    size = z.rows // CHUNKS
    gathers = [
        Gather(ex, z.rows, s.row_buf, s.normed.at[layer], s.gather_send.at[layer], s.gather_recv.at[layer]) for layer in range(LAYERS)
    ]
    hidden = a.residual[...]
    s.hidden[...] = hidden
    s.row_buf[...] = (hidden * row_scale_of(hidden) * a.norm_gain[0:1, :]).astype(BF)
    gathers[0].start(*range(CHUNKS))
    build_meta(z.count, a.segments, s.column, s.meta, s.segrow)
    for layer in range(LAYERS):
        step_rows(z, a, s, layer, layer)
    means = []
    for layer in range(LAYERS):
        normed = s.normed.at[layer]

        def project(g, layer=layer, normed=normed):
            if g == 0:
                for copy in loads[layer]:
                    copy.wait()
            here = group_rows(ex, g, z.rows)
            beyond = pl.ds(pl.multiple_of(((me ^ g) // 2) * (2 * z.rows) + 8, 8), 2 * z.rows)
            nb = normed[here, :]
            s.gate[here, :] = dot(nb, s.win[layer, 0])
            s.vbuf[beyond, :] = dot(nb, s.win[layer, 1])
            s.sbuf[beyond, :] = dot(nb, s.wst[layer])
            s.step_in[here, :] = dot_t(nb, s.wstep[layer].astype(BF))

        sent = gathers[layer].run(project)
        mix_forward(z, layer, s, a, s.meta, s.segrow)
        for i, name in enumerate(names_out[: len(saved_shapes(z))]):
            src = normed if i == 0 else getattr(s, name)
            saves.append(pltpu.make_async_copy(src, getattr(o, name).at[layer], s.save_sem.at[layer, i]))
            saves[-1].start()
        for copy in sent:
            copy.wait_send()

        def produce(g, layer=layer):
            here = group_rows(ex, g, z.rows)
            s.part[here, :] = dot(s.scaled[here, :], s.wout[layer]).astype(BF)

        squares = []
        for r in range(1, n):
            squares.append(
                remote(s.squares.at[me ^ r], s.square_got.at[layer, r], s.square_send.at[layer, r], s.square_recv.at[layer, r], me ^ r)
            )
            squares[-1].start()
        gates = []

        def final(q, value, layer=layer, squares=squares, gates=gates):
            if not gates:
                square = s.squares[me]
                for r, copy in enumerate(squares, 1):
                    copy.wait_recv()
                    square = square + s.square_got[layer, r]
                gates.append(lax.rsqrt(column_of(square) / z.inner_all + EPS))
                if layer + 1 < LAYERS:
                    o.gates[layer] = gates[0]
            rows = slice(q * size, (q + 1) * size)
            gate = gates[0][rows, :]
            mixed = gate * value
            hidden = s.hidden[rows, :] + mixed
            if layer + 1 < LAYERS:
                s.row_buf[rows, :] = (hidden * row_scale_of(hidden) * a.norm_gain[layer + 1 : layer + 2, :]).astype(BF)
                gathers[layer + 1].start(q)
                s.hidden[rows, :] = hidden
                o.resids[layer, rows, :] = hidden
                o.mixeds[layer, rows, :] = mixed
            else:
                grad = a.cotangent[rows, :]
                o.block_output[rows, :] = hidden
                o.sent[rows, :] = (gate * grad).astype(BF)
                means.append((q, -0.5 * gate * gate * jnp.sum(mixed * grad, axis=1, keepdims=True)))

        links = []
        reduce_rows(
            ex, z.rows, s.part, s.pair, s.stage, s.got,
            (s.pair_send.at[layer], s.pair_recv.at[layer], s.link_send.at[layer], s.link_recv.at[layer]), produce, final, links,
        )
        for copy in links + squares:
            copy.wait_send()
        for copy in saves:
            copy.wait()
        saves = []
    o.mean[...] = tile_of(jnp.concatenate([v for _, v in sorted(means, key=lambda m: m[0])], axis=0))


def run_kernel(kernel, ex, z, inputs, outputs, scratch, collective, name):
    vm, anywhere = pl.BlockSpec(memory_space=pltpu.VMEM), pl.BlockSpec(memory_space=pl.ANY)
    made = pl.pallas_call(
        functools.partial(kernel, ex, z, tuple(inputs), tuple(outputs), tuple(scratch)),
        out_shape=tuple(jax.ShapeDtypeStruct(shape, kind) for shape, kind, _ in outputs.values()),
        in_specs=[vm if inside else anywhere for _, inside in inputs.values()],
        out_specs=tuple(vm if inside else anywhere for _, _, inside in outputs.values()),
        scratch_shapes=list(scratch.values()),
        compiler_params=pltpu.CompilerParams(collective_id=collective, has_side_effects=True, vmem_limit_bytes=VM),
        cost_estimate=cost_of(1 << 35),
        name=name,
    )(*[array for array, _ in inputs.values()])
    return SimpleNamespace(**dict(zip(outputs, made)))


def small_inputs(w):
    return dict(
        norm_gain=(w.norm_gain, True), step_bias=(w.step_bias, True), decay_log=(w.decay_log, True),
        skip_gain=(w.skip_gain, True), conv_weight=(w.conv_weight, True), conv_bias=(w.conv_bias, True),
        state_conv_weight=(w.state_conv_weight, True), state_conv_bias=(w.state_conv_bias, True), gate_gain=(w.gate_gain, True),
        inner_weight=(w.inner_weight, False), state_weight=(w.state_weight, False), step_weight=(w.step_weight, True),
        out_weight=(w.out_weight, False),
    )


def forward_pass(ex, z, residual, cotangent, segments, w):
    n = ex.size
    saved = saved_shapes(z)
    inputs = dict(residual=(residual, True), cotangent=(cotangent, True), segments=(segments, True), **small_inputs(w))
    rows = (z.rows, z.depth)
    outputs = {k: ((LAYERS,) + shape, kind, False) for k, (shape, kind) in saved.items()}
    outputs.update(
        resids=((LAYERS - 1,) + rows, F32, True), mixeds=((LAYERS - 1,) + rows, F32, True),
        gates=((LAYERS - 1, z.rows, 1), F32, True), block_output=(rows, F32, True),
        sent=(rows, BF, True), mean=((8, z.rows), F32, True),
    )
    scratch = {k: pltpu.VMEM(shape, kind) for k, (shape, kind) in saved.items()}
    scratch.update(normed=pltpu.VMEM((LAYERS, z.tokens, z.depth), BF))
    scratch.update(weight_scratch(z, LAYERS))
    scratch.update(meta_scratch(z))
    scratch.update(reduce_scratch(ex, z.rows, z.depth))
    slots = n // 2
    scratch.update(
        vbuf=pltpu.VMEM((z.tokens + 8, z.inner), F32), sbuf=pltpu.VMEM((z.tokens + 8, z.both), F32),
        state=pltpu.VMEM((z.half, z.inner), F32), part=pltpu.VMEM((z.tokens, z.depth), BF), row_buf=pltpu.VMEM(rows, BF),
        squares=pltpu.VMEM((n, 8, z.rows), F32), square_got=pltpu.VMEM((LAYERS, n, 8, z.rows), F32),
        square_send=dma(LAYERS, n), square_recv=dma(LAYERS, n), save_sem=dma(LAYERS, len(saved)),
        gather_send=dma(LAYERS, CHUNKS, n), gather_recv=dma(LAYERS, CHUNKS, n),
        pair_send=dma(LAYERS, slots), pair_recv=dma(LAYERS, slots), hidden=pltpu.VMEM(rows, F32),
        link_send=dma(LAYERS, CHUNKS * slots), link_recv=dma(LAYERS, CHUNKS * (slots - 1)),
    )
    return run_kernel(forward_kernel, ex, z, inputs, outputs, scratch, 0, "forward")


class Piece:
    def __init__(self, across, own, stage, got, send, recv):
        self.order = [1 << b for b in range(across.bit_length() - 1)]
        self.own, self.stage, self.got, self.send, self.recv = own, stage, got, send, recv
        self.slots = arrival_slots(self.order)
        self.row = lax.axis_index(DATA)
        self.arrivals, self.sent = {}, []

    def value(self, i, r):
        total = self.own[self.row ^ r].astype(F32)
        for j in range(i):
            self.arrivals[(j, r)].wait_recv()
            total = total + self.got[self.slots[(j, r)]].astype(F32)
        return total

    def phase(self, k):
        for number, (i, r) in enumerate(reduce_steps(self.order)):
            if i != k or r == 0:
                continue
            src = self.own.at[self.row ^ r]
            if i:
                self.stage[number] = self.value(i, r).astype(BF)
                src = self.stage.at[number]
            d = self.order[i]
            at = self.slots[(i, r ^ d)]
            copy = remote(src, self.got.at[at], self.send.at[number], self.recv.at[at], self.row ^ d, DATA)
            copy.start()
            self.arrivals[(i, r ^ d)] = copy
            self.sent.append(copy)

    def last(self):
        total = self.value(len(self.order), 0)
        for copy in self.sent:
            copy.wait_send()
        return total


def mix_backward(z, layer, s, a, meta, segrow):
    at = slice(layer, layer + 1)
    inner, width, half, heads, taps = z.inner, z.width, z.half, z.heads, z.taps
    s.state[...] = jnp.zeros_like(s.state)
    group = 2 if z.count % 2 == 0 else 1

    def chunk(c, after):
        rows = pl.ds(pl.multiple_of(c * SIZE, SIZE), SIZE)
        m = meta[rows, :]
        y, dy = s.y[rows, :], s.dy[rows, :]
        pre_v, pre_s = s.pre_v[rows, :], s.pre_s[rows, :]
        sig_v, sig_s = sigmoid(pre_v), sigmoid(pre_s)
        x = pre_v * sig_v
        st = pre_s * sig_s
        b_mat = st[:, :half].astype(BF)
        c_mat = st[:, half:].astype(BF)
        raw_step = s.step_in[rows, :] + a.step_bias[at, :]
        dt = softplus(raw_step)
        rate = jnp.exp(a.decay_log[at, :])
        log_decay = -dt * rate
        cum = exact(lower_ones(SIZE), log_decay)
        cum_t = turned(cum)
        last = cum[SIZE - 1 : SIZE, :]
        dt_all = expand(dt, inner, width)
        skip_all = expand(a.skip_gain[at, :], inner, width)
        xt = (x * dt_all).astype(BF)
        dy_b = dy.astype(BF)
        from_state = expand(jnp.exp(cum) * m[:, 4:5], inner, width)
        to_end = expand(jnp.exp(last - cum) * m[:, 5:6], inner, width)
        carry = expand(jnp.exp(last) * m[0:1, 6:7], inner, width)
        scores = dot_t(c_mat, b_mat)
        mask = pair_mask(m[:, 0:1], segrow[0:1, rows])
        d_scores = jnp.zeros((SIZE, SIZE), F32)
        parts = []
        for start, wide, first, number in tiles_of(inner, width):
            dy_split = head_split(dy_b[:, start : start + wide], width, number)
            d_mats = dot_t(dy_split, xt[:, start : start + wide])
            mats = []
            for j in range(number):
                h = first + j
                differ = cum[:, h : h + 1] - cum_t[h : h + 1, :]
                decay = jnp.exp(jnp.where(mask, differ, -1e30))
                mats.append((decay * scores).astype(BF))
                d_scores = d_scores + d_mats[j * SIZE : (j + 1) * SIZE, :] * decay
            left = mats[0] if number == 1 else jnp.concatenate(mats, axis=0)
            parts.append(t_dot(left, dy_split))
        intra = parts[0] if len(parts) == 1 else jnp.concatenate(parts, axis=1)
        d_scores = d_scores.astype(BF)
        before = s.entering[c]
        after_b = after.astype(BF)
        dy_in = (dy * from_state).astype(BF)
        xt_f = xt.astype(F32)
        ended = (xt_f * to_end).astype(BF)
        from_later = dot(b_mat, after_b) * to_end
        d_xt = intra + from_later
        d_c = dot(d_scores, b_mat) + dot_t(dy_in, before)
        d_b = t_dot(d_scores, c_mat) + dot_t(ended, after_b)
        across = carry * jnp.sum(before.astype(F32) * after, axis=0, keepdims=True)
        fresh = carry * after + t_dot(c_mat, dy_in)
        pairs = head_sum(dy_b.astype(F32) * (y - skip_all * x) - xt_f * intra, inner, heads, width, 2)
        sums = head_sum(
            jnp.concatenate([xt_f * from_later, x * d_xt, jnp.broadcast_to(across, (8, inner))], axis=0), inner, heads, width
        )
        seg_col, seg_row = m[:, 0:1], segrow[0:1, rows]
        d_log = (
            exact(later_ones(seg_col, seg_row), pairs)
            + exact(earlier_ones(seg_col, seg_row), sums[0:SIZE])
            + sums[2 * SIZE : 2 * SIZE + 1]
        )
        d_raw = (sums[SIZE : 2 * SIZE] - rate * d_log) * sigmoid(raw_step)
        s.rd[rows, :] = d_raw.astype(BF)
        d_x = dy * skip_all + d_xt * dt_all
        s.d_pre_v[rows, :] = d_x * (sig_v * (1.0 + pre_v * (1.0 - sig_v)))
        d_st = jnp.concatenate([d_b, d_c], axis=1)
        s.d_pre_s[rows, :] = d_st * (sig_s * (1.0 + pre_s * (1.0 - sig_s)))
        total = lambda v: jnp.sum(v, axis=0, keepdims=True)
        return fresh, (total(dy * x), total(d_raw), total(d_log * log_decay))

    def body(i, sums):
        after = s.state[...]
        for k in range(group):
            after, more = chunk(z.count - 1 - (i * group + k), after)
            sums = tuple(u + v for u, v in zip(sums, more))
        s.state[...] = after
        return sums

    zero = lambda wide: jnp.zeros((1, wide), F32)
    skip, bias, decay = lax.fori_loop(0, z.count // group, body, (zero(inner), zero(heads), zero(heads)))
    s.narrow[layer, taps + 2 : taps + 3, :] = skip
    s.narrow[layer, taps + 3 : taps + 4, 0:heads] = bias
    s.narrow[layer, taps + 4 : taps + 5, 0:heads] = decay

    def conv_body(c, sums):
        rows = pl.ds(pl.multiple_of(c * SIZE, SIZE), SIZE)
        window = pl.ds(pl.multiple_of(c * SIZE, SIZE), SIZE + 8)
        m = meta[window, :]
        more = []
        for src, w_ref, value_ref, dst in ((s.d_pre_v, a.conv_weight, s.value, s.rv), (s.d_pre_s, a.state_conv_weight, s.raw, s.rs)):
            win = src[window, :]
            value = value_ref[rows, :].astype(F32)
            now = win[0:SIZE, :]
            total = w_ref[layer, 0:1, :] * now
            lines = [jnp.sum(now * value, axis=0, keepdims=True)]
            for k in range(1, taps):
                moved = win[k : k + SIZE, :] * m[k : k + SIZE, k : k + 1]
                total = total + w_ref[layer, k : k + 1, :] * moved
                lines.append(jnp.sum(moved * value, axis=0, keepdims=True))
            lines.append(jnp.sum(now, axis=0, keepdims=True))
            dst[rows, :] = total.astype(BF)
            more.extend(lines)
        return tuple(u + v for u, v in zip(sums, more))

    lines = lax.fori_loop(0, z.count, conv_body, (zero(inner),) * (taps + 1) + (zero(z.both),) * (taps + 1))
    for k in range(taps + 1):
        s.narrow[layer, k : k + 1, :] = lines[k]
        s.wide[layer, k : k + 1, :] = lines[taps + 1 + k]


def norm_backward(total, resid, grad, gain):
    scale = row_scale_of(resid)
    weighted = total * gain
    inner = jnp.sum(weighted * resid, axis=1, keepdims=True)
    gain_grad = jnp.sum(total * resid * scale, axis=0, keepdims=True)
    return grad + scale * weighted - resid * (scale * scale * scale * inner / resid.shape[1]), gain_grad


def exchange(src, got, send, recv, place, number, axis):
    copies = [remote(src, got.at[r], send.at[r], recv.at[r], place ^ r, axis) for r in range(1, number)]
    for copy in copies:
        copy.start()
    return copies


def collected(own, got, copies):
    total = own
    for r, copy in enumerate(copies, 1):
        copy.wait_recv()
        total = total + got[r]
    return total


def backward_kernel(ex, z, names_in, names_out, names_scratch, *refs):
    count_in, count_out = len(names_in), len(names_out)
    a = SimpleNamespace(**dict(zip(names_in, refs)))
    o = SimpleNamespace(**dict(zip(names_out, refs[count_in:])))
    s = SimpleNamespace(**dict(zip(names_scratch, refs[count_in + count_out :])))
    me, row = lax.axis_index(AXIS), lax.axis_index(DATA)
    n, across, taps, heads = ex.size, z.across, z.taps, z.heads
    share = z.depth // across
    cells = z.depth // (n * across)
    padded = padded_cells(z, n)
    greet([me ^ r for r in range(1, n)], [row ^ r for r in range(1, across)])
    saved = list(saved_shapes(z))

    def start_loads(layer, late):
        found = weight_loads(s, a, layer, 0) if late else []
        for i, k in enumerate(saved):
            if late == (i == 0):
                found.append(pltpu.make_async_copy(getattr(a, k).at[layer], getattr(s, k), s.save_sem.at[layer, i]))
        for copy in found:
            copy.start()
        return found

    loads = start_loads(LAYERS - 1, False) + start_loads(LAYERS - 1, True)
    size = z.rows // CHUNKS
    s.row_buf[...] = a.sent[...]
    s.grad[...] = a.cotangent[...]
    gather = Gather(ex, z.rows, s.row_buf, s.sent_all, s.gather_send.at[LAYERS - 1], s.gather_recv.at[LAYERS - 1])
    gather.start(*range(CHUNKS))
    tile = a.mean[...]
    for ref in (s.narrow, s.wide, s.gain):
        ref[...] = jnp.zeros_like(ref)
    s.d_pre_v[z.tokens :, :] = jnp.zeros((8, z.inner), F32)
    s.d_pre_s[z.tokens :, :] = jnp.zeros((8, z.both), F32)
    if padded != cells:
        s.state_part[...] = jnp.zeros_like(s.state_part)
    narrow_copies, outs, older = [None] * LAYERS, [], None

    def finish(piece, k, layer):
        s.done[k] = piece.last()
        target = o.g_out.at[layer] if k == 0 else o.g_inner.at[layer, k - 1]
        copy = pltpu.make_async_copy(s.done.at[k], target, s.done_sem.at[layer, k])
        copy.start()
        return copy

    cell_links, cell_sums = [], {}
    cell_rows = LAYERS * across * padded
    state_steps = reduce_steps_of(
        ex, cell_rows, s.state_part, s.state_pair, s.state_stage, s.state_got,
        (s.cell_pair_send, s.cell_pair_recv, s.cell_link_send, s.cell_link_recv), lambda g: None, cell_sums.__setitem__, cell_links,
    )
    for layer in range(LAYERS - 1, -1, -1):
        s.mean_own[layer] = tile
        means = []
        for r in range(1, n):
            means.append(
                remote(s.mean_own.at[layer], s.mean_all.at[layer, me], s.mean_send.at[layer, r], s.mean_recv.at[layer, r], me ^ r)
            )
            means[-1].start()
        s.mean_all[layer, me] = tile
        step_rows(z, a, s, layer, 0)
        if layer + 1 == LAYERS:
            build_meta(z.count, a.segments, s.column, s.meta, s.segrow)

        def visit(g, layer=layer, means=means, loads=loads):
            if g == 0:
                for copy in loads:
                    copy.wait()
            here = group_rows(ex, g, z.rows)
            first = (me ^ g) // 2 * 2
            for r in (g, g ^ 1):
                if r:
                    means[r - 1].wait_recv()
            mean = jnp.concatenate([column_of(s.mean_all[layer, first]), column_of(s.mean_all[layer, first + 1])], axis=0)
            at = slice(layer, layer + 1)
            grad_scaled = dot_t(s.sent_all[here, :], s.wout[0])
            gate, y = s.gate[here, :], s.y[here, :]
            gate_sig = sigmoid(gate)
            silu_gate = gate * gate_sig
            gated = y * silu_gate
            s.narrow[layer, taps + 1 : taps + 2, :] += jnp.sum(grad_scaled * gated, axis=0, keepdims=True)
            grad_gated = grad_scaled * a.gate_gain[at, :] + (2.0 / z.inner_all) * mean * gated
            s.rg[here, :] = (grad_gated * y * (gate_sig * (1.0 + gate * (1.0 - gate_sig)))).astype(BF)
            s.dy[here, :] = grad_gated * silu_gate

        sent = gather.run(visit)
        pieces = [
            Piece(
                across, own, s.piece_stage.at[k], s.piece_got.at[layer, k], s.piece_send.at[layer, k], s.piece_recv.at[layer, k]
            )
            for k, own in enumerate((s.own_out, s.own_inner.at[0], s.own_inner.at[1]))
        ]
        if older is not None:
            older[2].phase(1)
            for k in range(2):
                for j in range(2, len(older[k].order)):
                    older[k].phase(j)
                outs.append(finish(older[k], k, layer + 1))
        for i in range(across):
            s.own_out[i] = t_dot(s.scaled[...], s.sent_all[:, i * share : (i + 1) * share]).astype(BF)
        pieces[0].phase(0)
        for i in range(across):
            s.own_inner[0, i] = t_dot(s.normed[:, i * share : (i + 1) * share], s.rg[...]).astype(BF)
        pieces[1].phase(0)
        mix_backward(z, layer, s, a, s.meta, s.segrow)
        for copy in sent + means:
            copy.wait_send()
        loads = start_loads(layer - 1, False) if layer else []
        if older is not None:
            for k in range(2, len(older[2].order)):
                older[2].phase(k)
            outs.append(finish(older[2], 2, layer + 1))
        pieces[0].phase(1)
        narrow_copies[layer] = exchange(
            s.narrow.at[layer], s.narrow_got.at[layer], s.narrow_send.at[layer], s.narrow_recv.at[layer], row, across, DATA
        )

        def value_grads(pieces=pieces):
            for i in range(across):
                s.own_inner[1, i] = t_dot(s.normed[:, i * share : (i + 1) * share], s.rv[...]).astype(BF)
            pieces[2].phase(0)

        def state_grads(layer=layer):
            for i in range(across):
                here = slice(i * share, (i + 1) * share)
                state = t_dot(s.normed[:, here], s.rs[...])
                for j in range(n):
                    to = ((j * LAYERS + layer) * across + i) * padded
                    s.state_part[to : to + cells, :] = state[j * cells : (j + 1) * cells, :].astype(BF)
                s.step_part[layer, i, 0:heads, :] = t_dot(s.rd[...], s.normed[:, here])

        if layer == 0:
            value_grads()

        def idle(t, layer=layer, pieces=pieces, value_grads=value_grads, state_grads=state_grads):
            if t == 1:
                if layer:
                    value_grads()
                else:
                    state_grads()
            elif t == 2 and layer:
                state_grads()
            elif t == 3:
                pieces[1].phase(1)
            if t >= 2 and not layer:
                next(state_steps)

        def produce(g, layer=layer):
            here = group_rows(ex, g, z.rows)
            total = dot_t(s.rg[here, :], s.win[0, 0]) + dot_t(s.rv[here, :], s.win[0, 1])
            total = total + dot_t(s.rs[here, :], s.wst[0]) + dot(s.rd[here, :], s.wstep[0].astype(BF))
            s.part[here, :] = total.astype(BF)

        after = Gather(ex, z.rows, s.row_buf, s.sent_all, s.gather_send.at[layer - 1], s.gather_recv.at[layer - 1]) if layer else None
        found = []

        def final(q, value, layer=layer, after=after, found=found):
            rows = slice(q * size, (q + 1) * size)
            resid = a.resids[layer - 1, rows, :] if layer else a.residual[rows, :]
            fresh, gain_grad = norm_backward(value, resid, s.grad[rows, :], a.norm_gain[layer : layer + 1, :])
            mean = None
            if layer:
                mixed, gate = a.mixeds[layer - 1, rows, :], a.gates[layer - 1, rows, :]
                s.row_buf[rows, :] = (gate * fresh).astype(BF)
                after.start(q)
                s.grad[rows, :] = fresh
                mean = -0.5 * gate * gate * jnp.sum(mixed * fresh, axis=1, keepdims=True)
            else:
                o.input_grad[rows, :] = fresh
            found.append((q, gain_grad, mean))

        links = []
        reduce_rows(
            ex, z.rows, s.part, s.pair, s.stage, s.got,
            (s.pair_send.at[layer], s.pair_recv.at[layer], s.link_send.at[layer], s.link_recv.at[layer]), produce, final, links, idle=idle,
        )
        found.sort(key=lambda item: item[0])
        gain_grad = sum(item[1] for item in found)
        eighth = z.depth // 8
        for k in range(8):
            s.gain[layer, k : k + 1, :] = gain_grad[:, k * eighth : (k + 1) * eighth]
        for copy in links:
            copy.wait_send()
        if layer:
            tile = tile_of(jnp.concatenate([item[2] for item in found], axis=0))
            loads = loads + start_loads(layer - 1, True)
            gather = after
            older = pieces
    gains = exchange(s.gain, s.gain_got, s.gain_send, s.gain_recv, me, n, AXIS)
    wides = exchange(s.wide, s.wide_got, s.wide_send, s.wide_recv, me, n, AXIS)
    for _ in state_steps:
        pass
    state = jnp.concatenate([cell_sums[q] for q in range(CHUNKS)], axis=0)
    s.gain_mid[...] = collected(s.gain[...], s.gain_got, gains)
    s.wide_mid[...] = collected(s.wide[...], s.wide_got, wides)
    gains_two = exchange(s.gain_mid, s.gain_two, s.gain_send_two, s.gain_recv_two, row, across, DATA)
    wides_two = exchange(s.wide_mid, s.wide_two, s.wide_send_two, s.wide_recv_two, row, across, DATA)
    for layer in range(LAYERS):
        for i in range(across):
            at = (layer * across + i) * padded
            s.cell_own[i, layer * padded : (layer + 1) * padded, :] = state[at : at + padded, :].astype(BF)
            s.step_own[i, layer * 16 : layer * 16 + 8, :] = s.step_part[layer, i].astype(BF)
    pieces[2].phase(1)
    cell = Piece(across, s.cell_own, s.cell_stage, s.cell_got, s.cell_send, s.cell_recv)
    step = Piece(across, s.step_own, s.step_stage, s.step_got, s.step_send, s.step_recv)
    for k in range(len(cell.order)):
        cell.phase(k)
        step.phase(k)
    for layer in range(LAYERS):
        o.narrow[layer] = collected(s.narrow[layer], s.narrow_got.at[layer], narrow_copies[layer])
    o.gain[...] = collected(s.gain_mid[...], s.gain_two, gains_two)
    o.wide[...] = collected(s.wide_mid[...], s.wide_two, wides_two)
    state, steps = cell.last(), step.last()
    for layer in range(LAYERS):
        o.g_state[layer] = state[layer * padded : layer * padded + cells, :]
        o.g_step[layer] = steps[layer * 16 : layer * 16 + 8, :]
    for copy in outs:
        copy.wait()
    for k, piece in enumerate(pieces):
        for j in range(2, len(piece.order)):
            piece.phase(j)
    last = [finish(piece, k, 0) for k, piece in enumerate(pieces)]
    for copy in cell_links + gains + wides + gains_two + wides_two + [c for copies in narrow_copies for c in copies]:
        copy.wait_send()
    for copy in last:
        copy.wait()


def padded_cells(z, n):
    cells = z.depth // (n * z.across)
    return -(-cells // 16) * 16


def piece_slots(across):
    order = [1 << b for b in range(across.bit_length() - 1)]
    return len(reduce_steps(order)), len(arrival_slots(order))


def backward_pass(ex, z, forward, residual, cotangent, segments, w):
    n, across = ex.size, z.across
    share = z.depth // across
    if share != z.inner:
        raise ValueError(share)
    saved = saved_shapes(z)
    rows = (z.rows, z.depth)
    inputs = dict(
        residual=(residual, True), cotangent=(cotangent, True), sent=(forward.sent, True), mean=(forward.mean, True),
        resids=(forward.resids, True), mixeds=(forward.mixeds, True), gates=(forward.gates, True),
        segments=(segments, True), **small_inputs(w),
    )
    for k in saved:
        inputs[k] = (getattr(forward, k), False)
    cells, padded = z.depth // (n * across), padded_cells(z, n)
    narrow, wide, gain = (LAYERS, 16, z.inner), (LAYERS, 8, z.both), (LAYERS, 8, z.depth // 8)
    outputs = dict(
        input_grad=(rows, F32, True),
        g_inner=((LAYERS, 2, share, z.inner), F32, False), g_out=((LAYERS, z.inner, share), F32, False),
        g_state=((LAYERS, cells, z.both), F32, True), g_step=((LAYERS, 8, share), F32, True),
        narrow=(narrow, F32, True), wide=(wide, F32, True), gain=(gain, F32, True),
    )
    scratch = {k: pltpu.VMEM(shape, kind) for k, (shape, kind) in saved.items()}
    scratch.update(weight_scratch(z, 1))
    scratch.update(meta_scratch(z))
    scratch.update(reduce_scratch(ex, z.rows, z.depth))
    slots = n // 2
    stages, arrivals = piece_slots(across)
    cell_rows = LAYERS * across * padded
    state = {"state_" + k: v for k, v in reduce_scratch(ex, cell_rows, z.both).items()}
    scratch.update(
        state_part=pltpu.VMEM((n * cell_rows, z.both), BF), **state,
        sent_all=pltpu.VMEM((z.tokens, z.depth), BF), part=pltpu.VMEM((z.tokens, z.depth), BF), row_buf=pltpu.VMEM(rows, BF),
        dy=pltpu.VMEM((z.tokens, z.inner), F32), rg=pltpu.VMEM((z.tokens, z.inner), BF), rv=pltpu.VMEM((z.tokens, z.inner), BF),
        rs=pltpu.VMEM((z.tokens, z.both), BF), rd=pltpu.VMEM((z.tokens, z.heads), BF), state=pltpu.VMEM((z.half, z.inner), F32),
        d_pre_v=pltpu.VMEM((z.tokens + 8, z.inner), F32), d_pre_s=pltpu.VMEM((z.tokens + 8, z.both), F32),
        mean_own=pltpu.VMEM((LAYERS, 8, z.rows), F32), mean_all=pltpu.VMEM((LAYERS, n, 8, z.rows), F32),
        mean_send=dma(LAYERS, n), mean_recv=dma(LAYERS, n), save_sem=dma(LAYERS, len(saved)),
        own_out=pltpu.VMEM((across, z.inner, share), BF), own_inner=pltpu.VMEM((2, across, share, z.inner), BF),
        piece_stage=pltpu.VMEM((3, stages, share, z.inner), BF), piece_got=pltpu.VMEM((LAYERS, 3, arrivals, share, z.inner), BF),
        piece_send=dma(LAYERS, 3, stages), piece_recv=dma(LAYERS, 3, arrivals),
        done=pltpu.VMEM((3, share, z.inner), F32), done_sem=dma(LAYERS, 3),
        narrow=pltpu.VMEM(narrow, F32), narrow_got=pltpu.VMEM((LAYERS, across) + narrow[1:], F32),
        narrow_send=dma(LAYERS, across), narrow_recv=dma(LAYERS, across),
        wide=pltpu.VMEM(wide, F32), wide_mid=pltpu.VMEM(wide, F32),
        wide_got=pltpu.VMEM((n,) + wide, F32), wide_two=pltpu.VMEM((across,) + wide, F32),
        gain=pltpu.VMEM(gain, F32), gain_mid=pltpu.VMEM(gain, F32),
        gain_got=pltpu.VMEM((n,) + gain, F32), gain_two=pltpu.VMEM((across,) + gain, F32),
        wide_send=dma(n), wide_recv=dma(n), gain_send=dma(n), gain_recv=dma(n),
        wide_send_two=dma(across), wide_recv_two=dma(across), gain_send_two=dma(across), gain_recv_two=dma(across),
        step_part=pltpu.VMEM((LAYERS, across, 8, share), F32), step_own=pltpu.VMEM((across, LAYERS * 16, share), BF),
        step_stage=pltpu.VMEM((stages, LAYERS * 16, share), BF), step_got=pltpu.VMEM((arrivals, LAYERS * 16, share), BF),
        step_send=dma(stages), step_recv=dma(arrivals),
        cell_own=pltpu.VMEM((across, LAYERS * padded, z.both), BF),
        cell_stage=pltpu.VMEM((stages, LAYERS * padded, z.both), BF), cell_got=pltpu.VMEM((arrivals, LAYERS * padded, z.both), BF),
        cell_send=dma(stages), cell_recv=dma(arrivals),
        cell_pair_send=dma(slots), cell_pair_recv=dma(slots), cell_link_send=dma(CHUNKS * slots),
        cell_link_recv=dma(CHUNKS * (slots - 1)), grad=pltpu.VMEM(rows, F32),
        gather_send=dma(LAYERS, CHUNKS, n), gather_recv=dma(LAYERS, CHUNKS, n),
        pair_send=dma(LAYERS, slots), pair_recv=dma(LAYERS, slots),
        link_send=dma(LAYERS, CHUNKS * slots), link_recv=dma(LAYERS, CHUNKS * (slots - 1)),
    )
    return run_kernel(backward_kernel, ex, z, inputs, outputs, scratch, 1, "backward")


def final_kernel(z, n, *refs):
    block, grad, inner, out, state, step, narrow, wide, gain = refs[:9]
    (o_block, o_grad, o_norm, o_inner, o_state, o_step, o_bias, o_decay, o_skip, o_conv, o_cbias, o_sconv, o_sbias, o_gate, o_out) = refs[9:]
    o_block[...] = block[...]
    o_grad[...] = grad[...]
    o_inner[...] = inner[...]
    o_out[...] = out[...]

    @pl.when(pl.program_id(0) == 0)
    def _():
        taps, heads = z.taps, z.heads
        o_state[...] = state[...]
        cells, eighth = o_norm.shape[1], gain.shape[2]
        per = eighth // cells
        device = lax.axis_index(DATA) * n + lax.axis_index(AXIS)
        pick = lax.broadcasted_iota(jnp.int32, (eighth, cells), 0)
        pick = (pick == lax.broadcasted_iota(jnp.int32, (eighth, cells), 1) + (device % per) * cells).astype(F32)
        line = lax.broadcasted_iota(jnp.int32, (8, eighth), 0) == device // per
        ones = head_sum_matrix(z.inner, heads, z.width).astype(F32)
        for layer in range(LAYERS):
            at = slice(layer, layer + 1)
            row = jnp.sum(jnp.where(line, gain[layer], 0.0), axis=0, keepdims=True)
            o_norm[at, :] = exact(jnp.broadcast_to(row, (8, eighth)), pick)[0:1, :]
            lines = narrow[layer]
            for h in range(heads):
                o_step[h, at, :] = step[layer, h : h + 1, :]
            skip = jnp.broadcast_to(lines[taps + 2 : taps + 3, :], (8, z.inner))
            o_skip[at, :] = exact(skip, ones)[0:1, :]
            o_bias[at, :] = lines[taps + 3 : taps + 4, 0:heads]
            o_decay[at, :] = lines[taps + 4 : taps + 5, 0:heads]
            o_conv[layer] = lines[0:taps, :]
            o_cbias[at, :] = lines[taps : taps + 1, :]
            o_gate[at, :] = lines[taps + 1 : taps + 2, :]
            o_sconv[layer] = wide[layer, 0:taps, :]
            o_sbias[at, :] = wide[layer, taps : taps + 1, :]


def final_pass(ex, z, block_output, b):
    share, both, heads, taps, inner = z.depth // z.across, z.both, z.heads, z.taps, z.inner
    cells = z.depth // (ex.size * z.across)
    steps = 4 if z.rows % 32 == 0 and share % 32 == 0 and inner % 32 == 0 else 1
    whole = lambda shape: pl.BlockSpec(shape, lambda i: (0,) * len(shape))
    rows = pl.BlockSpec((z.rows // steps, z.depth), lambda i: (i, 0))
    inner_spec = pl.BlockSpec((LAYERS, 2, share // steps, inner), lambda i: (0, 0, i, 0))
    out_spec = pl.BlockSpec((LAYERS, inner // steps, share), lambda i: (0, i, 0))
    arrays = (block_output, b.input_grad, b.g_inner, b.g_out, b.g_state, b.g_step, b.narrow, b.wide, b.gain)
    small = [
        (LAYERS, cells, both), (heads, LAYERS, share), (LAYERS, heads), (LAYERS, heads), (LAYERS, heads), (LAYERS, taps, inner),
        (LAYERS, inner), (LAYERS, taps, both), (LAYERS, both), (LAYERS, inner),
    ]
    shapes = [(z.rows, z.depth), (z.rows, z.depth), (LAYERS, cells), b.g_inner.shape] + small + [b.g_out.shape]
    return pl.pallas_call(
        functools.partial(final_kernel, z, ex.size),
        grid=(steps,),
        out_shape=tuple(jax.ShapeDtypeStruct(shape, F32) for shape in shapes),
        in_specs=[rows, rows, inner_spec, out_spec] + [whole(v.shape) for v in arrays[4:]],
        out_specs=tuple([rows, rows, whole((LAYERS, cells)), inner_spec] + [whole(shape) for shape in small] + [out_spec]),
        compiler_params=pltpu.CompilerParams(vmem_limit_bytes=VM),
        cost_estimate=cost_of(1 << 20),
        name="final",
    )(*arrays)


def sizes_of(ex, across, residual, segments, w):
    inner = w.inner_weight.shape[3]
    return Sizes(
        segments.shape[1], residual.shape[0], residual.shape[1], inner, w.step_weight.shape[2], w.state_weight.shape[2],
        w.conv_weight.shape[1], inner * ex.size, across,
    )


def shards(ex, across, residual, cotangent, segments, *weights):
    w = Weights(*weights)
    z = sizes_of(ex, across, residual, segments, w)
    w = w._replace(step_weight=jnp.transpose(w.step_weight, (2, 0, 1)))
    f = forward_pass(ex, z, residual, cotangent, segments, w)
    b = backward_pass(ex, z, f, residual, cotangent, segments, w)
    made = list(final_pass(ex, z, f.block_output, b))
    made[5] = jnp.transpose(made[5], (1, 2, 0))
    return tuple(made)


def solution(mesh):
    ex = Cube(mesh.shape[AXIS])
    both, rest = (DATA, AXIS), None
    return jax.shard_map(
        functools.partial(shards, ex, mesh.shape[DATA]),
        mesh=mesh,
        in_specs=(
            P(both, rest),
            P(both, rest),
            P(DATA, rest),
            P(),
            P(rest, rest, rest, AXIS),
            P(),
            P(rest, rest, AXIS),
            P(rest, AXIS),
            P(rest, AXIS),
            P(rest, AXIS),
            P(rest, rest, AXIS),
            P(rest, AXIS),
            P(),
            P(),
            P(rest, AXIS),
            P(rest, AXIS, rest),
        ),
        out_specs=(
            P(both, rest),
            P(both, rest),
            P(rest, both),
            P(rest, rest, DATA, AXIS),
            P(rest, both, rest),
            P(rest, DATA, AXIS),
            P(rest, AXIS),
            P(rest, AXIS),
            P(rest, AXIS),
            P(rest, rest, AXIS),
            P(rest, AXIS),
            P(),
            P(),
            P(rest, AXIS),
            P(rest, AXIS, DATA),
        ),
        check_vma=False,
    )
```

```python
import functools
from types import SimpleNamespace
from typing import NamedTuple

import jax
import jax.numpy as jnp
from jax import lax
from jax.experimental import pallas as pl
from jax.experimental.pallas import tpu as pltpu
from jax.sharding import PartitionSpec as P

LAYERS = 2
SIZE = 128
CHUNKS = 2
AXIS = "tensor"
DATA = "dp"
EPS = 1e-05
HIGH = lax.Precision.HIGHEST
F32 = jnp.float32
BF = jnp.bfloat16
VM = 67_000_000


def cost_of(flops, moved=1 << 24):
    return pl.CostEstimate(flops=flops, bytes_accessed=moved, transcendentals=0)


class Weights(NamedTuple):
    norm_gain: jax.Array
    inner_weight: jax.Array
    state_weight: jax.Array
    step_weight: jax.Array
    step_bias: jax.Array
    decay_log: jax.Array
    skip_gain: jax.Array
    conv_weight: jax.Array
    conv_bias: jax.Array
    state_conv_weight: jax.Array
    state_conv_bias: jax.Array
    gate_gain: jax.Array
    out_weight: jax.Array


def dot(a, b):
    return lax.dot_general(a, b, (((1,), (0,)), ((), ())), preferred_element_type=F32)


def dot_t(a, b):
    return lax.dot_general(a, b, (((1,), (1,)), ((), ())), preferred_element_type=F32)


def t_dot(a, b):
    return lax.dot_general(a, b, (((0,), (0,)), ((), ())), preferred_element_type=F32)


def exact(a, b):
    return lax.dot_general(
        a, b, (((1,), (0,)), ((), ())), preferred_element_type=F32, precision=HIGH
    )


def sigmoid(x):
    return 1.0 / (1.0 + jnp.exp(-x))


def softplus(x):
    return jnp.maximum(x, 0.0) + jnp.log1p(jnp.exp(-jnp.abs(x)))


def tiles_of(inner, width):
    return [
        (start, min(128, inner - start), start // width, min(128, inner - start) // width)
        for start in range(0, inner, 128)
    ]


def expand(cols, inner, width):
    rows = cols.shape[0]
    parts = []
    for _, wide, first, number in tiles_of(inner, width):
        lane = lax.broadcasted_iota(jnp.int32, (rows, wide), 1)
        value = jnp.broadcast_to(cols[:, first : first + 1], (rows, wide))
        for j in range(1, number):
            value = jnp.where(lane >= j * width, cols[:, first + j : first + j + 1], value)
        parts.append(value)
    return parts[0] if len(parts) == 1 else jnp.concatenate(parts, axis=1)


def head_sum_matrix(inner, heads, width):
    row = lax.broadcasted_iota(jnp.int32, (inner, heads), 0)
    col = lax.broadcasted_iota(jnp.int32, (inner, heads), 1)
    return ((row >= col * width) & (row < (col + 1) * width)).astype(BF)


def head_sum(value, inner, heads, width, parts=1):
    ones = head_sum_matrix(inner, heads, width)
    high = value.astype(BF)
    if parts == 1:
        return dot(high, ones)
    return dot(high, ones) + dot((value - high.astype(F32)).astype(BF), ones)


def head_split(tile, width, number):
    if number == 1:
        return tile
    lane = lax.broadcasted_iota(jnp.int32, tile.shape, 1)
    zero = jnp.zeros_like(tile)
    return jnp.concatenate(
        [
            jnp.where((lane >= j * width) & (lane < (j + 1) * width), tile, zero)
            for j in range(number)
        ],
        axis=0,
    )


def pair_mask(seg_col, seg_row):
    rows, cols = seg_col.shape[0], seg_row.shape[1]
    row = lax.broadcasted_iota(jnp.int32, (rows, cols), 0)
    col = lax.broadcasted_iota(jnp.int32, (rows, cols), 1)
    return (row >= col) & (seg_col == seg_row)


def lower_ones(size):
    row = lax.broadcasted_iota(jnp.int32, (size, size), 0)
    col = lax.broadcasted_iota(jnp.int32, (size, size), 1)
    return (row >= col).astype(F32)


def turned(value):
    return jnp.transpose(value)


def column_of(tile):
    rows = tile.shape[1]
    return jnp.transpose(jnp.broadcast_to(tile[0:1, :], (rows, rows)))[:, 0:1]


def tile_of(column):
    rows = column.shape[0]
    return jnp.transpose(jnp.broadcast_to(column, (rows, rows)))[0:8, :]


def later_ones(seg_col, seg_row):
    rows, cols = seg_col.shape[0], seg_row.shape[1]
    row = lax.broadcasted_iota(jnp.int32, (rows, cols), 0)
    col = lax.broadcasted_iota(jnp.int32, (rows, cols), 1)
    return ((row <= col) & (seg_col == seg_row)).astype(F32)


def earlier_ones(seg_col, seg_row):
    rows, cols = seg_col.shape[0], seg_row.shape[1]
    row = lax.broadcasted_iota(jnp.int32, (rows, cols), 0)
    col = lax.broadcasted_iota(jnp.int32, (rows, cols), 1)
    return ((row > col) & (seg_col == seg_row)).astype(F32)


def build_meta(count, seg_ref, column, meta, segrow):
    row = seg_ref[...].astype(F32)
    segrow[0:1, :] = row
    wide = column.shape[1]
    column[0:8, :] = jnp.full((8, wide), -1.0, F32)
    for c in range(count):
        part = row[:, c * SIZE : (c + 1) * SIZE]
        column[8 + c * SIZE : 8 + (c + 1) * SIZE, :] = jnp.transpose(jnp.broadcast_to(part, (SIZE, SIZE)))
    lane = lax.broadcasted_iota(jnp.int32, (SIZE, wide), 1)
    for c in range(count):
        first = 8 + c * SIZE
        now = column[first : first + SIZE, :]
        before = column[first - 1 : first, :]
        end = column[first + SIZE - 1 : first + SIZE, :]
        value = now
        for k in range(1, 4):
            kept = (column[first - k : first - k + SIZE, :] == now).astype(F32)
            value = jnp.where(lane == k, kept, value)
        value = jnp.where(lane == 4, (now == before).astype(F32), value)
        value = jnp.where(lane == 5, (now == end).astype(F32), value)
        value = jnp.where(lane == 6, jnp.broadcast_to((end == before).astype(F32), (SIZE, wide)), value)
        meta[c * SIZE : (c + 1) * SIZE, :] = value[:, 0:8]
    meta[count * SIZE :, :] = jnp.zeros((8, 8), F32)


def span_of(dims):
    found = [0]
    for d in dims:
        found = found + [r ^ d for r in found]
    return found


def most_first(offsets):
    return sorted(offsets, key=lambda r: -bin(r).count("1"))


class Cube:
    def __init__(self, size):
        self.size = size
        self.links = [1 << b for b in range(1, size.bit_length() - 1)]
        self.orders = [self.links, self.links[::-1]]
        self.offsets = most_first(span_of(self.links))

    def gather_dims(self, q):
        return self.orders[q % 2] + [1]

    def gather_last(self, q, r):
        return max([i for i, d in enumerate(self.gather_dims(q)) if r & d], default=-1)

    def gather_steps(self, q):
        found = [r for r in span_of(self.links) if r]
        return sorted(found, key=lambda r: (self.gather_last(q, r), r & (r - 1) != 0))


def reduce_steps(order):
    steps = []
    for i, d in enumerate(order):
        for s in most_first(span_of(order[i + 1 :])):
            steps.append((i, d ^ s))
    return steps + [(len(order), 0)]


def arrival_slots(order, first=0):
    found = {}
    for i, r in reduce_steps(order):
        for j in range(i):
            found[(j, r)] = first + len(found)
    return found


def remote(src, dst, send, recv, target, axis=AXIS):
    return pltpu.make_async_remote_copy(
        src_ref=src, dst_ref=dst, send_sem=send, recv_sem=recv,
        device_id={axis: target}, device_id_type=pl.DeviceIdType.MESH,
    )


def greet(targets, across=()):
    barrier = pltpu.get_barrier_semaphore()
    for axis, group in ((AXIS, targets), (DATA, across)):
        for target in group:
            pl.semaphore_signal(barrier, inc=1, device_id={axis: target}, device_id_type=pl.DeviceIdType.MESH)
    pl.semaphore_wait(barrier, len(targets) + len(across))


def rows_of(block, rows, many=1):
    return pl.ds(pl.multiple_of(block * rows, rows), rows * many)


def dma(*shape):
    return pltpu.SemaphoreType.DMA(shape)


class Gather:
    def __init__(self, ex, rows, row_buf, out, send_sem, recv_sem):
        self.ex, self.rows, self.row_buf, self.out = ex, rows, row_buf, out
        self.send_sem, self.recv_sem = send_sem, recv_sem
        self.me = lax.axis_index(AXIS)
        self.copies, self.arrived = {}, set()

    def hops(self, q, r):
        dims, part = self.ex.gather_dims(q), self.rows // CHUNKS
        place = pl.ds(pl.multiple_of((self.me ^ r) * self.rows + q * part, part), part)
        src = self.row_buf.at[pl.ds(q * part, part), :] if r == 0 else self.out.at[place, :]
        found = []
        for i in range(self.ex.gather_last(q, r) + 1, len(dims)):
            b = r ^ dims[i]
            found.append((b, remote(src, self.out.at[place, :], self.send_sem.at[q, b], self.recv_sem.at[q, b], self.me ^ dims[i])))
        return found

    def start(self, *pieces):
        part = self.rows // CHUNKS
        hops = [self.hops(q, 0) for q in pieces]
        for step in zip(*hops):
            for q, (b, copy) in zip(pieces, step):
                copy.start()
                self.copies[(q, b)] = copy
        for q in pieces:
            here = pl.ds(pl.multiple_of(self.me * self.rows + q * part, part), part)
            self.out[here, :] = self.row_buf[q * part : (q + 1) * part, :]

    def need(self, q, r):
        if (q, r) not in self.arrived:
            self.copies[(q, r)].wait_recv()
            self.arrived.add((q, r))
            for b, copy in self.hops(q, r):
                copy.start()
                self.copies[(q, b)] = copy

    def run(self, visit):
        ex = self.ex
        steps = [ex.gather_steps(q) for q in range(CHUNKS)]
        visits = sorted(span_of(ex.links), key=lambda g: (ex.gather_last(0, g), g & (g - 1) != 0))
        k = 0
        for g in visits:
            while g and not all((q, g) in self.arrived for q in range(CHUNKS)):
                for q in range(CHUNKS):
                    self.need(q, steps[q][k])
                k += 1
            for q in range(CHUNKS):
                self.need(q, g ^ 1)
            visit(g)
        return list(self.copies.values())


def reduce_scratch(ex, rows, depth):
    slots, part = ex.size // 2, rows // CHUNKS
    return dict(
        pair=pltpu.VMEM((slots, rows, depth), BF),
        stage=pltpu.VMEM((CHUNKS * slots, part, depth), BF),
        got=pltpu.VMEM((CHUNKS * (slots - 1), part, depth), BF),
    )


def reduce_rows(*args, idle=None, ahead=True):
    for t, _ in enumerate(reduce_steps_of(*args, ahead=ahead)):
        if idle is not None:
            idle(t)


def reduce_steps_of(ex, rows, part, pair, stage, got, sems, produce, final, pending, ahead=True):
    me = lax.axis_index(AXIS)
    pair_send, pair_recv, link_send, link_recv = sems
    n, size = ex.size, rows // CHUNKS
    slot_of = {r: i for i, r in enumerate(ex.offsets)}
    orders = [ex.orders[q % 2] for q in range(CHUNKS)]
    steps = [reduce_steps(order) for order in orders]
    slots = [arrival_slots(order, q * (n // 2 - 1)) for q, order in enumerate(orders)]
    waiting = list(ex.offsets)
    pairs, ready, arrivals = {}, set(), {}

    def advance():
        r = waiting.pop(0)
        produce(r, False)
        i = slot_of[r]
        pairs[r] = remote(part.at[rows_of(me ^ r ^ 1, rows), :], pair.at[i], pair_send.at[i], pair_recv.at[i], me ^ 1)
        pairs[r].start()
        produce(r, True)

    def step(q, k):
        i, r = steps[q][k]
        while r not in pairs:
            advance()
        if r not in ready:
            pairs[r].wait_recv()
            ready.add(r)
        own = part[pl.ds(pl.multiple_of((me ^ r) * rows + q * size, size), size), :]
        value = own.astype(F32) + pair[slot_of[r], pl.ds(q * size, size), :].astype(F32)
        for j in range(i):
            arrivals[(q, j, r)].wait_recv()
            value = value + got[slots[q][(j, r)]].astype(F32)
        if r == 0:
            final(q, value)
            return
        d = orders[q][i]
        s = q * (n // 2) + slot_of[r]
        stage[s] = value.astype(BF)
        at = slots[q][(i, r ^ d)]
        copy = remote(stage.at[s], got.at[at], link_send.at[s], link_recv.at[at], me ^ d)
        copy.start()
        arrivals[(q, i, r ^ d)] = copy
        pending.append(copy)

    advance()
    waves = CHUNKS // 2
    for t in range(len(steps[0]) + waves - 1):
        if waiting and ahead:
            advance()
        for p in range(waves):
            if 0 <= t - p < len(steps[0]):
                step(2 * p, t - p)
                step(2 * p + 1, t - p)
        if waiting and not ahead:
            advance()
        if t + 1 == len(steps[0]) + waves - 1:
            pending.extend(pairs.values())
        yield t


def row_scale_of(resid):
    return lax.rsqrt(jnp.mean(resid * resid, axis=1, keepdims=True) + EPS)


def group_rows(ex, g, rows):
    me = lax.axis_index(AXIS)
    return pl.ds(pl.multiple_of(((me ^ g) // 2) * (2 * rows), 2 * rows), 2 * rows)


class Sizes(NamedTuple):
    tokens: int
    rows: int
    depth: int
    inner: int
    heads: int
    both: int
    taps: int
    inner_all: int
    across: int

    @property
    def width(self):
        return self.inner // self.heads

    @property
    def half(self):
        return self.both // 2

    @property
    def count(self):
        return self.tokens // SIZE


def weight_scratch(z, layers):
    return dict(
        win=pltpu.VMEM((layers, 2, z.depth, z.inner), BF),
        wst=pltpu.VMEM((layers, z.depth, z.both), BF),
        wstep=pltpu.VMEM((layers, z.heads, z.depth), F32),
        wout=pltpu.VMEM((layers, z.inner, z.depth), BF),
        weight_sem=dma(LAYERS, 3),
    )


def step_rows(z, a, s, layer, slot):
    for h in range(z.heads):
        s.wstep[slot, h : h + 1, :] = a.step_weight[h, layer : layer + 1, :].astype(F32)


def meta_scratch(z):
    return dict(
        column=pltpu.VMEM((z.tokens + 8, SIZE), F32), meta=pltpu.VMEM((z.tokens + 8, 8), F32), segrow=pltpu.VMEM((8, z.tokens), F32)
    )


def weight_loads(s, a, layer, slot):
    return [
        pltpu.make_async_copy(src.at[layer], dst.at[slot], s.weight_sem.at[layer, i])
        for i, (src, dst) in enumerate(
            ((a.inner_weight, s.win), (a.state_weight, s.wst), (a.out_weight, s.wout))
        )
    ]


def saved_shapes(z):
    t, i = z.tokens, z.inner
    return dict(
        normed=((t, z.depth), BF), gate=((t, i), F32), pre_v=((t, i), F32), y=((t, i), F32), pre_s=((t, z.both), F32),
        step_in=((t, z.heads), F32), value=((t, i), BF), raw=((t, z.both), BF), scaled=((t, i), BF),
        entering=((z.count, z.half, i), BF),
    )


def mix_states(z, layer, s, a, meta):
    at = slice(layer, layer + 1)
    inner, width, half = z.inner, z.width, z.half
    s.state[...] = jnp.zeros_like(s.state)

    def chunk(c, carry):
        rows = pl.ds(pl.multiple_of(c * SIZE, SIZE), SIZE)
        window = pl.ds(pl.multiple_of(c * SIZE, SIZE), SIZE + 8)
        m = meta[rows, :]

        def conv(buf, w_ref, b_ref):
            win = buf[window, :]
            total = b_ref[at, :] + w_ref[layer, 0:1, :] * win[8:, :]
            for k in range(1, z.taps):
                total = total + w_ref[layer, k : k + 1, :] * (win[8 - k : 8 - k + SIZE, :] * m[:, k : k + 1])
            return total, win[8:, :]

        pre_v, value = conv(s.vbuf, a.conv_weight, a.conv_bias)
        pre_s, raw = conv(s.sbuf, a.state_conv_weight, a.state_conv_bias)
        s.value[rows, :] = value.astype(BF)
        s.raw[rows, :] = raw.astype(BF)
        s.pre_v[rows, :] = pre_v
        s.pre_s[rows, :] = pre_s
        x = pre_v * sigmoid(pre_v)
        st = (pre_s * sigmoid(pre_s)).astype(BF)
        dt = softplus(s.step_in[rows, :] + a.step_bias[at, :])
        cum = exact(lower_ones(SIZE), -dt * jnp.exp(a.decay_log[at, :]))
        last = cum[SIZE - 1 : SIZE, :]
        xt = (x * expand(dt, inner, width)).astype(BF)
        s.x[rows, :] = x
        s.xt[rows, :] = xt
        s.states[rows, :] = st
        s.cum[rows, :] = cum
        before = s.state[...]
        s.entering[c] = before.astype(BF)
        to_end = jnp.exp(last - cum) * m[:, 5:6]
        ended = (xt.astype(F32) * expand(to_end, inner, width)).astype(BF)
        s.state[...] = expand(jnp.exp(last) * m[0:1, 6:7], inner, width) * before + t_dot(st[:, :half], ended)
        return carry

    lax.fori_loop(0, z.count, chunk, 0)


def mix_outputs(z, layer, s, a, meta, segrow, c):
    at = slice(layer, layer + 1)
    inner, width, half = z.inner, z.width, z.half
    rows = pl.ds(pl.multiple_of(c * SIZE, SIZE), SIZE)
    m = meta[rows, :]
    st, cum, xt = s.states[rows, :], s.cum[rows, :], s.xt[rows, :]
    b_mat, c_mat = st[:, :half], st[:, half:]
    cum_t = turned(cum)
    from_state = jnp.exp(cum) * m[:, 4:5]
    scores = dot_t(c_mat, b_mat)
    mask = pair_mask(m[:, 0:1], segrow[0:1, rows])
    parts = []
    for start, wide, first, number in tiles_of(inner, width):
        mats = []
        for h in range(first, first + number):
            differ = cum[:, h : h + 1] - cum_t[h : h + 1, :]
            mats.append((jnp.exp(jnp.where(mask, differ, -1e30)) * scores).astype(BF))
        left = mats[0] if number == 1 else jnp.concatenate(mats, axis=1)
        parts.append(dot(left, head_split(xt[:, start : start + wide], width, number)))
    intra = parts[0] if len(parts) == 1 else jnp.concatenate(parts, axis=1)
    inter = dot(c_mat, s.entering[c]) * expand(from_state, inner, width)
    y = intra + inter + expand(a.skip_gain[at, :], inner, width) * s.x[rows, :]
    s.y[rows, :] = y
    gate = s.gate[rows, :]
    gated = y * (gate * sigmoid(gate))
    square = jnp.sum(gated * gated, axis=1, keepdims=True)
    tile = tile_of(square)
    per = SIZE // z.rows if SIZE > z.rows else 1
    wide = SIZE // per
    for k in range(per):
        s.squares[c * per + k] = tile[:, k * wide : (k + 1) * wide]
    s.scaled[rows, :] = (gated * a.gate_gain[at, :]).astype(BF)


def forward_kernel(ex, z, names_in, names_out, names_scratch, *refs):
    count_in, count_out = len(names_in), len(names_out)
    a = SimpleNamespace(**dict(zip(names_in, refs)))
    o = SimpleNamespace(**dict(zip(names_out, refs[count_in:])))
    s = SimpleNamespace(**dict(zip(names_scratch, refs[count_in + count_out :])))
    me = lax.axis_index(AXIS)
    n = ex.size
    greet([me ^ r for r in range(1, n)])
    loads = [weight_loads(s, a, layer, layer) for layer in range(LAYERS)]
    for copy in loads[0] + loads[1]:
        copy.start()
    s.vbuf[0:8, :] = jnp.zeros((8, z.inner), F32)
    s.sbuf[0:8, :] = jnp.zeros((8, z.both), F32)
    saves = []
    size = z.rows // CHUNKS
    gathers = [
        Gather(ex, z.rows, s.row_buf, s.normed.at[layer], s.gather_send.at[layer], s.gather_recv.at[layer]) for layer in range(LAYERS)
    ]
    hidden = a.residual[...]
    s.hidden[...] = hidden
    s.row_buf[...] = (hidden * row_scale_of(hidden) * a.norm_gain[0:1, :]).astype(BF)
    gathers[0].start(*range(CHUNKS))
    build_meta(z.count, a.segments, s.column, s.meta, s.segrow)
    for layer in range(LAYERS):
        step_rows(z, a, s, layer, layer)
    means = []
    for layer in range(LAYERS):
        normed = s.normed.at[layer]

        def project(g, layer=layer, normed=normed):
            if g == 0:
                for copy in loads[layer]:
                    copy.wait()
            here = group_rows(ex, g, z.rows)
            beyond = pl.ds(pl.multiple_of(((me ^ g) // 2) * (2 * z.rows) + 8, 8), 2 * z.rows)
            nb = normed[here, :]
            s.gate[here, :] = dot(nb, s.win[layer, 0])
            s.vbuf[beyond, :] = dot(nb, s.win[layer, 1])
            s.sbuf[beyond, :] = dot(nb, s.wst[layer])
            s.step_in[here, :] = dot_t(nb, s.wstep[layer].astype(BF))

        sent = gathers[layer].run(project)
        mix_states(z, layer, s, a, s.meta)

        def save(late, layer=layer, normed=normed):
            for i, name in enumerate(names_out[: len(saved_shapes(z))]):
                src = normed if i == 0 else getattr(s, name)
                if late == (src is s.y or src is s.scaled):
                    saves.append(pltpu.make_async_copy(src, getattr(o, name).at[layer], s.save_sem.at[layer, i]))
                    saves[-1].start()

        save(False)
        for copy in sent:
            copy.wait_send()
        squares = {}

        def produce(g, own, layer=layer, squares=squares):
            if 2 * z.rows > SIZE:
                block = me ^ g if own else me ^ g ^ 1
                here, first, many = rows_of(block, z.rows), block * (z.rows // SIZE), z.rows // SIZE
            elif not own:
                here, first, many = group_rows(ex, g, z.rows), (me ^ g) // 2, 1
            if own <= (2 * z.rows > SIZE):
                for i in range(many):
                    mix_outputs(z, layer, s, a, s.meta, s.segrow, first + i)
                s.part[here, :] = dot(s.scaled[here, :], s.wout[layer]).astype(BF)
            for r in (g, g ^ 1) if own else ():
                if r:
                    squares[r] = remote(
                        s.squares.at[me ^ r], s.square_got.at[layer, r], s.square_send.at[layer, r], s.square_recv.at[layer, r], me ^ r
                    )
                    squares[r].start()

        def idle(t, save=save):
            if t == 2:
                save(True)

        gates = []

        def final(q, value, layer=layer, squares=squares, gates=gates):
            if not gates:
                square = s.squares[me]
                for r, copy in squares.items():
                    copy.wait_recv()
                    square = square + s.square_got[layer, r]
                gates.append(lax.rsqrt(column_of(square) / z.inner_all + EPS))
                if layer + 1 < LAYERS:
                    o.gates[layer] = gates[0]
            rows = slice(q * size, (q + 1) * size)
            gate = gates[0][rows, :]
            mixed = gate * value
            hidden = s.hidden[rows, :] + mixed
            if layer + 1 < LAYERS:
                s.row_buf[rows, :] = (hidden * row_scale_of(hidden) * a.norm_gain[layer + 1 : layer + 2, :]).astype(BF)
                gathers[layer + 1].start(q)
                s.hidden[rows, :] = hidden
                o.resids[layer, rows, :] = hidden
                o.mixeds[layer, rows, :] = mixed
            else:
                grad = a.cotangent[rows, :]
                o.block_output[rows, :] = hidden
                o.sent[rows, :] = (gate * grad).astype(BF)
                means.append((q, -0.5 * gate * gate * jnp.sum(mixed * grad, axis=1, keepdims=True)))

        links = []
        reduce_rows(
            ex, z.rows, s.part, s.pair, s.stage, s.got,
            (s.pair_send.at[layer], s.pair_recv.at[layer], s.link_send.at[layer], s.link_recv.at[layer]), produce, final, links, idle=idle, ahead=False,
        )
        for copy in links + list(squares.values()):
            copy.wait_send()
        for copy in saves:
            copy.wait()
        saves = []
    o.mean[...] = tile_of(jnp.concatenate([v for _, v in sorted(means, key=lambda m: m[0])], axis=0))


def run_kernel(kernel, ex, z, inputs, outputs, scratch, collective, name):
    vm, anywhere = pl.BlockSpec(memory_space=pltpu.VMEM), pl.BlockSpec(memory_space=pl.ANY)
    made = pl.pallas_call(
        functools.partial(kernel, ex, z, tuple(inputs), tuple(outputs), tuple(scratch)),
        out_shape=tuple(jax.ShapeDtypeStruct(shape, kind) for shape, kind, _ in outputs.values()),
        in_specs=[vm if inside else anywhere for _, inside in inputs.values()],
        out_specs=tuple(vm if inside else anywhere for _, _, inside in outputs.values()),
        scratch_shapes=list(scratch.values()),
        compiler_params=pltpu.CompilerParams(collective_id=collective, has_side_effects=True, vmem_limit_bytes=VM),
        cost_estimate=cost_of(1 << 35),
        name=name,
    )(*[array for array, _ in inputs.values()])
    return SimpleNamespace(**dict(zip(outputs, made)))


def small_inputs(w):
    return dict(
        norm_gain=(w.norm_gain, True), step_bias=(w.step_bias, True), decay_log=(w.decay_log, True),
        skip_gain=(w.skip_gain, True), conv_weight=(w.conv_weight, True), conv_bias=(w.conv_bias, True),
        state_conv_weight=(w.state_conv_weight, True), state_conv_bias=(w.state_conv_bias, True), gate_gain=(w.gate_gain, True),
        inner_weight=(w.inner_weight, False), state_weight=(w.state_weight, False), step_weight=(w.step_weight, True),
        out_weight=(w.out_weight, False),
    )


def forward_pass(ex, z, residual, cotangent, segments, w):
    n = ex.size
    saved = saved_shapes(z)
    inputs = dict(residual=(residual, True), cotangent=(cotangent, True), segments=(segments, True), **small_inputs(w))
    rows = (z.rows, z.depth)
    outputs = {k: ((LAYERS,) + shape, kind, False) for k, (shape, kind) in saved.items()}
    outputs.update(
        resids=((LAYERS - 1,) + rows, F32, True), mixeds=((LAYERS - 1,) + rows, F32, True),
        gates=((LAYERS - 1, z.rows, 1), F32, True), block_output=(rows, F32, True),
        sent=(rows, BF, True), mean=((8, z.rows), F32, True),
    )
    scratch = {k: pltpu.VMEM(shape, kind) for k, (shape, kind) in saved.items()}
    scratch.update(normed=pltpu.VMEM((LAYERS, z.tokens, z.depth), BF))
    scratch.update(weight_scratch(z, LAYERS))
    scratch.update(meta_scratch(z))
    scratch.update(reduce_scratch(ex, z.rows, z.depth))
    slots = n // 2
    scratch.update(
        vbuf=pltpu.VMEM((z.tokens + 8, z.inner), F32), sbuf=pltpu.VMEM((z.tokens + 8, z.both), F32),
        x=pltpu.VMEM((z.tokens, z.inner), F32), xt=pltpu.VMEM((z.tokens, z.inner), BF), states=pltpu.VMEM((z.tokens, z.both), BF),
        cum=pltpu.VMEM((z.tokens, z.heads), F32), state=pltpu.VMEM((z.half, z.inner), F32), part=pltpu.VMEM((z.tokens, z.depth), BF), row_buf=pltpu.VMEM(rows, BF),
        squares=pltpu.VMEM((n, 8, z.rows), F32), square_got=pltpu.VMEM((LAYERS, n, 8, z.rows), F32),
        square_send=dma(LAYERS, n), square_recv=dma(LAYERS, n), save_sem=dma(LAYERS, len(saved)),
        gather_send=dma(LAYERS, CHUNKS, n), gather_recv=dma(LAYERS, CHUNKS, n),
        pair_send=dma(LAYERS, slots), pair_recv=dma(LAYERS, slots), hidden=pltpu.VMEM(rows, F32),
        link_send=dma(LAYERS, CHUNKS * slots), link_recv=dma(LAYERS, CHUNKS * (slots - 1)),
    )
    return run_kernel(forward_kernel, ex, z, inputs, outputs, scratch, 0, "forward")


class Piece:
    def __init__(self, across, own, stage, got, send, recv):
        self.order = [1 << b for b in range(across.bit_length() - 1)]
        self.own, self.stage, self.got, self.send, self.recv = own, stage, got, send, recv
        self.slots = arrival_slots(self.order)
        self.row = lax.axis_index(DATA)
        self.arrivals, self.sent = {}, []

    def value(self, i, r):
        total = self.own[self.row ^ r].astype(F32)
        for j in range(i):
            self.arrivals[(j, r)].wait_recv()
            total = total + self.got[self.slots[(j, r)]].astype(F32)
        return total

    def phase(self, k):
        for number, (i, r) in enumerate(reduce_steps(self.order)):
            if i != k or r == 0:
                continue
            src = self.own.at[self.row ^ r]
            if i:
                self.stage[number] = self.value(i, r).astype(BF)
                src = self.stage.at[number]
            d = self.order[i]
            at = self.slots[(i, r ^ d)]
            copy = remote(src, self.got.at[at], self.send.at[number], self.recv.at[at], self.row ^ d, DATA)
            copy.start()
            self.arrivals[(i, r ^ d)] = copy
            self.sent.append(copy)

    def last(self):
        total = self.value(len(self.order), 0)
        for copy in self.sent:
            copy.wait_send()
        return total


def mix_backward(z, layer, s, a, meta, segrow):
    at = slice(layer, layer + 1)
    inner, width, half, heads, taps = z.inner, z.width, z.half, z.heads, z.taps
    s.state[...] = jnp.zeros_like(s.state)
    group = 2 if z.count % 2 == 0 else 1

    def chunk(c, after):
        rows = pl.ds(pl.multiple_of(c * SIZE, SIZE), SIZE)
        m = meta[rows, :]
        y, dy = s.y[rows, :], s.dy[rows, :]
        pre_v, pre_s = s.pre_v[rows, :], s.pre_s[rows, :]
        sig_v, sig_s = sigmoid(pre_v), sigmoid(pre_s)
        x = pre_v * sig_v
        st = pre_s * sig_s
        b_mat = st[:, :half].astype(BF)
        c_mat = st[:, half:].astype(BF)
        raw_step = s.step_in[rows, :] + a.step_bias[at, :]
        dt = softplus(raw_step)
        rate = jnp.exp(a.decay_log[at, :])
        log_decay = -dt * rate
        cum = exact(lower_ones(SIZE), log_decay)
        cum_t = turned(cum)
        last = cum[SIZE - 1 : SIZE, :]
        dt_all = expand(dt, inner, width)
        skip_all = expand(a.skip_gain[at, :], inner, width)
        xt = (x * dt_all).astype(BF)
        dy_b = dy.astype(BF)
        from_state = expand(jnp.exp(cum) * m[:, 4:5], inner, width)
        to_end = expand(jnp.exp(last - cum) * m[:, 5:6], inner, width)
        carry = expand(jnp.exp(last) * m[0:1, 6:7], inner, width)
        scores = dot_t(c_mat, b_mat)
        mask = pair_mask(m[:, 0:1], segrow[0:1, rows])
        d_scores = jnp.zeros((SIZE, SIZE), F32)
        parts = []
        for start, wide, first, number in tiles_of(inner, width):
            dy_split = head_split(dy_b[:, start : start + wide], width, number)
            d_mats = dot_t(dy_split, xt[:, start : start + wide])
            mats = []
            for j in range(number):
                h = first + j
                differ = cum[:, h : h + 1] - cum_t[h : h + 1, :]
                decay = jnp.exp(jnp.where(mask, differ, -1e30))
                mats.append((decay * scores).astype(BF))
                d_scores = d_scores + d_mats[j * SIZE : (j + 1) * SIZE, :] * decay
            left = mats[0] if number == 1 else jnp.concatenate(mats, axis=0)
            parts.append(t_dot(left, dy_split))
        intra = parts[0] if len(parts) == 1 else jnp.concatenate(parts, axis=1)
        d_scores = d_scores.astype(BF)
        before = s.entering[c]
        after_b = after.astype(BF)
        dy_in = (dy * from_state).astype(BF)
        xt_f = xt.astype(F32)
        ended = (xt_f * to_end).astype(BF)
        from_later = dot(b_mat, after_b) * to_end
        d_xt = intra + from_later
        d_c = dot(d_scores, b_mat) + dot_t(dy_in, before)
        d_b = t_dot(d_scores, c_mat) + dot_t(ended, after_b)
        across = carry * jnp.sum(before.astype(F32) * after, axis=0, keepdims=True)
        fresh = carry * after + t_dot(c_mat, dy_in)
        pairs = head_sum(dy_b.astype(F32) * (y - skip_all * x) - xt_f * intra, inner, heads, width, 2)
        sums = head_sum(
            jnp.concatenate([xt_f * from_later, x * d_xt, jnp.broadcast_to(across, (8, inner))], axis=0), inner, heads, width
        )
        seg_col, seg_row = m[:, 0:1], segrow[0:1, rows]
        d_log = (
            exact(later_ones(seg_col, seg_row), pairs)
            + exact(earlier_ones(seg_col, seg_row), sums[0:SIZE])
            + sums[2 * SIZE : 2 * SIZE + 1]
        )
        d_raw = (sums[SIZE : 2 * SIZE] - rate * d_log) * sigmoid(raw_step)
        s.rd[rows, :] = d_raw.astype(BF)
        d_x = dy * skip_all + d_xt * dt_all
        s.d_pre_v[rows, :] = d_x * (sig_v * (1.0 + pre_v * (1.0 - sig_v)))
        d_st = jnp.concatenate([d_b, d_c], axis=1)
        s.d_pre_s[rows, :] = d_st * (sig_s * (1.0 + pre_s * (1.0 - sig_s)))
        total = lambda v: jnp.sum(v, axis=0, keepdims=True)
        return fresh, (total(dy * x), total(d_raw), total(d_log * log_decay))

    def body(i, sums):
        after = s.state[...]
        for k in range(group):
            after, more = chunk(z.count - 1 - (i * group + k), after)
            sums = tuple(u + v for u, v in zip(sums, more))
        s.state[...] = after
        return sums

    zero = lambda wide: jnp.zeros((1, wide), F32)
    skip, bias, decay = lax.fori_loop(0, z.count // group, body, (zero(inner), zero(heads), zero(heads)))
    s.narrow[layer, taps + 2 : taps + 3, :] = skip
    s.narrow[layer, taps + 3 : taps + 4, 0:heads] = bias
    s.narrow[layer, taps + 4 : taps + 5, 0:heads] = decay

    def conv_body(c, sums):
        rows = pl.ds(pl.multiple_of(c * SIZE, SIZE), SIZE)
        window = pl.ds(pl.multiple_of(c * SIZE, SIZE), SIZE + 8)
        m = meta[window, :]
        more = []
        for src, w_ref, value_ref, dst in ((s.d_pre_v, a.conv_weight, s.value, s.rv), (s.d_pre_s, a.state_conv_weight, s.raw, s.rs)):
            win = src[window, :]
            value = value_ref[rows, :].astype(F32)
            now = win[0:SIZE, :]
            total = w_ref[layer, 0:1, :] * now
            lines = [jnp.sum(now * value, axis=0, keepdims=True)]
            for k in range(1, taps):
                moved = win[k : k + SIZE, :] * m[k : k + SIZE, k : k + 1]
                total = total + w_ref[layer, k : k + 1, :] * moved
                lines.append(jnp.sum(moved * value, axis=0, keepdims=True))
            lines.append(jnp.sum(now, axis=0, keepdims=True))
            dst[rows, :] = total.astype(BF)
            more.extend(lines)
        return tuple(u + v for u, v in zip(sums, more))

    lines = lax.fori_loop(0, z.count, conv_body, (zero(inner),) * (taps + 1) + (zero(z.both),) * (taps + 1))
    for k in range(taps + 1):
        s.narrow[layer, k : k + 1, :] = lines[k]
        s.wide[layer, k : k + 1, :] = lines[taps + 1 + k]


def norm_backward(total, resid, grad, gain):
    scale = row_scale_of(resid)
    weighted = total * gain
    inner = jnp.sum(weighted * resid, axis=1, keepdims=True)
    gain_grad = jnp.sum(total * resid * scale, axis=0, keepdims=True)
    return grad + scale * weighted - resid * (scale * scale * scale * inner / resid.shape[1]), gain_grad


def exchange(src, got, send, recv, place, number, axis):
    copies = [remote(src, got.at[r], send.at[r], recv.at[r], place ^ r, axis) for r in range(1, number)]
    for copy in copies:
        copy.start()
    return copies


def collected(own, got, copies):
    total = own
    for r, copy in enumerate(copies, 1):
        copy.wait_recv()
        total = total + got[r]
    return total


def backward_kernel(ex, z, names_in, names_out, names_scratch, *refs):
    count_in, count_out = len(names_in), len(names_out)
    a = SimpleNamespace(**dict(zip(names_in, refs)))
    o = SimpleNamespace(**dict(zip(names_out, refs[count_in:])))
    s = SimpleNamespace(**dict(zip(names_scratch, refs[count_in + count_out :])))
    me, row = lax.axis_index(AXIS), lax.axis_index(DATA)
    n, across, taps, heads = ex.size, z.across, z.taps, z.heads
    share = z.depth // across
    cells = z.depth // (n * across)
    padded = padded_cells(z, n)
    greet([me ^ r for r in range(1, n)], [row ^ r for r in range(1, across)])
    saved = list(saved_shapes(z))

    def start_loads(layer, late):
        found = weight_loads(s, a, layer, 0) if late else []
        for i, k in enumerate(saved):
            if late == (i == 0):
                found.append(pltpu.make_async_copy(getattr(a, k).at[layer], getattr(s, k), s.save_sem.at[layer, i]))
        for copy in found:
            copy.start()
        return found

    loads = start_loads(LAYERS - 1, False) + start_loads(LAYERS - 1, True)
    size = z.rows // CHUNKS
    s.row_buf[...] = a.sent[...]
    s.grad[...] = a.cotangent[...]
    gather = Gather(ex, z.rows, s.row_buf, s.sent_all, s.gather_send.at[LAYERS - 1], s.gather_recv.at[LAYERS - 1])
    gather.start(*range(CHUNKS))
    tile = a.mean[...]
    for ref in (s.narrow, s.wide, s.gain):
        ref[...] = jnp.zeros_like(ref)
    s.d_pre_v[z.tokens :, :] = jnp.zeros((8, z.inner), F32)
    s.d_pre_s[z.tokens :, :] = jnp.zeros((8, z.both), F32)
    if padded != cells:
        s.state_part[...] = jnp.zeros_like(s.state_part)
    narrow_copies, outs, older = [None] * LAYERS, [], None

    def finish(piece, k, layer):
        s.done[k] = piece.last()
        target = o.g_out.at[layer] if k == 0 else o.g_inner.at[layer, k - 1]
        copy = pltpu.make_async_copy(s.done.at[k], target, s.done_sem.at[layer, k])
        copy.start()
        return copy

    cell_links, cell_sums = [], {}
    cell_rows = LAYERS * across * padded
    state_steps = reduce_steps_of(
        ex, cell_rows, s.state_part, s.state_pair, s.state_stage, s.state_got,
        (s.cell_pair_send, s.cell_pair_recv, s.cell_link_send, s.cell_link_recv), lambda g, own: None, cell_sums.__setitem__, cell_links,
    )
    for layer in range(LAYERS - 1, -1, -1):
        s.mean_own[layer] = tile
        means = []
        for r in range(1, n):
            means.append(
                remote(s.mean_own.at[layer], s.mean_all.at[layer, me], s.mean_send.at[layer, r], s.mean_recv.at[layer, r], me ^ r)
            )
            means[-1].start()
        s.mean_all[layer, me] = tile
        step_rows(z, a, s, layer, 0)
        if layer + 1 == LAYERS:
            build_meta(z.count, a.segments, s.column, s.meta, s.segrow)

        pieces = [
            Piece(
                across, own, s.piece_stage.at[k], s.piece_got.at[layer, k], s.piece_send.at[layer, k], s.piece_recv.at[layer, k]
            )
            for k, own in enumerate((s.own_out, s.own_inner.at[0], s.own_inner.at[1]))
        ]

        def visit(g, layer=layer, means=means, loads=loads, older=older, pieces=pieces):
            if g == 0:
                for copy in loads:
                    copy.wait()
            if g == sum(ex.links):
                if older is not None:
                    older[2].phase(1)
                    for k in range(2):
                        for j in range(2, len(older[k].order)):
                            older[k].phase(j)
                    outs.append(finish(older[0], 0, layer + 1))
                for i in range(across):
                    s.own_out[i] = t_dot(s.scaled[...], s.sent_all[:, i * share : (i + 1) * share]).astype(BF)
                pieces[0].phase(0)
            here = group_rows(ex, g, z.rows)
            first = (me ^ g) // 2 * 2
            for r in (g, g ^ 1):
                if r:
                    means[r - 1].wait_recv()
            mean = jnp.concatenate([column_of(s.mean_all[layer, first]), column_of(s.mean_all[layer, first + 1])], axis=0)
            at = slice(layer, layer + 1)
            grad_scaled = dot_t(s.sent_all[here, :], s.wout[0])
            gate, y = s.gate[here, :], s.y[here, :]
            gate_sig = sigmoid(gate)
            silu_gate = gate * gate_sig
            gated = y * silu_gate
            s.narrow[layer, taps + 1 : taps + 2, :] += jnp.sum(grad_scaled * gated, axis=0, keepdims=True)
            grad_gated = grad_scaled * a.gate_gain[at, :] + (2.0 / z.inner_all) * mean * gated
            s.rg[here, :] = (grad_gated * y * (gate_sig * (1.0 + gate * (1.0 - gate_sig)))).astype(BF)
            s.dy[here, :] = grad_gated * silu_gate

        sent = gather.run(visit)
        if older is not None:
            outs.append(finish(older[1], 1, layer + 1))
        for i in range(across):
            s.own_inner[0, i] = t_dot(s.normed[:, i * share : (i + 1) * share], s.rg[...]).astype(BF)
        pieces[1].phase(0)
        mix_backward(z, layer, s, a, s.meta, s.segrow)
        for copy in sent + means:
            copy.wait_send()
        loads = start_loads(layer - 1, False) if layer else []
        if older is not None:
            for k in range(2, len(older[2].order)):
                older[2].phase(k)
            outs.append(finish(older[2], 2, layer + 1))
        pieces[0].phase(1)
        narrow_copies[layer] = exchange(
            s.narrow.at[layer], s.narrow_got.at[layer], s.narrow_send.at[layer], s.narrow_recv.at[layer], row, across, DATA
        )

        def value_grads(pieces=pieces):
            for i in range(across):
                s.own_inner[1, i] = t_dot(s.normed[:, i * share : (i + 1) * share], s.rv[...]).astype(BF)
            pieces[2].phase(0)

        def state_grads(layer=layer):
            for i in range(across):
                here = slice(i * share, (i + 1) * share)
                state = t_dot(s.normed[:, here], s.rs[...])
                for j in range(n):
                    to = ((j * LAYERS + layer) * across + i) * padded
                    s.state_part[to : to + cells, :] = state[j * cells : (j + 1) * cells, :].astype(BF)
                s.step_part[layer, i, 0:heads, :] = t_dot(s.rd[...], s.normed[:, here])

        if layer == 0:
            value_grads()

        def idle(t, layer=layer, pieces=pieces, value_grads=value_grads, state_grads=state_grads):
            if t == 1:
                if layer:
                    value_grads()
                else:
                    state_grads()
            elif t == 2 and layer:
                state_grads()
            elif t == 3:
                pieces[1].phase(1)
            if t >= 2 and not layer:
                next(state_steps)

        def produce(g, own, layer=layer):
            if own:
                return
            here = group_rows(ex, g, z.rows)
            total = dot_t(s.rg[here, :], s.win[0, 0]) + dot_t(s.rv[here, :], s.win[0, 1])
            total = total + dot_t(s.rs[here, :], s.wst[0]) + dot(s.rd[here, :], s.wstep[0].astype(BF))
            s.part[here, :] = total.astype(BF)

        after = Gather(ex, z.rows, s.row_buf, s.sent_all, s.gather_send.at[layer - 1], s.gather_recv.at[layer - 1]) if layer else None
        found = []

        def final(q, value, layer=layer, after=after, found=found):
            rows = slice(q * size, (q + 1) * size)
            resid = a.resids[layer - 1, rows, :] if layer else a.residual[rows, :]
            fresh, gain_grad = norm_backward(value, resid, s.grad[rows, :], a.norm_gain[layer : layer + 1, :])
            mean = None
            if layer:
                mixed, gate = a.mixeds[layer - 1, rows, :], a.gates[layer - 1, rows, :]
                s.row_buf[rows, :] = (gate * fresh).astype(BF)
                after.start(q)
                s.grad[rows, :] = fresh
                mean = -0.5 * gate * gate * jnp.sum(mixed * fresh, axis=1, keepdims=True)
            else:
                o.input_grad[rows, :] = fresh
            found.append((q, gain_grad, mean))

        links = []
        reduce_rows(
            ex, z.rows, s.part, s.pair, s.stage, s.got,
            (s.pair_send.at[layer], s.pair_recv.at[layer], s.link_send.at[layer], s.link_recv.at[layer]), produce, final, links, idle=idle,
        )
        found.sort(key=lambda item: item[0])
        gain_grad = sum(item[1] for item in found)
        eighth = z.depth // 8
        for k in range(8):
            s.gain[layer, k : k + 1, :] = gain_grad[:, k * eighth : (k + 1) * eighth]
        for copy in links:
            copy.wait_send()
        if layer:
            tile = tile_of(jnp.concatenate([item[2] for item in found], axis=0))
            loads = loads + start_loads(layer - 1, True)
            gather = after
            older = pieces
    gains = exchange(s.gain, s.gain_got, s.gain_send, s.gain_recv, me, n, AXIS)
    wides = exchange(s.wide, s.wide_got, s.wide_send, s.wide_recv, me, n, AXIS)
    for _ in state_steps:
        pass
    state = jnp.concatenate([cell_sums[q] for q in range(CHUNKS)], axis=0)
    s.gain_mid[...] = collected(s.gain[...], s.gain_got, gains)
    s.wide_mid[...] = collected(s.wide[...], s.wide_got, wides)
    gains_two = exchange(s.gain_mid, s.gain_two, s.gain_send_two, s.gain_recv_two, row, across, DATA)
    wides_two = exchange(s.wide_mid, s.wide_two, s.wide_send_two, s.wide_recv_two, row, across, DATA)
    for layer in range(LAYERS):
        for i in range(across):
            at = (layer * across + i) * padded
            s.cell_own[i, layer * padded : (layer + 1) * padded, :] = state[at : at + padded, :].astype(BF)
            s.step_own[i, layer * 16 : layer * 16 + 8, :] = s.step_part[layer, i].astype(BF)
    cell = Piece(across, s.cell_own, s.cell_stage, s.cell_got, s.cell_send, s.cell_recv)
    step = Piece(across, s.step_own, s.step_stage, s.step_got, s.step_send, s.step_recv)
    cell.phase(0)
    step.phase(0)
    for copy in outs:
        copy.wait()
    for j in range(2, len(pieces[0].order)):
        pieces[0].phase(j)
    last = [finish(pieces[0], 0, 0)]
    pieces[2].phase(1)
    for k in range(1, len(cell.order)):
        cell.phase(k)
        step.phase(k)
    for j in range(2, len(pieces[1].order)):
        pieces[1].phase(j)
    last.append(finish(pieces[1], 1, 0))
    for layer in range(LAYERS):
        o.narrow[layer] = collected(s.narrow[layer], s.narrow_got.at[layer], narrow_copies[layer])
    o.gain[...] = collected(s.gain_mid[...], s.gain_two, gains_two)
    o.wide[...] = collected(s.wide_mid[...], s.wide_two, wides_two)
    state, steps = cell.last(), step.last()
    for layer in range(LAYERS):
        o.g_state[layer] = state[layer * padded : layer * padded + cells, :]
        o.g_step[layer] = steps[layer * 16 : layer * 16 + 8, :]
    for j in range(2, len(pieces[2].order)):
        pieces[2].phase(j)
    last.append(finish(pieces[2], 2, 0))
    for copy in cell_links + gains + wides + gains_two + wides_two + [c for copies in narrow_copies for c in copies]:
        copy.wait_send()
    for copy in last:
        copy.wait()


def padded_cells(z, n):
    cells = z.depth // (n * z.across)
    return -(-cells // 16) * 16


def piece_slots(across):
    order = [1 << b for b in range(across.bit_length() - 1)]
    return len(reduce_steps(order)), len(arrival_slots(order))


def backward_pass(ex, z, forward, residual, cotangent, segments, w):
    n, across = ex.size, z.across
    share = z.depth // across
    if share != z.inner:
        raise ValueError(share)
    saved = saved_shapes(z)
    rows = (z.rows, z.depth)
    inputs = dict(
        residual=(residual, True), cotangent=(cotangent, True), sent=(forward.sent, True), mean=(forward.mean, True),
        resids=(forward.resids, True), mixeds=(forward.mixeds, True), gates=(forward.gates, True),
        segments=(segments, True), **small_inputs(w),
    )
    for k in saved:
        inputs[k] = (getattr(forward, k), False)
    cells, padded = z.depth // (n * across), padded_cells(z, n)
    narrow, wide, gain = (LAYERS, 16, z.inner), (LAYERS, 8, z.both), (LAYERS, 8, z.depth // 8)
    outputs = dict(
        input_grad=(rows, F32, True),
        g_inner=((LAYERS, 2, share, z.inner), F32, False), g_out=((LAYERS, z.inner, share), F32, False),
        g_state=((LAYERS, cells, z.both), F32, True), g_step=((LAYERS, 8, share), F32, True),
        narrow=(narrow, F32, True), wide=(wide, F32, True), gain=(gain, F32, True),
    )
    scratch = {k: pltpu.VMEM(shape, kind) for k, (shape, kind) in saved.items()}
    scratch.update(weight_scratch(z, 1))
    scratch.update(meta_scratch(z))
    scratch.update(reduce_scratch(ex, z.rows, z.depth))
    slots = n // 2
    stages, arrivals = piece_slots(across)
    cell_rows = LAYERS * across * padded
    state = {"state_" + k: v for k, v in reduce_scratch(ex, cell_rows, z.both).items()}
    scratch.update(
        state_part=pltpu.VMEM((n * cell_rows, z.both), BF), **state,
        sent_all=pltpu.VMEM((z.tokens, z.depth), BF), part=pltpu.VMEM((z.tokens, z.depth), BF), row_buf=pltpu.VMEM(rows, BF),
        dy=pltpu.VMEM((z.tokens, z.inner), F32), rg=pltpu.VMEM((z.tokens, z.inner), BF), rv=pltpu.VMEM((z.tokens, z.inner), BF),
        rs=pltpu.VMEM((z.tokens, z.both), BF), rd=pltpu.VMEM((z.tokens, z.heads), BF), state=pltpu.VMEM((z.half, z.inner), F32),
        d_pre_v=pltpu.VMEM((z.tokens + 8, z.inner), F32), d_pre_s=pltpu.VMEM((z.tokens + 8, z.both), F32),
        mean_own=pltpu.VMEM((LAYERS, 8, z.rows), F32), mean_all=pltpu.VMEM((LAYERS, n, 8, z.rows), F32),
        mean_send=dma(LAYERS, n), mean_recv=dma(LAYERS, n), save_sem=dma(LAYERS, len(saved)),
        own_out=pltpu.VMEM((across, z.inner, share), BF), own_inner=pltpu.VMEM((2, across, share, z.inner), BF),
        piece_stage=pltpu.VMEM((3, stages, share, z.inner), BF), piece_got=pltpu.VMEM((LAYERS, 3, arrivals, share, z.inner), BF),
        piece_send=dma(LAYERS, 3, stages), piece_recv=dma(LAYERS, 3, arrivals),
        done=pltpu.VMEM((3, share, z.inner), F32), done_sem=dma(LAYERS, 3),
        narrow=pltpu.VMEM(narrow, F32), narrow_got=pltpu.VMEM((LAYERS, across) + narrow[1:], F32),
        narrow_send=dma(LAYERS, across), narrow_recv=dma(LAYERS, across),
        wide=pltpu.VMEM(wide, F32), wide_mid=pltpu.VMEM(wide, F32),
        wide_got=pltpu.VMEM((n,) + wide, F32), wide_two=pltpu.VMEM((across,) + wide, F32),
        gain=pltpu.VMEM(gain, F32), gain_mid=pltpu.VMEM(gain, F32),
        gain_got=pltpu.VMEM((n,) + gain, F32), gain_two=pltpu.VMEM((across,) + gain, F32),
        wide_send=dma(n), wide_recv=dma(n), gain_send=dma(n), gain_recv=dma(n),
        wide_send_two=dma(across), wide_recv_two=dma(across), gain_send_two=dma(across), gain_recv_two=dma(across),
        step_part=pltpu.VMEM((LAYERS, across, 8, share), F32), step_own=pltpu.VMEM((across, LAYERS * 16, share), BF),
        step_stage=pltpu.VMEM((stages, LAYERS * 16, share), BF), step_got=pltpu.VMEM((arrivals, LAYERS * 16, share), BF),
        step_send=dma(stages), step_recv=dma(arrivals),
        cell_own=pltpu.VMEM((across, LAYERS * padded, z.both), BF),
        cell_stage=pltpu.VMEM((stages, LAYERS * padded, z.both), BF), cell_got=pltpu.VMEM((arrivals, LAYERS * padded, z.both), BF),
        cell_send=dma(stages), cell_recv=dma(arrivals),
        cell_pair_send=dma(slots), cell_pair_recv=dma(slots), cell_link_send=dma(CHUNKS * slots),
        cell_link_recv=dma(CHUNKS * (slots - 1)), grad=pltpu.VMEM(rows, F32),
        gather_send=dma(LAYERS, CHUNKS, n), gather_recv=dma(LAYERS, CHUNKS, n),
        pair_send=dma(LAYERS, slots), pair_recv=dma(LAYERS, slots),
        link_send=dma(LAYERS, CHUNKS * slots), link_recv=dma(LAYERS, CHUNKS * (slots - 1)),
    )
    return run_kernel(backward_kernel, ex, z, inputs, outputs, scratch, 1, "backward")


def final_kernel(z, n, *refs):
    block, grad, inner, out, state, step, narrow, wide, gain = refs[:9]
    (o_block, o_grad, o_norm, o_inner, o_state, o_step, o_bias, o_decay, o_skip, o_conv, o_cbias, o_sconv, o_sbias, o_gate, o_out) = refs[9:]
    o_block[...] = block[...]
    o_grad[...] = grad[...]
    o_inner[...] = inner[...]
    o_out[...] = out[...]

    @pl.when(pl.program_id(0) == 0)
    def _():
        taps, heads = z.taps, z.heads
        o_state[...] = state[...]
        cells, eighth = o_norm.shape[1], gain.shape[2]
        per = eighth // cells
        device = lax.axis_index(DATA) * n + lax.axis_index(AXIS)
        pick = lax.broadcasted_iota(jnp.int32, (eighth, cells), 0)
        pick = (pick == lax.broadcasted_iota(jnp.int32, (eighth, cells), 1) + (device % per) * cells).astype(F32)
        line = lax.broadcasted_iota(jnp.int32, (8, eighth), 0) == device // per
        ones = head_sum_matrix(z.inner, heads, z.width).astype(F32)
        for layer in range(LAYERS):
            at = slice(layer, layer + 1)
            row = jnp.sum(jnp.where(line, gain[layer], 0.0), axis=0, keepdims=True)
            o_norm[at, :] = exact(jnp.broadcast_to(row, (8, eighth)), pick)[0:1, :]
            lines = narrow[layer]
            for h in range(heads):
                o_step[h, at, :] = step[layer, h : h + 1, :]
            skip = jnp.broadcast_to(lines[taps + 2 : taps + 3, :], (8, z.inner))
            o_skip[at, :] = exact(skip, ones)[0:1, :]
            o_bias[at, :] = lines[taps + 3 : taps + 4, 0:heads]
            o_decay[at, :] = lines[taps + 4 : taps + 5, 0:heads]
            o_conv[layer] = lines[0:taps, :]
            o_cbias[at, :] = lines[taps : taps + 1, :]
            o_gate[at, :] = lines[taps + 1 : taps + 2, :]
            o_sconv[layer] = wide[layer, 0:taps, :]
            o_sbias[at, :] = wide[layer, taps : taps + 1, :]


def final_pass(ex, z, block_output, b):
    share, both, heads, taps, inner = z.depth // z.across, z.both, z.heads, z.taps, z.inner
    cells = z.depth // (ex.size * z.across)
    steps = 2 if z.rows % 16 == 0 and share % 16 == 0 and inner % 16 == 0 else 1
    whole = lambda shape: pl.BlockSpec(shape, lambda i: (0,) * len(shape))
    rows = pl.BlockSpec((z.rows // steps, z.depth), lambda i: (i, 0))
    inner_spec = pl.BlockSpec((LAYERS, 2, share // steps, inner), lambda i: (0, 0, i, 0))
    out_spec = pl.BlockSpec((LAYERS, inner // steps, share), lambda i: (0, i, 0))
    arrays = (block_output, b.input_grad, b.g_inner, b.g_out, b.g_state, b.g_step, b.narrow, b.wide, b.gain)
    small = [
        (LAYERS, cells, both), (heads, LAYERS, share), (LAYERS, heads), (LAYERS, heads), (LAYERS, heads), (LAYERS, taps, inner),
        (LAYERS, inner), (LAYERS, taps, both), (LAYERS, both), (LAYERS, inner),
    ]
    shapes = [(z.rows, z.depth), (z.rows, z.depth), (LAYERS, cells), b.g_inner.shape] + small + [b.g_out.shape]
    return pl.pallas_call(
        functools.partial(final_kernel, z, ex.size),
        grid=(steps,),
        out_shape=tuple(jax.ShapeDtypeStruct(shape, F32) for shape in shapes),
        in_specs=[rows, rows, inner_spec, out_spec] + [whole(v.shape) for v in arrays[4:]],
        out_specs=tuple([rows, rows, whole((LAYERS, cells)), inner_spec] + [whole(shape) for shape in small] + [out_spec]),
        compiler_params=pltpu.CompilerParams(vmem_limit_bytes=VM),
        cost_estimate=cost_of(1 << 20),
        name="final",
    )(*arrays)


def sizes_of(ex, across, residual, segments, w):
    inner = w.inner_weight.shape[3]
    return Sizes(
        segments.shape[1], residual.shape[0], residual.shape[1], inner, w.step_weight.shape[2], w.state_weight.shape[2],
        w.conv_weight.shape[1], inner * ex.size, across,
    )


def shards(ex, across, residual, cotangent, segments, *weights):
    w = Weights(*weights)
    z = sizes_of(ex, across, residual, segments, w)
    w = w._replace(step_weight=jnp.transpose(w.step_weight, (2, 0, 1)))
    f = forward_pass(ex, z, residual, cotangent, segments, w)
    b = backward_pass(ex, z, f, residual, cotangent, segments, w)
    made = list(final_pass(ex, z, f.block_output, b))
    made[5] = jnp.transpose(made[5], (1, 2, 0))
    return tuple(made)


def solution(mesh):
    ex = Cube(mesh.shape[AXIS])
    both, rest = (DATA, AXIS), None
    return jax.shard_map(
        functools.partial(shards, ex, mesh.shape[DATA]),
        mesh=mesh,
        in_specs=(
            P(both, rest),
            P(both, rest),
            P(DATA, rest),
            P(),
            P(rest, rest, rest, AXIS),
            P(),
            P(rest, rest, AXIS),
            P(rest, AXIS),
            P(rest, AXIS),
            P(rest, AXIS),
            P(rest, rest, AXIS),
            P(rest, AXIS),
            P(),
            P(),
            P(rest, AXIS),
            P(rest, AXIS, rest),
        ),
        out_specs=(
            P(both, rest),
            P(both, rest),
            P(rest, both),
            P(rest, rest, DATA, AXIS),
            P(rest, both, rest),
            P(rest, DATA, AXIS),
            P(rest, AXIS),
            P(rest, AXIS),
            P(rest, AXIS),
            P(rest, rest, AXIS),
            P(rest, AXIS),
            P(),
            P(),
            P(rest, AXIS),
            P(rest, AXIS, DATA),
        ),
        check_vma=False,
    )
```

```python
import functools
from types import SimpleNamespace
from typing import NamedTuple

import jax
import jax.numpy as jnp
from jax import lax
from jax.experimental import pallas as pl
from jax.experimental.pallas import tpu as pltpu
from jax.sharding import PartitionSpec as P

LAYERS = 2
SIZE = 128
CHUNKS = 2
AXIS = "tensor"
DATA = "dp"
EPS = 1e-05
HIGH = lax.Precision.HIGHEST
F32 = jnp.float32
BF = jnp.bfloat16
VM = 67_000_000


def cost_of(flops, moved=1 << 24):
    return pl.CostEstimate(flops=flops, bytes_accessed=moved, transcendentals=0)


class Weights(NamedTuple):
    norm_gain: jax.Array
    inner_weight: jax.Array
    state_weight: jax.Array
    step_weight: jax.Array
    step_bias: jax.Array
    decay_log: jax.Array
    skip_gain: jax.Array
    conv_weight: jax.Array
    conv_bias: jax.Array
    state_conv_weight: jax.Array
    state_conv_bias: jax.Array
    gate_gain: jax.Array
    out_weight: jax.Array


def dot(a, b):
    return lax.dot_general(a, b, (((1,), (0,)), ((), ())), preferred_element_type=F32)


def dot_t(a, b):
    return lax.dot_general(a, b, (((1,), (1,)), ((), ())), preferred_element_type=F32)


def t_dot(a, b):
    return lax.dot_general(a, b, (((0,), (0,)), ((), ())), preferred_element_type=F32)


def exact(a, b):
    return lax.dot_general(
        a, b, (((1,), (0,)), ((), ())), preferred_element_type=F32, precision=HIGH
    )


def masked_sum(mask, value, parts=3):
    ones = mask.astype(BF)
    total = None
    for _ in range(parts):
        part = value.astype(BF)
        total = dot(ones, part) if total is None else total + dot(ones, part)
        value = value - part.astype(F32)
    return total


def sigmoid(x):
    return 1.0 / (1.0 + jnp.exp(-x))


def softplus(x):
    return jnp.maximum(x, 0.0) + jnp.log1p(jnp.exp(-jnp.abs(x)))


def tiles_of(inner, width):
    return [
        (start, min(128, inner - start), start // width, min(128, inner - start) // width)
        for start in range(0, inner, 128)
    ]


def expand(cols, inner, width):
    rows, heads = cols.shape
    if rows > 8:
        row = lax.broadcasted_iota(jnp.int32, (heads, inner), 0)
        col = lax.broadcasted_iota(jnp.int32, (heads, inner), 1)
        ones = ((col >= row * width) & (col < (row + 1) * width)).astype(BF)
        high = cols.astype(BF)
        return dot(high, ones) + dot((cols - high.astype(F32)).astype(BF), ones)
    parts = []
    for _, wide, first, number in tiles_of(inner, width):
        lane = lax.broadcasted_iota(jnp.int32, (rows, wide), 1)
        value = jnp.broadcast_to(cols[:, first : first + 1], (rows, wide))
        for j in range(1, number):
            value = jnp.where(lane >= j * width, cols[:, first + j : first + j + 1], value)
        parts.append(value)
    return parts[0] if len(parts) == 1 else jnp.concatenate(parts, axis=1)


def head_sum_matrix(inner, heads, width):
    row = lax.broadcasted_iota(jnp.int32, (inner, heads), 0)
    col = lax.broadcasted_iota(jnp.int32, (inner, heads), 1)
    return ((row >= col * width) & (row < (col + 1) * width)).astype(BF)


def head_sum(value, inner, heads, width, parts=1):
    ones = head_sum_matrix(inner, heads, width)
    high = value.astype(BF)
    if parts == 1:
        return dot(high, ones)
    return dot(high, ones) + dot((value - high.astype(F32)).astype(BF), ones)


def head_split(tile, width, number):
    if number == 1:
        return tile
    lane = lax.broadcasted_iota(jnp.int32, tile.shape, 1)
    zero = jnp.zeros_like(tile)
    return jnp.concatenate(
        [
            jnp.where((lane >= j * width) & (lane < (j + 1) * width), tile, zero)
            for j in range(number)
        ],
        axis=0,
    )


def pair_mask(seg_col, seg_row):
    rows, cols = seg_col.shape[0], seg_row.shape[1]
    row = lax.broadcasted_iota(jnp.int32, (rows, cols), 0)
    col = lax.broadcasted_iota(jnp.int32, (rows, cols), 1)
    return (row >= col) & (seg_col == seg_row)


def lower_ones(size):
    row = lax.broadcasted_iota(jnp.int32, (size, size), 0)
    col = lax.broadcasted_iota(jnp.int32, (size, size), 1)
    return (row >= col).astype(F32)


def turned(value):
    return jnp.transpose(value)


def column_of(tile):
    rows = tile.shape[1]
    return jnp.transpose(jnp.broadcast_to(tile[0:1, :], (rows, rows)))[:, 0:1]


def tile_of(column):
    rows = column.shape[0]
    return jnp.transpose(jnp.broadcast_to(column, (rows, rows)))[0:8, :]


def later_ones(seg_col, seg_row):
    rows, cols = seg_col.shape[0], seg_row.shape[1]
    row = lax.broadcasted_iota(jnp.int32, (rows, cols), 0)
    col = lax.broadcasted_iota(jnp.int32, (rows, cols), 1)
    return ((row <= col) & (seg_col == seg_row)).astype(F32)


def earlier_ones(seg_col, seg_row):
    rows, cols = seg_col.shape[0], seg_row.shape[1]
    row = lax.broadcasted_iota(jnp.int32, (rows, cols), 0)
    col = lax.broadcasted_iota(jnp.int32, (rows, cols), 1)
    return ((row > col) & (seg_col == seg_row)).astype(F32)


def build_meta(count, seg_ref, column, meta, segrow):
    row = seg_ref[...].astype(F32)
    segrow[0:1, :] = row
    wide = column.shape[1]
    column[0:8, :] = jnp.full((8, wide), -1.0, F32)
    for c in range(count):
        part = row[:, c * SIZE : (c + 1) * SIZE]
        column[8 + c * SIZE : 8 + (c + 1) * SIZE, :] = jnp.transpose(jnp.broadcast_to(part, (SIZE, SIZE)))
    lane = lax.broadcasted_iota(jnp.int32, (SIZE, wide), 1)
    for c in range(count):
        first = 8 + c * SIZE
        now = column[first : first + SIZE, :]
        before = column[first - 1 : first, :]
        end = column[first + SIZE - 1 : first + SIZE, :]
        value = now
        for k in range(1, 4):
            kept = (column[first - k : first - k + SIZE, :] == now).astype(F32)
            value = jnp.where(lane == k, kept, value)
        value = jnp.where(lane == 4, (now == before).astype(F32), value)
        value = jnp.where(lane == 5, (now == end).astype(F32), value)
        value = jnp.where(lane == 6, jnp.broadcast_to((end == before).astype(F32), (SIZE, wide)), value)
        meta[c * SIZE : (c + 1) * SIZE, :] = value[:, 0:8]
    meta[count * SIZE :, :] = jnp.zeros((8, 8), F32)


def span_of(dims):
    found = [0]
    for d in dims:
        found = found + [r ^ d for r in found]
    return found


def most_first(offsets):
    return sorted(offsets, key=lambda r: -bin(r).count("1"))


class Cube:
    def __init__(self, size):
        self.size = size
        self.links = [1 << b for b in range(1, size.bit_length() - 1)]
        self.orders = [self.links, self.links[::-1]]
        self.offsets = most_first(span_of(self.links))

    def gather_dims(self, q):
        return self.orders[q % 2] + [1]

    def gather_last(self, q, r):
        return max([i for i, d in enumerate(self.gather_dims(q)) if r & d], default=-1)

    def gather_steps(self, q):
        found = [r for r in span_of(self.links) if r]
        return sorted(found, key=lambda r: (self.gather_last(q, r), r & (r - 1) != 0))


def reduce_steps(order):
    steps = []
    for i, d in enumerate(order):
        for s in most_first(span_of(order[i + 1 :])):
            steps.append((i, d ^ s))
    return steps + [(len(order), 0)]


def arrival_slots(order, first=0):
    found = {}
    for i, r in reduce_steps(order):
        for j in range(i):
            found[(j, r)] = first + len(found)
    return found


def remote(src, dst, send, recv, target, axis=AXIS):
    return pltpu.make_async_remote_copy(
        src_ref=src, dst_ref=dst, send_sem=send, recv_sem=recv,
        device_id={axis: target}, device_id_type=pl.DeviceIdType.MESH,
    )


def greet(targets, across=()):
    barrier = pltpu.get_barrier_semaphore()
    for axis, group in ((AXIS, targets), (DATA, across)):
        for target in group:
            pl.semaphore_signal(barrier, inc=1, device_id={axis: target}, device_id_type=pl.DeviceIdType.MESH)
    pl.semaphore_wait(barrier, len(targets) + len(across))


def rows_of(block, rows, many=1):
    return pl.ds(pl.multiple_of(block * rows, rows), rows * many)


def dma(*shape):
    return pltpu.SemaphoreType.DMA(shape)


class Gather:
    def __init__(self, ex, rows, row_buf, out, send_sem, recv_sem):
        self.ex, self.rows, self.row_buf, self.out = ex, rows, row_buf, out
        self.send_sem, self.recv_sem = send_sem, recv_sem
        self.me = lax.axis_index(AXIS)
        self.copies, self.arrived = {}, set()

    def hops(self, q, r):
        dims, part = self.ex.gather_dims(q), self.rows // CHUNKS
        place = pl.ds(pl.multiple_of((self.me ^ r) * self.rows + q * part, part), part)
        src = self.row_buf.at[pl.ds(q * part, part), :] if r == 0 else self.out.at[place, :]
        found = []
        for i in range(self.ex.gather_last(q, r) + 1, len(dims)):
            b = r ^ dims[i]
            found.append((b, remote(src, self.out.at[place, :], self.send_sem.at[q, b], self.recv_sem.at[q, b], self.me ^ dims[i])))
        return found

    def start(self, *pieces):
        part = self.rows // CHUNKS
        hops = [self.hops(q, 0) for q in pieces]
        for step in zip(*hops):
            for q, (b, copy) in zip(pieces, step):
                copy.start()
                self.copies[(q, b)] = copy
        for q in pieces:
            here = pl.ds(pl.multiple_of(self.me * self.rows + q * part, part), part)
            self.out[here, :] = self.row_buf[q * part : (q + 1) * part, :]

    def need(self, q, r):
        if (q, r) not in self.arrived:
            self.copies[(q, r)].wait_recv()
            self.arrived.add((q, r))
            for b, copy in self.hops(q, r):
                copy.start()
                self.copies[(q, b)] = copy

    def run(self, visit):
        ex = self.ex
        steps = [ex.gather_steps(q) for q in range(CHUNKS)]
        visits = sorted(span_of(ex.links), key=lambda g: (ex.gather_last(0, g), g & (g - 1) != 0))
        k = 0
        for g in visits:
            while g and not all((q, g) in self.arrived for q in range(CHUNKS)):
                for q in range(CHUNKS):
                    self.need(q, steps[q][k])
                k += 1
            for q in range(CHUNKS):
                self.need(q, g ^ 1)
            visit(g)
        return list(self.copies.values())


def reduce_scratch(ex, rows, depth):
    slots, part = ex.size // 2, rows // CHUNKS
    return dict(
        pair=pltpu.VMEM((slots, rows, depth), BF),
        stage=pltpu.VMEM((CHUNKS * slots, part, depth), BF),
        got=pltpu.VMEM((CHUNKS * (slots - 1), part, depth), BF),
    )


def reduce_rows(*args, idle=None, ahead=True):
    for t, _ in enumerate(reduce_steps_of(*args, ahead=ahead)):
        if idle is not None:
            idle(t)


def reduce_steps_of(ex, rows, part, pair, stage, got, sems, produce, final, pending, ahead=True):
    me = lax.axis_index(AXIS)
    pair_send, pair_recv, link_send, link_recv = sems
    n, size = ex.size, rows // CHUNKS
    slot_of = {r: i for i, r in enumerate(ex.offsets)}
    orders = [ex.orders[q % 2] for q in range(CHUNKS)]
    steps = [reduce_steps(order) for order in orders]
    slots = [arrival_slots(order, q * (n // 2 - 1)) for q, order in enumerate(orders)]
    waiting = list(ex.offsets)
    pairs, ready, arrivals = {}, set(), {}

    def advance():
        r = waiting.pop(0)
        produce(r, False)
        i = slot_of[r]
        pairs[r] = remote(part.at[rows_of(me ^ r ^ 1, rows), :], pair.at[i], pair_send.at[i], pair_recv.at[i], me ^ 1)
        pairs[r].start()
        produce(r, True)

    def step(q, k):
        i, r = steps[q][k]
        while r not in pairs:
            advance()
        if r not in ready:
            pairs[r].wait_recv()
            ready.add(r)
        own = part[pl.ds(pl.multiple_of((me ^ r) * rows + q * size, size), size), :]
        value = own.astype(F32) + pair[slot_of[r], pl.ds(q * size, size), :].astype(F32)
        for j in range(i):
            arrivals[(q, j, r)].wait_recv()
            value = value + got[slots[q][(j, r)]].astype(F32)
        if r == 0:
            final(q, value)
            return
        d = orders[q][i]
        s = q * (n // 2) + slot_of[r]
        stage[s] = value.astype(BF)
        at = slots[q][(i, r ^ d)]
        copy = remote(stage.at[s], got.at[at], link_send.at[s], link_recv.at[at], me ^ d)
        copy.start()
        arrivals[(q, i, r ^ d)] = copy
        pending.append(copy)

    advance()
    waves = CHUNKS // 2
    for t in range(len(steps[0]) + waves - 1):
        if waiting and ahead:
            advance()
        for p in range(waves):
            if 0 <= t - p < len(steps[0]):
                step(2 * p, t - p)
                step(2 * p + 1, t - p)
        if waiting and not ahead:
            advance()
        if t + 1 == len(steps[0]) + waves - 1:
            pending.extend(pairs.values())
        yield t


def row_scale_of(resid):
    return lax.rsqrt(jnp.mean(resid * resid, axis=1, keepdims=True) + EPS)


def group_rows(ex, g, rows):
    me = lax.axis_index(AXIS)
    return pl.ds(pl.multiple_of(((me ^ g) // 2) * (2 * rows), 2 * rows), 2 * rows)


class Sizes(NamedTuple):
    tokens: int
    rows: int
    depth: int
    inner: int
    heads: int
    both: int
    taps: int
    inner_all: int
    across: int

    @property
    def width(self):
        return self.inner // self.heads

    @property
    def half(self):
        return self.both // 2

    @property
    def count(self):
        return self.tokens // SIZE


def weight_scratch(z, layers):
    return dict(
        win=pltpu.VMEM((layers, 2, z.depth, z.inner), BF),
        wst=pltpu.VMEM((layers, z.depth, z.both), BF),
        wstep=pltpu.VMEM((layers, z.heads, z.depth), F32),
        wout=pltpu.VMEM((layers, z.inner, z.depth), BF),
        weight_sem=dma(LAYERS, 3),
    )


def step_rows(z, a, s, layer, slot):
    for h in range(z.heads):
        s.wstep[slot, h : h + 1, :] = a.step_weight[h, layer : layer + 1, :].astype(F32)


def meta_scratch(z):
    return dict(
        column=pltpu.VMEM((z.tokens + 8, SIZE), F32), meta=pltpu.VMEM((z.tokens + 8, 8), F32), segrow=pltpu.VMEM((8, z.tokens), F32)
    )


def weight_loads(s, a, layer, slot):
    return [
        pltpu.make_async_copy(src.at[layer], dst.at[slot], s.weight_sem.at[layer, i])
        for i, (src, dst) in enumerate(
            ((a.inner_weight, s.win), (a.state_weight, s.wst), (a.out_weight, s.wout))
        )
    ]


def saved_shapes(z):
    t, i = z.tokens, z.inner
    return dict(
        normed=((t, z.depth), BF), gate=((t, i), F32), pre_v=((t, i), F32), y=((t, i), F32), pre_s=((t, z.both), F32),
        step_in=((t, z.heads), F32), value=((t, i), BF), raw=((t, z.both), BF), scaled=((t, i), BF),
        entering=((z.count, z.half, i), BF),
    )


def mix_states(z, layer, s, a, meta):
    at = slice(layer, layer + 1)
    inner, width, half = z.inner, z.width, z.half
    s.state[...] = jnp.zeros_like(s.state)

    def chunk(c, carry):
        rows = pl.ds(pl.multiple_of(c * SIZE, SIZE), SIZE)
        window = pl.ds(pl.multiple_of(c * SIZE, SIZE), SIZE + 8)
        m = meta[rows, :]

        def conv(buf, w_ref, b_ref):
            win = buf[window, :]
            total = b_ref[at, :] + w_ref[layer, 0:1, :] * win[8:, :]
            for k in range(1, z.taps):
                total = total + w_ref[layer, k : k + 1, :] * (win[8 - k : 8 - k + SIZE, :] * m[:, k : k + 1])
            return total, win[8:, :]

        pre_v, value = conv(s.vbuf, a.conv_weight, a.conv_bias)
        pre_s, raw = conv(s.sbuf, a.state_conv_weight, a.state_conv_bias)
        s.value[rows, :] = value.astype(BF)
        s.raw[rows, :] = raw.astype(BF)
        s.pre_v[rows, :] = pre_v
        s.pre_s[rows, :] = pre_s
        x = pre_v * sigmoid(pre_v)
        st = (pre_s * sigmoid(pre_s)).astype(BF)
        dt = softplus(s.step_in[rows, :] + a.step_bias[at, :])
        cum = masked_sum(lower_ones(SIZE), -dt * jnp.exp(a.decay_log[at, :]))
        last = cum[SIZE - 1 : SIZE, :]
        xt = (x * expand(dt, inner, width)).astype(BF)
        s.x[rows, :] = x
        s.xt[rows, :] = xt
        s.states[rows, :] = st
        s.cum[rows, :] = cum
        before = s.state[...]
        s.entering[c] = before.astype(BF)
        to_end = jnp.exp(last - cum) * m[:, 5:6]
        ended = (xt.astype(F32) * expand(to_end, inner, width)).astype(BF)
        s.state[...] = expand(jnp.exp(last) * m[0:1, 6:7], inner, width) * before + t_dot(st[:, :half], ended)
        return carry

    lax.fori_loop(0, z.count, chunk, 0)


def mix_outputs(z, layer, s, a, meta, segrow, c):
    at = slice(layer, layer + 1)
    inner, width, half = z.inner, z.width, z.half
    rows = pl.ds(pl.multiple_of(c * SIZE, SIZE), SIZE)
    m = meta[rows, :]
    st, cum, xt = s.states[rows, :], s.cum[rows, :], s.xt[rows, :]
    b_mat, c_mat = st[:, :half], st[:, half:]
    cum_t = turned(cum)
    from_state = jnp.exp(cum) * m[:, 4:5]
    scores = dot_t(c_mat, b_mat)
    mask = pair_mask(m[:, 0:1], segrow[0:1, rows])
    parts = []
    for start, wide, first, number in tiles_of(inner, width):
        mats = []
        for h in range(first, first + number):
            differ = cum[:, h : h + 1] - cum_t[h : h + 1, :]
            mats.append((jnp.exp(jnp.where(mask, differ, -1e30)) * scores).astype(BF))
        left = mats[0] if number == 1 else jnp.concatenate(mats, axis=1)
        parts.append(dot(left, head_split(xt[:, start : start + wide], width, number)))
    intra = parts[0] if len(parts) == 1 else jnp.concatenate(parts, axis=1)
    inter = dot(c_mat, s.entering[c]) * expand(from_state, inner, width)
    y = intra + inter + expand(a.skip_gain[at, :], inner, width) * s.x[rows, :]
    s.y[rows, :] = y
    gate = s.gate[rows, :]
    gated = y * (gate * sigmoid(gate))
    square = jnp.sum(gated * gated, axis=1, keepdims=True)
    tile = tile_of(square)
    per = SIZE // z.rows if SIZE > z.rows else 1
    wide = SIZE // per
    for k in range(per):
        s.squares[c * per + k] = tile[:, k * wide : (k + 1) * wide]
    s.scaled[rows, :] = (gated * a.gate_gain[at, :]).astype(BF)


def forward_kernel(ex, z, names_in, names_out, names_scratch, *refs):
    count_in, count_out = len(names_in), len(names_out)
    a = SimpleNamespace(**dict(zip(names_in, refs)))
    o = SimpleNamespace(**dict(zip(names_out, refs[count_in:])))
    s = SimpleNamespace(**dict(zip(names_scratch, refs[count_in + count_out :])))
    me = lax.axis_index(AXIS)
    n = ex.size
    greet([me ^ r for r in range(1, n)])
    loads = [weight_loads(s, a, layer, layer) for layer in range(LAYERS)]
    for copy in loads[0] + loads[1]:
        copy.start()
    s.vbuf[0:8, :] = jnp.zeros((8, z.inner), F32)
    s.sbuf[0:8, :] = jnp.zeros((8, z.both), F32)
    saves = []
    size = z.rows // CHUNKS
    gathers = [
        Gather(ex, z.rows, s.row_buf, s.normed.at[layer], s.gather_send.at[layer], s.gather_recv.at[layer]) for layer in range(LAYERS)
    ]
    hidden = a.residual[...]
    s.hidden[...] = hidden
    s.row_buf[...] = (hidden * row_scale_of(hidden) * a.norm_gain[0:1, :]).astype(BF)
    gathers[0].start(*range(CHUNKS))
    build_meta(z.count, a.segments, s.column, s.meta, s.segrow)
    for layer in range(LAYERS):
        step_rows(z, a, s, layer, layer)
    means = []
    for layer in range(LAYERS):
        normed = s.normed.at[layer]

        def project(g, layer=layer, normed=normed):
            if g == 0:
                for copy in loads[layer]:
                    copy.wait()
            here = group_rows(ex, g, z.rows)
            beyond = pl.ds(pl.multiple_of(((me ^ g) // 2) * (2 * z.rows) + 8, 8), 2 * z.rows)
            nb = normed[here, :]
            s.gate[here, :] = dot(nb, s.win[layer, 0])
            s.vbuf[beyond, :] = dot(nb, s.win[layer, 1])
            s.sbuf[beyond, :] = dot(nb, s.wst[layer])
            s.step_in[here, :] = dot_t(nb, s.wstep[layer].astype(BF))

        sent = gathers[layer].run(project)
        mix_states(z, layer, s, a, s.meta)

        def save(late, layer=layer, normed=normed):
            for i, name in enumerate(names_out[: len(saved_shapes(z))]):
                src = normed if i == 0 else getattr(s, name)
                if late == (src is s.y or src is s.scaled):
                    saves.append(pltpu.make_async_copy(src, getattr(o, name).at[layer], s.save_sem.at[layer, i]))
                    saves[-1].start()

        save(False)
        for copy in sent:
            copy.wait_send()
        squares = {}

        def produce(g, own, layer=layer, squares=squares):
            if 2 * z.rows > SIZE:
                block = me ^ g if own else me ^ g ^ 1
                here, first, many = rows_of(block, z.rows), block * (z.rows // SIZE), z.rows // SIZE
            elif not own:
                here, first, many = group_rows(ex, g, z.rows), (me ^ g) // 2, 1
            if own <= (2 * z.rows > SIZE):
                for i in range(many):
                    mix_outputs(z, layer, s, a, s.meta, s.segrow, first + i)
                s.part[here, :] = dot(s.scaled[here, :], s.wout[layer]).astype(BF)
            for r in (g, g ^ 1) if own else ():
                if r:
                    squares[r] = remote(
                        s.squares.at[me ^ r], s.square_got.at[layer, r], s.square_send.at[layer, r], s.square_recv.at[layer, r], me ^ r
                    )
                    squares[r].start()

        def idle(t, save=save):
            if t == 2:
                save(True)

        gates = []

        def final(q, value, layer=layer, squares=squares, gates=gates):
            if not gates:
                square = s.squares[me]
                for r, copy in squares.items():
                    copy.wait_recv()
                    square = square + s.square_got[layer, r]
                gates.append(lax.rsqrt(column_of(square) / z.inner_all + EPS))
                if layer + 1 < LAYERS:
                    o.gates[layer] = gates[0]
            rows = slice(q * size, (q + 1) * size)
            gate = gates[0][rows, :]
            mixed = gate * value
            hidden = s.hidden[rows, :] + mixed
            if layer + 1 < LAYERS:
                s.row_buf[rows, :] = (hidden * row_scale_of(hidden) * a.norm_gain[layer + 1 : layer + 2, :]).astype(BF)
                gathers[layer + 1].start(q)
                s.hidden[rows, :] = hidden
                o.resids[layer, rows, :] = hidden
                o.mixeds[layer, rows, :] = mixed
            else:
                grad = a.cotangent[rows, :]
                o.block_output[rows, :] = hidden
                o.sent[rows, :] = (gate * grad).astype(BF)
                means.append((q, -0.5 * gate * gate * jnp.sum(mixed * grad, axis=1, keepdims=True)))

        links = []
        reduce_rows(
            ex, z.rows, s.part, s.pair, s.stage, s.got,
            (s.pair_send.at[layer], s.pair_recv.at[layer], s.link_send.at[layer], s.link_recv.at[layer]), produce, final, links, idle=idle, ahead=False,
        )
        for copy in links + list(squares.values()):
            copy.wait_send()
        for copy in saves:
            copy.wait()
        saves = []
    o.mean[...] = tile_of(jnp.concatenate([v for _, v in sorted(means, key=lambda m: m[0])], axis=0))


def run_kernel(kernel, ex, z, inputs, outputs, scratch, collective, name):
    vm, anywhere = pl.BlockSpec(memory_space=pltpu.VMEM), pl.BlockSpec(memory_space=pl.ANY)
    made = pl.pallas_call(
        functools.partial(kernel, ex, z, tuple(inputs), tuple(outputs), tuple(scratch)),
        out_shape=tuple(jax.ShapeDtypeStruct(shape, kind) for shape, kind, _ in outputs.values()),
        in_specs=[vm if inside else anywhere for _, inside in inputs.values()],
        out_specs=tuple(vm if inside else anywhere for _, _, inside in outputs.values()),
        scratch_shapes=list(scratch.values()),
        compiler_params=pltpu.CompilerParams(collective_id=collective, has_side_effects=True, vmem_limit_bytes=VM),
        cost_estimate=cost_of(1 << 35),
        name=name,
    )(*[array for array, _ in inputs.values()])
    return SimpleNamespace(**dict(zip(outputs, made)))


def small_inputs(w):
    return dict(
        norm_gain=(w.norm_gain, True), step_bias=(w.step_bias, True), decay_log=(w.decay_log, True),
        skip_gain=(w.skip_gain, True), conv_weight=(w.conv_weight, True), conv_bias=(w.conv_bias, True),
        state_conv_weight=(w.state_conv_weight, True), state_conv_bias=(w.state_conv_bias, True), gate_gain=(w.gate_gain, True),
        inner_weight=(w.inner_weight, False), state_weight=(w.state_weight, False), step_weight=(w.step_weight, True),
        out_weight=(w.out_weight, False),
    )


def forward_pass(ex, z, residual, cotangent, segments, w):
    n = ex.size
    saved = saved_shapes(z)
    inputs = dict(residual=(residual, True), cotangent=(cotangent, True), segments=(segments, True), **small_inputs(w))
    rows = (z.rows, z.depth)
    outputs = {k: ((LAYERS,) + shape, kind, False) for k, (shape, kind) in saved.items()}
    outputs.update(
        resids=((LAYERS - 1,) + rows, F32, True), mixeds=((LAYERS - 1,) + rows, F32, True),
        gates=((LAYERS - 1, z.rows, 1), F32, True), block_output=(rows, F32, True),
        sent=(rows, BF, True), mean=((8, z.rows), F32, True),
    )
    scratch = {k: pltpu.VMEM(shape, kind) for k, (shape, kind) in saved.items()}
    scratch.update(normed=pltpu.VMEM((LAYERS, z.tokens, z.depth), BF))
    scratch.update(weight_scratch(z, LAYERS))
    scratch.update(meta_scratch(z))
    scratch.update(reduce_scratch(ex, z.rows, z.depth))
    slots = n // 2
    scratch.update(
        vbuf=pltpu.VMEM((z.tokens + 8, z.inner), F32), sbuf=pltpu.VMEM((z.tokens + 8, z.both), F32),
        x=pltpu.VMEM((z.tokens, z.inner), F32), xt=pltpu.VMEM((z.tokens, z.inner), BF), states=pltpu.VMEM((z.tokens, z.both), BF),
        cum=pltpu.VMEM((z.tokens, z.heads), F32), state=pltpu.VMEM((z.half, z.inner), F32), part=pltpu.VMEM((z.tokens, z.depth), BF), row_buf=pltpu.VMEM(rows, BF),
        squares=pltpu.VMEM((n, 8, z.rows), F32), square_got=pltpu.VMEM((LAYERS, n, 8, z.rows), F32),
        square_send=dma(LAYERS, n), square_recv=dma(LAYERS, n), save_sem=dma(LAYERS, len(saved)),
        gather_send=dma(LAYERS, CHUNKS, n), gather_recv=dma(LAYERS, CHUNKS, n),
        pair_send=dma(LAYERS, slots), pair_recv=dma(LAYERS, slots), hidden=pltpu.VMEM(rows, F32),
        link_send=dma(LAYERS, CHUNKS * slots), link_recv=dma(LAYERS, CHUNKS * (slots - 1)),
    )
    return run_kernel(forward_kernel, ex, z, inputs, outputs, scratch, 0, "forward")


class Piece:
    def __init__(self, across, own, stage, got, send, recv):
        self.order = [1 << b for b in range(across.bit_length() - 1)]
        self.own, self.stage, self.got, self.send, self.recv = own, stage, got, send, recv
        self.slots = arrival_slots(self.order)
        self.row = lax.axis_index(DATA)
        self.arrivals, self.sent = {}, []

    def value(self, i, r):
        total = self.own[self.row ^ r].astype(F32)
        for j in range(i):
            self.arrivals[(j, r)].wait_recv()
            total = total + self.got[self.slots[(j, r)]].astype(F32)
        return total

    def phase(self, k):
        for number, (i, r) in enumerate(reduce_steps(self.order)):
            if i != k or r == 0:
                continue
            src = self.own.at[self.row ^ r]
            if i:
                self.stage[number] = self.value(i, r).astype(BF)
                src = self.stage.at[number]
            d = self.order[i]
            at = self.slots[(i, r ^ d)]
            copy = remote(src, self.got.at[at], self.send.at[number], self.recv.at[at], self.row ^ d, DATA)
            copy.start()
            self.arrivals[(i, r ^ d)] = copy
            self.sent.append(copy)

    def last(self):
        total = self.value(len(self.order), 0)
        for copy in self.sent:
            copy.wait_send()
        return total


def mix_backward(z, layer, s, a, meta, segrow):
    at = slice(layer, layer + 1)
    inner, width, half, heads, taps = z.inner, z.width, z.half, z.heads, z.taps
    s.state[...] = jnp.zeros_like(s.state)
    group = 2 if z.count % 2 == 0 else 1

    def chunk(c, after):
        rows = pl.ds(pl.multiple_of(c * SIZE, SIZE), SIZE)
        m = meta[rows, :]
        y, dy = s.y[rows, :], s.dy[rows, :]
        pre_v, pre_s = s.pre_v[rows, :], s.pre_s[rows, :]
        sig_v, sig_s = sigmoid(pre_v), sigmoid(pre_s)
        x = pre_v * sig_v
        st = pre_s * sig_s
        b_mat = st[:, :half].astype(BF)
        c_mat = st[:, half:].astype(BF)
        raw_step = s.step_in[rows, :] + a.step_bias[at, :]
        dt = softplus(raw_step)
        rate = jnp.exp(a.decay_log[at, :])
        log_decay = -dt * rate
        cum = masked_sum(lower_ones(SIZE), log_decay)
        cum_t = turned(cum)
        last = cum[SIZE - 1 : SIZE, :]
        dt_all = expand(dt, inner, width)
        skip_all = expand(a.skip_gain[at, :], inner, width)
        xt = (x * dt_all).astype(BF)
        dy_b = dy.astype(BF)
        from_state = expand(jnp.exp(cum) * m[:, 4:5], inner, width)
        to_end = expand(jnp.exp(last - cum) * m[:, 5:6], inner, width)
        carry = expand(jnp.exp(last) * m[0:1, 6:7], inner, width)
        scores = dot_t(c_mat, b_mat)
        mask = pair_mask(m[:, 0:1], segrow[0:1, rows])
        d_scores = jnp.zeros((SIZE, SIZE), F32)
        parts = []
        for start, wide, first, number in tiles_of(inner, width):
            dy_split = head_split(dy_b[:, start : start + wide], width, number)
            d_mats = dot_t(dy_split, xt[:, start : start + wide])
            mats = []
            for j in range(number):
                h = first + j
                differ = cum[:, h : h + 1] - cum_t[h : h + 1, :]
                decay = jnp.exp(jnp.where(mask, differ, -1e30))
                mats.append((decay * scores).astype(BF))
                d_scores = d_scores + d_mats[j * SIZE : (j + 1) * SIZE, :] * decay
            left = mats[0] if number == 1 else jnp.concatenate(mats, axis=0)
            parts.append(t_dot(left, dy_split))
        intra = parts[0] if len(parts) == 1 else jnp.concatenate(parts, axis=1)
        d_scores = d_scores.astype(BF)
        before = s.entering[c]
        after_b = after.astype(BF)
        dy_in = (dy * from_state).astype(BF)
        xt_f = xt.astype(F32)
        ended = (xt_f * to_end).astype(BF)
        from_later = dot(b_mat, after_b) * to_end
        d_xt = intra + from_later
        d_c = dot(d_scores, b_mat) + dot_t(dy_in, before)
        d_b = t_dot(d_scores, c_mat) + dot_t(ended, after_b)
        across = carry * jnp.sum(before.astype(F32) * after, axis=0, keepdims=True)
        fresh = carry * after + t_dot(c_mat, dy_in)
        pairs = head_sum(dy_b.astype(F32) * (y - skip_all * x) - xt_f * intra, inner, heads, width, 2)
        sums = head_sum(
            jnp.concatenate([xt_f * from_later, x * d_xt, jnp.broadcast_to(across, (8, inner))], axis=0), inner, heads, width
        )
        seg_col, seg_row = m[:, 0:1], segrow[0:1, rows]
        d_log = (
            masked_sum(later_ones(seg_col, seg_row), pairs, 2)
            + masked_sum(earlier_ones(seg_col, seg_row), sums[0:SIZE], 2)
            + sums[2 * SIZE : 2 * SIZE + 1]
        )
        d_raw = (sums[SIZE : 2 * SIZE] - rate * d_log) * sigmoid(raw_step)
        s.rd[rows, :] = d_raw.astype(BF)
        d_x = dy * skip_all + d_xt * dt_all
        s.d_pre_v[rows, :] = d_x * (sig_v * (1.0 + pre_v * (1.0 - sig_v)))
        d_st = jnp.concatenate([d_b, d_c], axis=1)
        s.d_pre_s[rows, :] = d_st * (sig_s * (1.0 + pre_s * (1.0 - sig_s)))
        total = lambda v: jnp.sum(v, axis=0, keepdims=True)
        return fresh, (total(dy * x), total(d_raw), total(d_log * log_decay))

    def body(i, sums):
        after = s.state[...]
        for k in range(group):
            after, more = chunk(z.count - 1 - (i * group + k), after)
            sums = tuple(u + v for u, v in zip(sums, more))
        s.state[...] = after
        return sums

    zero = lambda wide: jnp.zeros((1, wide), F32)
    skip, bias, decay = lax.fori_loop(0, z.count // group, body, (zero(inner), zero(heads), zero(heads)))
    s.narrow[layer, taps + 2 : taps + 3, :] = skip
    s.narrow[layer, taps + 3 : taps + 4, 0:heads] = bias
    s.narrow[layer, taps + 4 : taps + 5, 0:heads] = decay

    def conv_body(c, sums):
        rows = pl.ds(pl.multiple_of(c * SIZE, SIZE), SIZE)
        window = pl.ds(pl.multiple_of(c * SIZE, SIZE), SIZE + 8)
        m = meta[window, :]
        more = []
        for src, w_ref, value_ref, dst in ((s.d_pre_v, a.conv_weight, s.value, s.rv), (s.d_pre_s, a.state_conv_weight, s.raw, s.rs)):
            win = src[window, :]
            value = value_ref[rows, :].astype(F32)
            now = win[0:SIZE, :]
            total = w_ref[layer, 0:1, :] * now
            lines = [jnp.sum(now * value, axis=0, keepdims=True)]
            for k in range(1, taps):
                moved = win[k : k + SIZE, :] * m[k : k + SIZE, k : k + 1]
                total = total + w_ref[layer, k : k + 1, :] * moved
                lines.append(jnp.sum(moved * value, axis=0, keepdims=True))
            lines.append(jnp.sum(now, axis=0, keepdims=True))
            dst[rows, :] = total.astype(BF)
            more.extend(lines)
        return tuple(u + v for u, v in zip(sums, more))

    lines = lax.fori_loop(0, z.count, conv_body, (zero(inner),) * (taps + 1) + (zero(z.both),) * (taps + 1))
    for k in range(taps + 1):
        s.narrow[layer, k : k + 1, :] = lines[k]
        s.wide[layer, k : k + 1, :] = lines[taps + 1 + k]


def norm_backward(total, resid, grad, gain):
    scale = row_scale_of(resid)
    weighted = total * gain
    inner = jnp.sum(weighted * resid, axis=1, keepdims=True)
    gain_grad = jnp.sum(total * resid * scale, axis=0, keepdims=True)
    return grad + scale * weighted - resid * (scale * scale * scale * inner / resid.shape[1]), gain_grad


def exchange(src, got, send, recv, place, number, axis):
    copies = [remote(src, got.at[r], send.at[r], recv.at[r], place ^ r, axis) for r in range(1, number)]
    for copy in copies:
        copy.start()
    return copies


def collected(own, got, copies):
    total = own
    for r, copy in enumerate(copies, 1):
        copy.wait_recv()
        total = total + got[r]
    return total


def backward_kernel(ex, z, names_in, names_out, names_scratch, *refs):
    count_in, count_out = len(names_in), len(names_out)
    a = SimpleNamespace(**dict(zip(names_in, refs)))
    o = SimpleNamespace(**dict(zip(names_out, refs[count_in:])))
    s = SimpleNamespace(**dict(zip(names_scratch, refs[count_in + count_out :])))
    me, row = lax.axis_index(AXIS), lax.axis_index(DATA)
    n, across, taps, heads = ex.size, z.across, z.taps, z.heads
    share = z.depth // across
    cells = z.depth // (n * across)
    padded = padded_cells(z, n)
    greet([me ^ r for r in range(1, n)], [row ^ r for r in range(1, across)])
    saved = list(saved_shapes(z))

    def start_loads(layer, late):
        found = weight_loads(s, a, layer, 0) if late else []
        for i, k in enumerate(saved):
            if late == (i == 0):
                found.append(pltpu.make_async_copy(getattr(a, k).at[layer], getattr(s, k), s.save_sem.at[layer, i]))
        for copy in found:
            copy.start()
        return found

    loads = start_loads(LAYERS - 1, False) + start_loads(LAYERS - 1, True)
    size = z.rows // CHUNKS
    s.row_buf[...] = a.sent[...]
    s.grad[...] = a.cotangent[...]
    gather = Gather(ex, z.rows, s.row_buf, s.sent_all, s.gather_send.at[LAYERS - 1], s.gather_recv.at[LAYERS - 1])
    gather.start(*range(CHUNKS))
    tile = a.mean[...]
    for ref in (s.narrow, s.wide, s.gain):
        ref[...] = jnp.zeros_like(ref)
    s.d_pre_v[z.tokens :, :] = jnp.zeros((8, z.inner), F32)
    s.d_pre_s[z.tokens :, :] = jnp.zeros((8, z.both), F32)
    if padded != cells:
        s.state_part[...] = jnp.zeros_like(s.state_part)
    narrow_copies, outs, older = [None] * LAYERS, [], None

    def finish(piece, k, layer):
        s.done[k] = piece.last()
        target = o.g_out.at[layer] if k == 0 else o.g_inner.at[layer, k - 1]
        copy = pltpu.make_async_copy(s.done.at[k], target, s.done_sem.at[layer, k])
        copy.start()
        return copy

    cell_links, cell_sums = [], {}
    cell_rows = LAYERS * across * padded
    state_steps = reduce_steps_of(
        ex, cell_rows, s.state_part, s.state_pair, s.state_stage, s.state_got,
        (s.cell_pair_send, s.cell_pair_recv, s.cell_link_send, s.cell_link_recv), lambda g, own: None, cell_sums.__setitem__, cell_links,
    )
    for layer in range(LAYERS - 1, -1, -1):
        s.mean_own[layer] = tile
        means = []
        for r in range(1, n):
            means.append(
                remote(s.mean_own.at[layer], s.mean_all.at[layer, me], s.mean_send.at[layer, r], s.mean_recv.at[layer, r], me ^ r)
            )
            means[-1].start()
        s.mean_all[layer, me] = tile
        step_rows(z, a, s, layer, 0)
        if layer + 1 == LAYERS:
            build_meta(z.count, a.segments, s.column, s.meta, s.segrow)

        pieces = [
            Piece(
                across, own, s.piece_stage.at[k], s.piece_got.at[layer, k], s.piece_send.at[layer, k], s.piece_recv.at[layer, k]
            )
            for k, own in enumerate((s.own_out, s.own_inner.at[0], s.own_inner.at[1]))
        ]

        def visit(g, layer=layer, means=means, loads=loads, older=older, pieces=pieces):
            if g == 0:
                for copy in loads:
                    copy.wait()
            if g == sum(ex.links):
                if older is not None:
                    older[2].phase(1)
                    for k in range(2):
                        for j in range(2, len(older[k].order)):
                            older[k].phase(j)
                    outs.append(finish(older[0], 0, layer + 1))
                for i in range(across):
                    s.own_out[i] = t_dot(s.scaled[...], s.sent_all[:, i * share : (i + 1) * share]).astype(BF)
                pieces[0].phase(0)
            here = group_rows(ex, g, z.rows)
            first = (me ^ g) // 2 * 2
            for r in (g, g ^ 1):
                if r:
                    means[r - 1].wait_recv()
            mean = jnp.concatenate([column_of(s.mean_all[layer, first]), column_of(s.mean_all[layer, first + 1])], axis=0)
            at = slice(layer, layer + 1)
            grad_scaled = dot_t(s.sent_all[here, :], s.wout[0])
            gate, y = s.gate[here, :], s.y[here, :]
            gate_sig = sigmoid(gate)
            silu_gate = gate * gate_sig
            gated = y * silu_gate
            s.narrow[layer, taps + 1 : taps + 2, :] += jnp.sum(grad_scaled * gated, axis=0, keepdims=True)
            grad_gated = grad_scaled * a.gate_gain[at, :] + (2.0 / z.inner_all) * mean * gated
            s.rg[here, :] = (grad_gated * y * (gate_sig * (1.0 + gate * (1.0 - gate_sig)))).astype(BF)
            s.dy[here, :] = grad_gated * silu_gate

        sent = gather.run(visit)
        if older is not None:
            outs.append(finish(older[1], 1, layer + 1))
        for i in range(across):
            s.own_inner[0, i] = t_dot(s.normed[:, i * share : (i + 1) * share], s.rg[...]).astype(BF)
        pieces[1].phase(0)
        mix_backward(z, layer, s, a, s.meta, s.segrow)
        for copy in sent + means:
            copy.wait_send()
        loads = start_loads(layer - 1, False) if layer else []
        if older is not None:
            for k in range(2, len(older[2].order)):
                older[2].phase(k)
            outs.append(finish(older[2], 2, layer + 1))
        pieces[0].phase(1)
        narrow_copies[layer] = exchange(
            s.narrow.at[layer], s.narrow_got.at[layer], s.narrow_send.at[layer], s.narrow_recv.at[layer], row, across, DATA
        )

        def value_grads(pieces=pieces):
            for i in range(across):
                s.own_inner[1, i] = t_dot(s.normed[:, i * share : (i + 1) * share], s.rv[...]).astype(BF)
            pieces[2].phase(0)

        def state_grads(layer=layer):
            for i in range(across):
                here = slice(i * share, (i + 1) * share)
                state = t_dot(s.normed[:, here], s.rs[...])
                for j in range(n):
                    to = ((j * LAYERS + layer) * across + i) * padded
                    s.state_part[to : to + cells, :] = state[j * cells : (j + 1) * cells, :].astype(BF)
                s.step_part[layer, i, 0:heads, :] = t_dot(s.rd[...], s.normed[:, here])

        if layer == 0:
            value_grads()

        def idle(t, layer=layer, pieces=pieces, value_grads=value_grads, state_grads=state_grads):
            if t == 1:
                if layer:
                    value_grads()
                else:
                    state_grads()
            elif t == 2 and layer:
                state_grads()
            elif t == 3:
                pieces[1].phase(1)
            if t >= 2 and not layer:
                next(state_steps)

        def produce(g, own, layer=layer):
            if own:
                return
            here = group_rows(ex, g, z.rows)
            total = dot_t(s.rg[here, :], s.win[0, 0]) + dot_t(s.rv[here, :], s.win[0, 1])
            total = total + dot_t(s.rs[here, :], s.wst[0]) + dot(s.rd[here, :], s.wstep[0].astype(BF))
            s.part[here, :] = total.astype(BF)

        after = Gather(ex, z.rows, s.row_buf, s.sent_all, s.gather_send.at[layer - 1], s.gather_recv.at[layer - 1]) if layer else None
        found = []

        def final(q, value, layer=layer, after=after, found=found):
            rows = slice(q * size, (q + 1) * size)
            resid = a.resids[layer - 1, rows, :] if layer else a.residual[rows, :]
            fresh, gain_grad = norm_backward(value, resid, s.grad[rows, :], a.norm_gain[layer : layer + 1, :])
            mean = None
            if layer:
                mixed, gate = a.mixeds[layer - 1, rows, :], a.gates[layer - 1, rows, :]
                s.row_buf[rows, :] = (gate * fresh).astype(BF)
                after.start(q)
                s.grad[rows, :] = fresh
                mean = -0.5 * gate * gate * jnp.sum(mixed * fresh, axis=1, keepdims=True)
            else:
                o.input_grad[rows, :] = fresh
            found.append((q, gain_grad, mean))

        links = []
        reduce_rows(
            ex, z.rows, s.part, s.pair, s.stage, s.got,
            (s.pair_send.at[layer], s.pair_recv.at[layer], s.link_send.at[layer], s.link_recv.at[layer]), produce, final, links, idle=idle,
        )
        found.sort(key=lambda item: item[0])
        gain_grad = sum(item[1] for item in found)
        eighth = z.depth // 8
        for k in range(8):
            s.gain[layer, k : k + 1, :] = gain_grad[:, k * eighth : (k + 1) * eighth]
        for copy in links:
            copy.wait_send()
        if layer:
            tile = tile_of(jnp.concatenate([item[2] for item in found], axis=0))
            loads = loads + start_loads(layer - 1, True)
            gather = after
            older = pieces
    gains = exchange(s.gain, s.gain_got, s.gain_send, s.gain_recv, me, n, AXIS)
    wides = exchange(s.wide, s.wide_got, s.wide_send, s.wide_recv, me, n, AXIS)
    for _ in state_steps:
        pass
    state = jnp.concatenate([cell_sums[q] for q in range(CHUNKS)], axis=0)
    s.gain_mid[...] = collected(s.gain[...], s.gain_got, gains)
    s.wide_mid[...] = collected(s.wide[...], s.wide_got, wides)
    gains_two = exchange(s.gain_mid, s.gain_two, s.gain_send_two, s.gain_recv_two, row, across, DATA)
    wides_two = exchange(s.wide_mid, s.wide_two, s.wide_send_two, s.wide_recv_two, row, across, DATA)
    for layer in range(LAYERS):
        for i in range(across):
            at = (layer * across + i) * padded
            s.cell_own[i, layer * padded : (layer + 1) * padded, :] = state[at : at + padded, :].astype(BF)
            s.step_own[i, layer * 16 : layer * 16 + 8, :] = s.step_part[layer, i].astype(BF)
    cell = Piece(across, s.cell_own, s.cell_stage, s.cell_got, s.cell_send, s.cell_recv)
    step = Piece(across, s.step_own, s.step_stage, s.step_got, s.step_send, s.step_recv)
    cell.phase(0)
    step.phase(0)
    for copy in outs:
        copy.wait()
    for j in range(2, len(pieces[0].order)):
        pieces[0].phase(j)
    last = [finish(pieces[0], 0, 0)]
    pieces[2].phase(1)
    for k in range(1, len(cell.order)):
        cell.phase(k)
        step.phase(k)
    for j in range(2, len(pieces[1].order)):
        pieces[1].phase(j)
    last.append(finish(pieces[1], 1, 0))
    for layer in range(LAYERS):
        o.narrow[layer] = collected(s.narrow[layer], s.narrow_got.at[layer], narrow_copies[layer])
    o.gain[...] = collected(s.gain_mid[...], s.gain_two, gains_two)
    o.wide[...] = collected(s.wide_mid[...], s.wide_two, wides_two)
    state, steps = cell.last(), step.last()
    for layer in range(LAYERS):
        o.g_state[layer] = state[layer * padded : layer * padded + cells, :]
        o.g_step[layer] = steps[layer * 16 : layer * 16 + 8, :]
    for j in range(2, len(pieces[2].order)):
        pieces[2].phase(j)
    last.append(finish(pieces[2], 2, 0))
    for copy in cell_links + gains + wides + gains_two + wides_two + [c for copies in narrow_copies for c in copies]:
        copy.wait_send()
    for copy in last:
        copy.wait()


def padded_cells(z, n):
    cells = z.depth // (n * z.across)
    return -(-cells // 16) * 16


def piece_slots(across):
    order = [1 << b for b in range(across.bit_length() - 1)]
    return len(reduce_steps(order)), len(arrival_slots(order))


def backward_pass(ex, z, forward, residual, cotangent, segments, w):
    n, across = ex.size, z.across
    share = z.depth // across
    if share != z.inner:
        raise ValueError(share)
    saved = saved_shapes(z)
    rows = (z.rows, z.depth)
    inputs = dict(
        residual=(residual, True), cotangent=(cotangent, True), sent=(forward.sent, True), mean=(forward.mean, True),
        resids=(forward.resids, True), mixeds=(forward.mixeds, True), gates=(forward.gates, True),
        segments=(segments, True), **small_inputs(w),
    )
    for k in saved:
        inputs[k] = (getattr(forward, k), False)
    cells, padded = z.depth // (n * across), padded_cells(z, n)
    narrow, wide, gain = (LAYERS, 16, z.inner), (LAYERS, 8, z.both), (LAYERS, 8, z.depth // 8)
    outputs = dict(
        input_grad=(rows, F32, True),
        g_inner=((LAYERS, 2, share, z.inner), F32, False), g_out=((LAYERS, z.inner, share), F32, False),
        g_state=((LAYERS, cells, z.both), F32, True), g_step=((LAYERS, 8, share), F32, True),
        narrow=(narrow, F32, True), wide=(wide, F32, True), gain=(gain, F32, True),
    )
    scratch = {k: pltpu.VMEM(shape, kind) for k, (shape, kind) in saved.items()}
    scratch.update(weight_scratch(z, 1))
    scratch.update(meta_scratch(z))
    scratch.update(reduce_scratch(ex, z.rows, z.depth))
    slots = n // 2
    stages, arrivals = piece_slots(across)
    cell_rows = LAYERS * across * padded
    state = {"state_" + k: v for k, v in reduce_scratch(ex, cell_rows, z.both).items()}
    scratch.update(
        state_part=pltpu.VMEM((n * cell_rows, z.both), BF), **state,
        sent_all=pltpu.VMEM((z.tokens, z.depth), BF), part=pltpu.VMEM((z.tokens, z.depth), BF), row_buf=pltpu.VMEM(rows, BF),
        dy=pltpu.VMEM((z.tokens, z.inner), F32), rg=pltpu.VMEM((z.tokens, z.inner), BF), rv=pltpu.VMEM((z.tokens, z.inner), BF),
        rs=pltpu.VMEM((z.tokens, z.both), BF), rd=pltpu.VMEM((z.tokens, z.heads), BF), state=pltpu.VMEM((z.half, z.inner), F32),
        d_pre_v=pltpu.VMEM((z.tokens + 8, z.inner), F32), d_pre_s=pltpu.VMEM((z.tokens + 8, z.both), F32),
        mean_own=pltpu.VMEM((LAYERS, 8, z.rows), F32), mean_all=pltpu.VMEM((LAYERS, n, 8, z.rows), F32),
        mean_send=dma(LAYERS, n), mean_recv=dma(LAYERS, n), save_sem=dma(LAYERS, len(saved)),
        own_out=pltpu.VMEM((across, z.inner, share), BF), own_inner=pltpu.VMEM((2, across, share, z.inner), BF),
        piece_stage=pltpu.VMEM((3, stages, share, z.inner), BF), piece_got=pltpu.VMEM((LAYERS, 3, arrivals, share, z.inner), BF),
        piece_send=dma(LAYERS, 3, stages), piece_recv=dma(LAYERS, 3, arrivals),
        done=pltpu.VMEM((3, share, z.inner), F32), done_sem=dma(LAYERS, 3),
        narrow=pltpu.VMEM(narrow, F32), narrow_got=pltpu.VMEM((LAYERS, across) + narrow[1:], F32),
        narrow_send=dma(LAYERS, across), narrow_recv=dma(LAYERS, across),
        wide=pltpu.VMEM(wide, F32), wide_mid=pltpu.VMEM(wide, F32),
        wide_got=pltpu.VMEM((n,) + wide, F32), wide_two=pltpu.VMEM((across,) + wide, F32),
        gain=pltpu.VMEM(gain, F32), gain_mid=pltpu.VMEM(gain, F32),
        gain_got=pltpu.VMEM((n,) + gain, F32), gain_two=pltpu.VMEM((across,) + gain, F32),
        wide_send=dma(n), wide_recv=dma(n), gain_send=dma(n), gain_recv=dma(n),
        wide_send_two=dma(across), wide_recv_two=dma(across), gain_send_two=dma(across), gain_recv_two=dma(across),
        step_part=pltpu.VMEM((LAYERS, across, 8, share), F32), step_own=pltpu.VMEM((across, LAYERS * 16, share), BF),
        step_stage=pltpu.VMEM((stages, LAYERS * 16, share), BF), step_got=pltpu.VMEM((arrivals, LAYERS * 16, share), BF),
        step_send=dma(stages), step_recv=dma(arrivals),
        cell_own=pltpu.VMEM((across, LAYERS * padded, z.both), BF),
        cell_stage=pltpu.VMEM((stages, LAYERS * padded, z.both), BF), cell_got=pltpu.VMEM((arrivals, LAYERS * padded, z.both), BF),
        cell_send=dma(stages), cell_recv=dma(arrivals),
        cell_pair_send=dma(slots), cell_pair_recv=dma(slots), cell_link_send=dma(CHUNKS * slots),
        cell_link_recv=dma(CHUNKS * (slots - 1)), grad=pltpu.VMEM(rows, F32),
        gather_send=dma(LAYERS, CHUNKS, n), gather_recv=dma(LAYERS, CHUNKS, n),
        pair_send=dma(LAYERS, slots), pair_recv=dma(LAYERS, slots),
        link_send=dma(LAYERS, CHUNKS * slots), link_recv=dma(LAYERS, CHUNKS * (slots - 1)),
    )
    return run_kernel(backward_kernel, ex, z, inputs, outputs, scratch, 1, "backward")


def final_kernel(z, n, *refs):
    block, grad, inner, out, state, step, narrow, wide, gain = refs[:9]
    (o_block, o_grad, o_norm, o_inner, o_state, o_step, o_bias, o_decay, o_skip, o_conv, o_cbias, o_sconv, o_sbias, o_gate, o_out) = refs[9:]
    o_block[...] = block[...]
    o_grad[...] = grad[...]
    o_inner[...] = inner[...]
    o_out[...] = out[...]

    @pl.when(pl.program_id(0) == 0)
    def _():
        taps, heads = z.taps, z.heads
        o_state[...] = state[...]
        cells, eighth = o_norm.shape[1], gain.shape[2]
        per = eighth // cells
        device = lax.axis_index(DATA) * n + lax.axis_index(AXIS)
        pick = lax.broadcasted_iota(jnp.int32, (eighth, cells), 0)
        pick = (pick == lax.broadcasted_iota(jnp.int32, (eighth, cells), 1) + (device % per) * cells).astype(F32)
        line = lax.broadcasted_iota(jnp.int32, (8, eighth), 0) == device // per
        ones = head_sum_matrix(z.inner, heads, z.width).astype(F32)
        for layer in range(LAYERS):
            at = slice(layer, layer + 1)
            row = jnp.sum(jnp.where(line, gain[layer], 0.0), axis=0, keepdims=True)
            o_norm[at, :] = exact(jnp.broadcast_to(row, (8, eighth)), pick)[0:1, :]
            lines = narrow[layer]
            for h in range(heads):
                o_step[h, at, :] = step[layer, h : h + 1, :]
            skip = jnp.broadcast_to(lines[taps + 2 : taps + 3, :], (8, z.inner))
            o_skip[at, :] = exact(skip, ones)[0:1, :]
            o_bias[at, :] = lines[taps + 3 : taps + 4, 0:heads]
            o_decay[at, :] = lines[taps + 4 : taps + 5, 0:heads]
            o_conv[layer] = lines[0:taps, :]
            o_cbias[at, :] = lines[taps : taps + 1, :]
            o_gate[at, :] = lines[taps + 1 : taps + 2, :]
            o_sconv[layer] = wide[layer, 0:taps, :]
            o_sbias[at, :] = wide[layer, taps : taps + 1, :]


def final_pass(ex, z, block_output, b):
    share, both, heads, taps, inner = z.depth // z.across, z.both, z.heads, z.taps, z.inner
    cells = z.depth // (ex.size * z.across)
    steps = 2 if z.rows % 16 == 0 and share % 16 == 0 and inner % 16 == 0 else 1
    whole = lambda shape: pl.BlockSpec(shape, lambda i: (0,) * len(shape))
    rows = pl.BlockSpec((z.rows // steps, z.depth), lambda i: (i, 0))
    inner_spec = pl.BlockSpec((LAYERS, 2, share // steps, inner), lambda i: (0, 0, i, 0))
    out_spec = pl.BlockSpec((LAYERS, inner // steps, share), lambda i: (0, i, 0))
    arrays = (block_output, b.input_grad, b.g_inner, b.g_out, b.g_state, b.g_step, b.narrow, b.wide, b.gain)
    small = [
        (LAYERS, cells, both), (heads, LAYERS, share), (LAYERS, heads), (LAYERS, heads), (LAYERS, heads), (LAYERS, taps, inner),
        (LAYERS, inner), (LAYERS, taps, both), (LAYERS, both), (LAYERS, inner),
    ]
    shapes = [(z.rows, z.depth), (z.rows, z.depth), (LAYERS, cells), b.g_inner.shape] + small + [b.g_out.shape]
    return pl.pallas_call(
        functools.partial(final_kernel, z, ex.size),
        grid=(steps,),
        out_shape=tuple(jax.ShapeDtypeStruct(shape, F32) for shape in shapes),
        in_specs=[rows, rows, inner_spec, out_spec] + [whole(v.shape) for v in arrays[4:]],
        out_specs=tuple([rows, rows, whole((LAYERS, cells)), inner_spec] + [whole(shape) for shape in small] + [out_spec]),
        compiler_params=pltpu.CompilerParams(vmem_limit_bytes=VM),
        cost_estimate=cost_of(1 << 20),
        name="final",
    )(*arrays)


def sizes_of(ex, across, residual, segments, w):
    inner = w.inner_weight.shape[3]
    return Sizes(
        segments.shape[1], residual.shape[0], residual.shape[1], inner, w.step_weight.shape[2], w.state_weight.shape[2],
        w.conv_weight.shape[1], inner * ex.size, across,
    )


def shards(ex, across, residual, cotangent, segments, *weights):
    w = Weights(*weights)
    z = sizes_of(ex, across, residual, segments, w)
    w = w._replace(step_weight=jnp.transpose(w.step_weight, (2, 0, 1)))
    f = forward_pass(ex, z, residual, cotangent, segments, w)
    b = backward_pass(ex, z, f, residual, cotangent, segments, w)
    made = list(final_pass(ex, z, f.block_output, b))
    made[5] = jnp.transpose(made[5], (1, 2, 0))
    return tuple(made)


def solution(mesh):
    ex = Cube(mesh.shape[AXIS])
    both, rest = (DATA, AXIS), None
    return jax.shard_map(
        functools.partial(shards, ex, mesh.shape[DATA]),
        mesh=mesh,
        in_specs=(
            P(both, rest),
            P(both, rest),
            P(DATA, rest),
            P(),
            P(rest, rest, rest, AXIS),
            P(),
            P(rest, rest, AXIS),
            P(rest, AXIS),
            P(rest, AXIS),
            P(rest, AXIS),
            P(rest, rest, AXIS),
            P(rest, AXIS),
            P(),
            P(),
            P(rest, AXIS),
            P(rest, AXIS, rest),
        ),
        out_specs=(
            P(both, rest),
            P(both, rest),
            P(rest, both),
            P(rest, rest, DATA, AXIS),
            P(rest, both, rest),
            P(rest, DATA, AXIS),
            P(rest, AXIS),
            P(rest, AXIS),
            P(rest, AXIS),
            P(rest, rest, AXIS),
            P(rest, AXIS),
            P(),
            P(),
            P(rest, AXIS),
            P(rest, AXIS, DATA),
        ),
        check_vma=False,
    )
```

```python
import functools
from types import SimpleNamespace
from typing import NamedTuple

import jax
import jax.numpy as jnp
from jax import lax
from jax.experimental import pallas as pl
from jax.experimental.pallas import tpu as pltpu
from jax.sharding import PartitionSpec as P

LAYERS = 2
SIZE = 128
CHUNKS = 2
AXIS = "tensor"
DATA = "dp"
EPS = 1e-05
HIGH = lax.Precision.HIGHEST
F32 = jnp.float32
BF = jnp.bfloat16
VM = 67_000_000


def cost_of(flops, moved=1 << 24):
    return pl.CostEstimate(flops=flops, bytes_accessed=moved, transcendentals=0)


class Weights(NamedTuple):
    norm_gain: jax.Array
    inner_weight: jax.Array
    state_weight: jax.Array
    step_weight: jax.Array
    step_bias: jax.Array
    decay_log: jax.Array
    skip_gain: jax.Array
    conv_weight: jax.Array
    conv_bias: jax.Array
    state_conv_weight: jax.Array
    state_conv_bias: jax.Array
    gate_gain: jax.Array
    out_weight: jax.Array


def dot(a, b):
    return lax.dot_general(a, b, (((1,), (0,)), ((), ())), preferred_element_type=F32)


def dot_t(a, b):
    return lax.dot_general(a, b, (((1,), (1,)), ((), ())), preferred_element_type=F32)


def t_dot(a, b):
    return lax.dot_general(a, b, (((0,), (0,)), ((), ())), preferred_element_type=F32)


def exact(a, b):
    return lax.dot_general(
        a, b, (((1,), (0,)), ((), ())), preferred_element_type=F32, precision=HIGH
    )


def masked_sum(mask, value, parts=3):
    ones = mask.astype(BF)
    total = None
    for _ in range(parts):
        part = value.astype(BF)
        total = dot(ones, part) if total is None else total + dot(ones, part)
        value = value - part.astype(F32)
    return total


def sigmoid(x):
    return 1.0 / (1.0 + jnp.exp(-x))


def softplus(x):
    return jnp.maximum(x, 0.0) + jnp.log1p(jnp.exp(-jnp.abs(x)))


def tiles_of(inner, width):
    return [
        (start, min(128, inner - start), start // width, min(128, inner - start) // width)
        for start in range(0, inner, 128)
    ]


def expand(cols, inner, width):
    rows, heads = cols.shape
    if rows > 8:
        row = lax.broadcasted_iota(jnp.int32, (heads, inner), 0)
        col = lax.broadcasted_iota(jnp.int32, (heads, inner), 1)
        ones = ((col >= row * width) & (col < (row + 1) * width)).astype(BF)
        high = cols.astype(BF)
        return dot(high, ones) + dot((cols - high.astype(F32)).astype(BF), ones)
    parts = []
    for _, wide, first, number in tiles_of(inner, width):
        lane = lax.broadcasted_iota(jnp.int32, (rows, wide), 1)
        value = jnp.broadcast_to(cols[:, first : first + 1], (rows, wide))
        for j in range(1, number):
            value = jnp.where(lane >= j * width, cols[:, first + j : first + j + 1], value)
        parts.append(value)
    return parts[0] if len(parts) == 1 else jnp.concatenate(parts, axis=1)


def head_sum_matrix(inner, heads, width):
    row = lax.broadcasted_iota(jnp.int32, (inner, heads), 0)
    col = lax.broadcasted_iota(jnp.int32, (inner, heads), 1)
    return ((row >= col * width) & (row < (col + 1) * width)).astype(BF)


def head_sum(value, inner, heads, width, parts=1):
    ones = head_sum_matrix(inner, heads, width)
    high = value.astype(BF)
    if parts == 1:
        return dot(high, ones)
    return dot(high, ones) + dot((value - high.astype(F32)).astype(BF), ones)


def head_split(tile, width, number):
    if number == 1:
        return tile
    lane = lax.broadcasted_iota(jnp.int32, tile.shape, 1)
    zero = jnp.zeros_like(tile)
    return jnp.concatenate(
        [
            jnp.where((lane >= j * width) & (lane < (j + 1) * width), tile, zero)
            for j in range(number)
        ],
        axis=0,
    )


def pair_mask(seg_col, seg_row):
    rows, cols = seg_col.shape[0], seg_row.shape[1]
    row = lax.broadcasted_iota(jnp.int32, (rows, cols), 0)
    col = lax.broadcasted_iota(jnp.int32, (rows, cols), 1)
    return (row >= col) & (seg_col == seg_row)


def lower_ones(size):
    row = lax.broadcasted_iota(jnp.int32, (size, size), 0)
    col = lax.broadcasted_iota(jnp.int32, (size, size), 1)
    return (row >= col).astype(F32)


def turned(value):
    return jnp.transpose(value)


def column_of(tile):
    rows = tile.shape[1]
    return jnp.transpose(jnp.broadcast_to(tile[0:1, :], (rows, rows)))[:, 0:1]


def tile_of(column):
    rows = column.shape[0]
    return jnp.transpose(jnp.broadcast_to(column, (rows, rows)))[0:8, :]


def later_ones(seg_col, seg_row):
    rows, cols = seg_col.shape[0], seg_row.shape[1]
    row = lax.broadcasted_iota(jnp.int32, (rows, cols), 0)
    col = lax.broadcasted_iota(jnp.int32, (rows, cols), 1)
    return ((row <= col) & (seg_col == seg_row)).astype(F32)


def earlier_ones(seg_col, seg_row):
    rows, cols = seg_col.shape[0], seg_row.shape[1]
    row = lax.broadcasted_iota(jnp.int32, (rows, cols), 0)
    col = lax.broadcasted_iota(jnp.int32, (rows, cols), 1)
    return ((row > col) & (seg_col == seg_row)).astype(F32)


def build_meta(count, seg_ref, column, meta, segrow):
    row = seg_ref[...].astype(F32)
    segrow[0:1, :] = row
    wide = column.shape[1]
    column[0:8, :] = jnp.full((8, wide), -1.0, F32)
    for c in range(count):
        part = row[:, c * SIZE : (c + 1) * SIZE]
        column[8 + c * SIZE : 8 + (c + 1) * SIZE, :] = jnp.transpose(jnp.broadcast_to(part, (SIZE, SIZE)))
    lane = lax.broadcasted_iota(jnp.int32, (SIZE, wide), 1)
    for c in range(count):
        first = 8 + c * SIZE
        now = column[first : first + SIZE, :]
        before = column[first - 1 : first, :]
        end = column[first + SIZE - 1 : first + SIZE, :]
        value = now
        for k in range(1, 4):
            kept = (column[first - k : first - k + SIZE, :] == now).astype(F32)
            value = jnp.where(lane == k, kept, value)
        value = jnp.where(lane == 4, (now == before).astype(F32), value)
        value = jnp.where(lane == 5, (now == end).astype(F32), value)
        value = jnp.where(lane == 6, jnp.broadcast_to((end == before).astype(F32), (SIZE, wide)), value)
        meta[c * SIZE : (c + 1) * SIZE, :] = value[:, 0:8]
    meta[count * SIZE :, :] = jnp.zeros((8, 8), F32)


def span_of(dims):
    found = [0]
    for d in dims:
        found = found + [r ^ d for r in found]
    return found


def most_first(offsets):
    return sorted(offsets, key=lambda r: -bin(r).count("1"))


class Cube:
    def __init__(self, size):
        self.size = size
        self.links = [1 << b for b in range(1, size.bit_length() - 1)]
        self.orders = [self.links, self.links[::-1]]
        self.offsets = most_first(span_of(self.links))

    def gather_dims(self, q):
        return self.orders[q % 2] + [1]

    def gather_last(self, q, r):
        return max([i for i, d in enumerate(self.gather_dims(q)) if r & d], default=-1)

    def gather_steps(self, q):
        found = [r for r in span_of(self.links) if r]
        return sorted(found, key=lambda r: (self.gather_last(q, r), r & (r - 1) != 0))


def reduce_steps(order):
    steps = []
    for i, d in enumerate(order):
        for s in most_first(span_of(order[i + 1 :])):
            steps.append((i, d ^ s))
    return steps + [(len(order), 0)]


def arrival_slots(order, first=0):
    found = {}
    for i, r in reduce_steps(order):
        for j in range(i):
            found[(j, r)] = first + len(found)
    return found


def remote(src, dst, send, recv, target, axis=AXIS):
    return pltpu.make_async_remote_copy(
        src_ref=src, dst_ref=dst, send_sem=send, recv_sem=recv,
        device_id={axis: target}, device_id_type=pl.DeviceIdType.MESH,
    )


def greet(targets, across=()):
    barrier = pltpu.get_barrier_semaphore()
    for axis, group in ((AXIS, targets), (DATA, across)):
        for target in group:
            pl.semaphore_signal(barrier, inc=1, device_id={axis: target}, device_id_type=pl.DeviceIdType.MESH)
    pl.semaphore_wait(barrier, len(targets) + len(across))


def rows_of(block, rows, many=1):
    return pl.ds(pl.multiple_of(block * rows, rows), rows * many)


def dma(*shape):
    return pltpu.SemaphoreType.DMA(shape)


class Gather:
    def __init__(self, ex, rows, row_buf, out, send_sem, recv_sem):
        self.ex, self.rows, self.row_buf, self.out = ex, rows, row_buf, out
        self.send_sem, self.recv_sem = send_sem, recv_sem
        self.me = lax.axis_index(AXIS)
        self.copies, self.arrived = {}, set()

    def hops(self, q, r):
        dims, part = self.ex.gather_dims(q), self.rows // CHUNKS
        place = pl.ds(pl.multiple_of((self.me ^ r) * self.rows + q * part, part), part)
        src = self.row_buf.at[pl.ds(q * part, part), :] if r == 0 else self.out.at[place, :]
        found = []
        for i in range(self.ex.gather_last(q, r) + 1, len(dims)):
            b = r ^ dims[i]
            found.append((b, remote(src, self.out.at[place, :], self.send_sem.at[q, b], self.recv_sem.at[q, b], self.me ^ dims[i])))
        return found

    def start(self, *pieces):
        part = self.rows // CHUNKS
        hops = [self.hops(q, 0) for q in pieces]
        for step in zip(*hops):
            for q, (b, copy) in zip(pieces, step):
                copy.start()
                self.copies[(q, b)] = copy
        for q in pieces:
            here = pl.ds(pl.multiple_of(self.me * self.rows + q * part, part), part)
            self.out[here, :] = self.row_buf[q * part : (q + 1) * part, :]

    def need(self, q, r):
        if (q, r) not in self.arrived:
            self.copies[(q, r)].wait_recv()
            self.arrived.add((q, r))
            for b, copy in self.hops(q, r):
                copy.start()
                self.copies[(q, b)] = copy

    def run(self, visit):
        ex = self.ex
        steps = [ex.gather_steps(q) for q in range(CHUNKS)]
        visits = sorted(span_of(ex.links), key=lambda g: (ex.gather_last(0, g), g & (g - 1) != 0))
        k = 0
        for g in visits:
            while g and not all((q, g) in self.arrived for q in range(CHUNKS)):
                for q in range(CHUNKS):
                    self.need(q, steps[q][k])
                k += 1
            for q in range(CHUNKS):
                self.need(q, g ^ 1)
            visit(g)
        return list(self.copies.values())


def reduce_scratch(ex, rows, depth):
    slots, part = ex.size // 2, rows // CHUNKS
    return dict(
        pair=pltpu.VMEM((slots, rows, depth), BF),
        stage=pltpu.VMEM((CHUNKS * slots, part, depth), BF),
        got=pltpu.VMEM((CHUNKS * (slots - 1), part, depth), BF),
    )


def reduce_rows(*args, idle=None, ahead=True):
    for t, _ in enumerate(reduce_steps_of(*args, ahead=ahead)):
        if idle is not None:
            idle(t)


def reduce_steps_of(ex, rows, part, pair, stage, got, sems, produce, final, pending, ahead=True):
    me = lax.axis_index(AXIS)
    pair_send, pair_recv, link_send, link_recv = sems
    n, size = ex.size, rows // CHUNKS
    slot_of = {r: i for i, r in enumerate(ex.offsets)}
    orders = [ex.orders[q % 2] for q in range(CHUNKS)]
    steps = [reduce_steps(order) for order in orders]
    slots = [arrival_slots(order, q * (n // 2 - 1)) for q, order in enumerate(orders)]
    waiting = list(ex.offsets)
    pairs, ready, arrivals = {}, set(), {}

    def advance():
        r = waiting.pop(0)
        produce(r, False)
        i = slot_of[r]
        pairs[r] = remote(part.at[rows_of(me ^ r ^ 1, rows), :], pair.at[i], pair_send.at[i], pair_recv.at[i], me ^ 1)
        pairs[r].start()
        produce(r, True)

    def step(q, k):
        i, r = steps[q][k]
        while r not in pairs:
            advance()
        if r not in ready:
            pairs[r].wait_recv()
            ready.add(r)
        own = part[pl.ds(pl.multiple_of((me ^ r) * rows + q * size, size), size), :]
        value = own.astype(F32) + pair[slot_of[r], pl.ds(q * size, size), :].astype(F32)
        for j in range(i):
            arrivals[(q, j, r)].wait_recv()
            value = value + got[slots[q][(j, r)]].astype(F32)
        if r == 0:
            final(q, value)
            return
        d = orders[q][i]
        s = q * (n // 2) + slot_of[r]
        stage[s] = value.astype(BF)
        at = slots[q][(i, r ^ d)]
        copy = remote(stage.at[s], got.at[at], link_send.at[s], link_recv.at[at], me ^ d)
        copy.start()
        arrivals[(q, i, r ^ d)] = copy
        pending.append(copy)

    advance()
    waves = CHUNKS // 2
    for t in range(len(steps[0]) + waves - 1):
        if waiting and ahead:
            advance()
        for p in range(waves):
            if 0 <= t - p < len(steps[0]):
                step(2 * p, t - p)
                step(2 * p + 1, t - p)
        if waiting and not ahead:
            advance()
        if t + 1 == len(steps[0]) + waves - 1:
            pending.extend(pairs.values())
        yield t


def row_scale_of(resid):
    return lax.rsqrt(jnp.mean(resid * resid, axis=1, keepdims=True) + EPS)


def group_rows(ex, g, rows):
    me = lax.axis_index(AXIS)
    return pl.ds(pl.multiple_of(((me ^ g) // 2) * (2 * rows), 2 * rows), 2 * rows)


class Sizes(NamedTuple):
    tokens: int
    rows: int
    depth: int
    inner: int
    heads: int
    both: int
    taps: int
    inner_all: int
    across: int

    @property
    def width(self):
        return self.inner // self.heads

    @property
    def half(self):
        return self.both // 2

    @property
    def count(self):
        return self.tokens // SIZE


def weight_scratch(z, layers):
    return dict(
        win=pltpu.VMEM((layers, 2, z.depth, z.inner), BF),
        wst=pltpu.VMEM((layers, z.depth, z.both), BF),
        wstep=pltpu.VMEM((layers, z.heads, z.depth), F32),
        wout=pltpu.VMEM((layers, z.inner, z.depth), BF),
        weight_sem=dma(LAYERS, 3),
    )


def step_rows(z, a, s, layer, slot):
    for h in range(z.heads):
        s.wstep[slot, h : h + 1, :] = a.step_weight[h, layer : layer + 1, :].astype(F32)


def meta_scratch(z):
    return dict(
        column=pltpu.VMEM((z.tokens + 8, SIZE), F32), meta=pltpu.VMEM((z.tokens + 8, 8), F32), segrow=pltpu.VMEM((8, z.tokens), F32)
    )


def weight_loads(s, a, layer, slot):
    return [
        pltpu.make_async_copy(src.at[layer], dst.at[slot], s.weight_sem.at[layer, i])
        for i, (src, dst) in enumerate(
            ((a.inner_weight, s.win), (a.state_weight, s.wst), (a.out_weight, s.wout))
        )
    ]


def saved_shapes(z):
    t, i = z.tokens, z.inner
    return dict(
        normed=((t, z.depth), BF), gate=((t, i), F32), pre_v=((t, i), F32), y=((t, i), F32), pre_s=((t, z.both), F32),
        step_in=((t, z.heads), F32), value=((t, i), BF), raw=((t, z.both), BF), scaled=((t, i), BF),
        entering=((z.count, z.half, i), BF),
    )


def mix_states(z, layer, s, a, meta):
    at = slice(layer, layer + 1)
    inner, width, half = z.inner, z.width, z.half
    s.state[...] = jnp.zeros_like(s.state)

    def chunk(c, carry):
        rows = pl.ds(pl.multiple_of(c * SIZE, SIZE), SIZE)
        window = pl.ds(pl.multiple_of(c * SIZE, SIZE), SIZE + 8)
        m = meta[rows, :]

        def conv(buf, w_ref, b_ref):
            win = buf[window, :]
            total = b_ref[at, :] + w_ref[layer, 0:1, :] * win[8:, :]
            for k in range(1, z.taps):
                total = total + w_ref[layer, k : k + 1, :] * (win[8 - k : 8 - k + SIZE, :] * m[:, k : k + 1])
            return total, win[8:, :]

        pre_v, value = conv(s.vbuf, a.conv_weight, a.conv_bias)
        pre_s, raw = conv(s.sbuf, a.state_conv_weight, a.state_conv_bias)
        s.value[rows, :] = value.astype(BF)
        s.raw[rows, :] = raw.astype(BF)
        s.pre_v[rows, :] = pre_v
        s.pre_s[rows, :] = pre_s
        x = pre_v * sigmoid(pre_v)
        st = (pre_s * sigmoid(pre_s)).astype(BF)
        dt = softplus(s.step_in[rows, :] + a.step_bias[at, :])
        cum = masked_sum(lower_ones(SIZE), -dt * jnp.exp(a.decay_log[at, :]))
        last = cum[SIZE - 1 : SIZE, :]
        xt = (x * expand(dt, inner, width)).astype(BF)
        s.x[rows, :] = x
        s.xt[rows, :] = xt
        s.states[rows, :] = st
        s.cum[rows, :] = cum
        before = s.state[...]
        s.entering[c] = before.astype(BF)
        to_end = jnp.exp(last - cum) * m[:, 5:6]
        ended = (xt.astype(F32) * expand(to_end, inner, width)).astype(BF)
        s.state[...] = expand(jnp.exp(last) * m[0:1, 6:7], inner, width) * before + t_dot(st[:, :half], ended)
        return carry

    lax.fori_loop(0, z.count, chunk, 0)


def mix_outputs(z, layer, s, a, meta, segrow, c):
    at = slice(layer, layer + 1)
    inner, width, half = z.inner, z.width, z.half
    rows = pl.ds(pl.multiple_of(c * SIZE, SIZE), SIZE)
    m = meta[rows, :]
    st, cum, xt = s.states[rows, :], s.cum[rows, :], s.xt[rows, :]
    b_mat, c_mat = st[:, :half], st[:, half:]
    cum_t = turned(cum)
    from_state = jnp.exp(cum) * m[:, 4:5]
    scores = dot_t(c_mat, b_mat)
    mask = pair_mask(m[:, 0:1], segrow[0:1, rows])
    parts = []
    for start, wide, first, number in tiles_of(inner, width):
        mats = []
        for h in range(first, first + number):
            differ = cum[:, h : h + 1] - cum_t[h : h + 1, :]
            mats.append((jnp.exp(jnp.where(mask, differ, -1e30)) * scores).astype(BF))
        left = mats[0] if number == 1 else jnp.concatenate(mats, axis=1)
        parts.append(dot(left, head_split(xt[:, start : start + wide], width, number)))
    intra = parts[0] if len(parts) == 1 else jnp.concatenate(parts, axis=1)
    inter = dot(c_mat, s.entering[c]) * expand(from_state, inner, width)
    y = intra + inter + expand(a.skip_gain[at, :], inner, width) * s.x[rows, :]
    s.y[rows, :] = y
    gate = s.gate[rows, :]
    gated = y * (gate * sigmoid(gate))
    square = jnp.sum(gated * gated, axis=1, keepdims=True)
    tile = tile_of(square)
    per = SIZE // z.rows if SIZE > z.rows else 1
    wide = SIZE // per
    for k in range(per):
        s.squares[c * per + k] = tile[:, k * wide : (k + 1) * wide]
    s.scaled[rows, :] = (gated * a.gate_gain[at, :]).astype(BF)


def forward_kernel(ex, z, names_in, names_out, names_scratch, *refs):
    count_in, count_out = len(names_in), len(names_out)
    a = SimpleNamespace(**dict(zip(names_in, refs)))
    o = SimpleNamespace(**dict(zip(names_out, refs[count_in:])))
    s = SimpleNamespace(**dict(zip(names_scratch, refs[count_in + count_out :])))
    me = lax.axis_index(AXIS)
    n = ex.size
    greet([me ^ r for r in range(1, n)])
    loads = [weight_loads(s, a, layer, layer) for layer in range(LAYERS)]
    for copy in loads[0] + loads[1]:
        copy.start()
    s.vbuf[0:8, :] = jnp.zeros((8, z.inner), F32)
    s.sbuf[0:8, :] = jnp.zeros((8, z.both), F32)
    saves = []
    size = z.rows // CHUNKS
    gathers = [
        Gather(ex, z.rows, s.row_buf, s.normed.at[layer], s.gather_send.at[layer], s.gather_recv.at[layer]) for layer in range(LAYERS)
    ]
    hidden = a.residual[...]
    s.hidden[...] = hidden
    s.row_buf[...] = (hidden * row_scale_of(hidden) * a.norm_gain[0:1, :]).astype(BF)
    gathers[0].start(*range(CHUNKS))
    build_meta(z.count, a.segments, s.column, s.meta, s.segrow)
    for layer in range(LAYERS):
        step_rows(z, a, s, layer, layer)
    means = []
    for layer in range(LAYERS):
        normed = s.normed.at[layer]

        def project(g, layer=layer, normed=normed):
            if g == 0:
                for copy in loads[layer]:
                    copy.wait()
            here = group_rows(ex, g, z.rows)
            beyond = pl.ds(pl.multiple_of(((me ^ g) // 2) * (2 * z.rows) + 8, 8), 2 * z.rows)
            nb = normed[here, :]
            s.gate[here, :] = dot(nb, s.win[layer, 0])
            s.vbuf[beyond, :] = dot(nb, s.win[layer, 1])
            s.sbuf[beyond, :] = dot(nb, s.wst[layer])
            s.step_in[here, :] = dot_t(nb, s.wstep[layer].astype(BF))

        sent = gathers[layer].run(project)
        mix_states(z, layer, s, a, s.meta)

        def save(late, layer=layer, normed=normed):
            for i, name in enumerate(names_out[: len(saved_shapes(z))]):
                src = normed if i == 0 else getattr(s, name)
                if late == (src is s.y or src is s.scaled):
                    saves.append(pltpu.make_async_copy(src, getattr(o, name).at[layer], s.save_sem.at[layer, i]))
                    saves[-1].start()

        save(False)
        for copy in sent:
            copy.wait_send()
        squares = {}

        def produce(g, own, layer=layer, squares=squares):
            if 2 * z.rows > SIZE:
                block = me ^ g if own else me ^ g ^ 1
                here, first, many = rows_of(block, z.rows), block * (z.rows // SIZE), z.rows // SIZE
            elif not own:
                here, first, many = group_rows(ex, g, z.rows), (me ^ g) // 2, 1
            if own <= (2 * z.rows > SIZE):
                for i in range(many):
                    mix_outputs(z, layer, s, a, s.meta, s.segrow, first + i)
                s.part[here, :] = dot(s.scaled[here, :], s.wout[layer]).astype(BF)
            for r in (g, g ^ 1) if own else ():
                if r:
                    squares[r] = remote(
                        s.squares.at[me ^ r], s.square_got.at[layer, r], s.square_send.at[layer, r], s.square_recv.at[layer, r], me ^ r
                    )
                    squares[r].start()

        def idle(t, save=save):
            if t == 2:
                save(True)

        gates = []

        def final(q, value, layer=layer, squares=squares, gates=gates):
            if not gates:
                square = s.squares[me]
                for r, copy in squares.items():
                    copy.wait_recv()
                    square = square + s.square_got[layer, r]
                gates.append(lax.rsqrt(column_of(square) / z.inner_all + EPS))
                if layer + 1 < LAYERS:
                    o.gates[layer] = gates[0]
            rows = slice(q * size, (q + 1) * size)
            gate = gates[0][rows, :]
            mixed = gate * value
            hidden = s.hidden[rows, :] + mixed
            if layer + 1 < LAYERS:
                s.row_buf[rows, :] = (hidden * row_scale_of(hidden) * a.norm_gain[layer + 1 : layer + 2, :]).astype(BF)
                gathers[layer + 1].start(q)
                s.hidden[rows, :] = hidden
                o.resids[layer, rows, :] = hidden
                o.mixeds[layer, rows, :] = mixed
            else:
                grad = a.cotangent[rows, :]
                o.block_output[rows, :] = hidden
                o.sent[rows, :] = (gate * grad).astype(BF)
                means.append((q, -0.5 * gate * gate * jnp.sum(mixed * grad, axis=1, keepdims=True)))

        links = []
        reduce_rows(
            ex, z.rows, s.part, s.pair, s.stage, s.got,
            (s.pair_send.at[layer], s.pair_recv.at[layer], s.link_send.at[layer], s.link_recv.at[layer]), produce, final, links, idle=idle, ahead=False,
        )
        for copy in links + list(squares.values()):
            copy.wait_send()
        for copy in saves:
            copy.wait()
        saves = []
    o.mean[...] = tile_of(jnp.concatenate([v for _, v in sorted(means, key=lambda m: m[0])], axis=0))


def run_kernel(kernel, ex, z, inputs, outputs, scratch, collective, name):
    vm, anywhere = pl.BlockSpec(memory_space=pltpu.VMEM), pl.BlockSpec(memory_space=pl.ANY)
    made = pl.pallas_call(
        functools.partial(kernel, ex, z, tuple(inputs), tuple(outputs), tuple(scratch)),
        out_shape=tuple(jax.ShapeDtypeStruct(shape, kind) for shape, kind, _ in outputs.values()),
        in_specs=[vm if inside else anywhere for _, inside in inputs.values()],
        out_specs=tuple(vm if inside else anywhere for _, _, inside in outputs.values()),
        scratch_shapes=list(scratch.values()),
        compiler_params=pltpu.CompilerParams(collective_id=collective, has_side_effects=True, vmem_limit_bytes=VM),
        cost_estimate=cost_of(1 << 35),
        name=name,
    )(*[array for array, _ in inputs.values()])
    return SimpleNamespace(**dict(zip(outputs, made)))


def small_inputs(w):
    return dict(
        norm_gain=(w.norm_gain, True), step_bias=(w.step_bias, True), decay_log=(w.decay_log, True),
        skip_gain=(w.skip_gain, True), conv_weight=(w.conv_weight, True), conv_bias=(w.conv_bias, True),
        state_conv_weight=(w.state_conv_weight, True), state_conv_bias=(w.state_conv_bias, True), gate_gain=(w.gate_gain, True),
        inner_weight=(w.inner_weight, False), state_weight=(w.state_weight, False), step_weight=(w.step_weight, True),
        out_weight=(w.out_weight, False),
    )


def forward_pass(ex, z, residual, cotangent, segments, w):
    n = ex.size
    saved = saved_shapes(z)
    inputs = dict(residual=(residual, True), cotangent=(cotangent, True), segments=(segments, True), **small_inputs(w))
    rows = (z.rows, z.depth)
    outputs = {k: ((LAYERS,) + shape, kind, False) for k, (shape, kind) in saved.items()}
    outputs.update(
        resids=((LAYERS - 1,) + rows, F32, True), mixeds=((LAYERS - 1,) + rows, F32, True),
        gates=((LAYERS - 1, z.rows, 1), F32, True), block_output=(rows, F32, True),
        sent=(rows, BF, True), mean=((8, z.rows), F32, True),
    )
    scratch = {k: pltpu.VMEM(shape, kind) for k, (shape, kind) in saved.items()}
    scratch.update(normed=pltpu.VMEM((LAYERS, z.tokens, z.depth), BF))
    scratch.update(weight_scratch(z, LAYERS))
    scratch.update(meta_scratch(z))
    scratch.update(reduce_scratch(ex, z.rows, z.depth))
    slots = n // 2
    scratch.update(
        vbuf=pltpu.VMEM((z.tokens + 8, z.inner), F32), sbuf=pltpu.VMEM((z.tokens + 8, z.both), F32),
        x=pltpu.VMEM((z.tokens, z.inner), F32), xt=pltpu.VMEM((z.tokens, z.inner), BF), states=pltpu.VMEM((z.tokens, z.both), BF),
        cum=pltpu.VMEM((z.tokens, z.heads), F32), state=pltpu.VMEM((z.half, z.inner), F32), part=pltpu.VMEM((z.tokens, z.depth), BF), row_buf=pltpu.VMEM(rows, BF),
        squares=pltpu.VMEM((n, 8, z.rows), F32), square_got=pltpu.VMEM((LAYERS, n, 8, z.rows), F32),
        square_send=dma(LAYERS, n), square_recv=dma(LAYERS, n), save_sem=dma(LAYERS, len(saved)),
        gather_send=dma(LAYERS, CHUNKS, n), gather_recv=dma(LAYERS, CHUNKS, n),
        pair_send=dma(LAYERS, slots), pair_recv=dma(LAYERS, slots), hidden=pltpu.VMEM(rows, F32),
        link_send=dma(LAYERS, CHUNKS * slots), link_recv=dma(LAYERS, CHUNKS * (slots - 1)),
    )
    return run_kernel(forward_kernel, ex, z, inputs, outputs, scratch, 0, "forward")


class Piece:
    def __init__(self, across, own, stage, got, send, recv):
        self.order = [1 << b for b in range(across.bit_length() - 1)]
        self.own, self.stage, self.got, self.send, self.recv = own, stage, got, send, recv
        self.slots = arrival_slots(self.order)
        self.row = lax.axis_index(DATA)
        self.arrivals, self.sent = {}, []

    def value(self, i, r):
        total = self.own[self.row ^ r].astype(F32)
        for j in range(i):
            self.arrivals[(j, r)].wait_recv()
            total = total + self.got[self.slots[(j, r)]].astype(F32)
        return total

    def phase(self, k):
        for number, (i, r) in enumerate(reduce_steps(self.order)):
            if i != k or r == 0:
                continue
            src = self.own.at[self.row ^ r]
            if i:
                self.stage[number] = self.value(i, r).astype(BF)
                src = self.stage.at[number]
            d = self.order[i]
            at = self.slots[(i, r ^ d)]
            copy = remote(src, self.got.at[at], self.send.at[number], self.recv.at[at], self.row ^ d, DATA)
            copy.start()
            self.arrivals[(i, r ^ d)] = copy
            self.sent.append(copy)

    def last(self):
        total = self.value(len(self.order), 0)
        for copy in self.sent:
            copy.wait_send()
        return total


def mix_backward(z, layer, s, a, meta, segrow):
    at = slice(layer, layer + 1)
    inner, width, half, heads, taps = z.inner, z.width, z.half, z.heads, z.taps
    s.state[...] = jnp.zeros_like(s.state)
    group = 2 if z.count % 2 == 0 else 1

    def chunk(c, after):
        rows = pl.ds(pl.multiple_of(c * SIZE, SIZE), SIZE)
        m = meta[rows, :]
        y, dy = s.y[rows, :], s.dy[rows, :]
        pre_v, pre_s = s.pre_v[rows, :], s.pre_s[rows, :]
        sig_v, sig_s = sigmoid(pre_v), sigmoid(pre_s)
        x = pre_v * sig_v
        st = pre_s * sig_s
        b_mat = st[:, :half].astype(BF)
        c_mat = st[:, half:].astype(BF)
        raw_step = s.step_in[rows, :] + a.step_bias[at, :]
        dt = softplus(raw_step)
        rate = jnp.exp(a.decay_log[at, :])
        log_decay = -dt * rate
        cum = masked_sum(lower_ones(SIZE), log_decay)
        cum_t = turned(cum)
        last = cum[SIZE - 1 : SIZE, :]
        dt_all = expand(dt, inner, width)
        skip_all = expand(a.skip_gain[at, :], inner, width)
        xt = (x * dt_all).astype(BF)
        dy_b = dy.astype(BF)
        from_state = expand(jnp.exp(cum) * m[:, 4:5], inner, width)
        to_end = expand(jnp.exp(last - cum) * m[:, 5:6], inner, width)
        carry = expand(jnp.exp(last) * m[0:1, 6:7], inner, width)
        scores = dot_t(c_mat, b_mat)
        mask = pair_mask(m[:, 0:1], segrow[0:1, rows])
        d_scores = jnp.zeros((SIZE, SIZE), F32)
        parts = []
        for start, wide, first, number in tiles_of(inner, width):
            dy_split = head_split(dy_b[:, start : start + wide], width, number)
            d_mats = dot_t(dy_split, xt[:, start : start + wide])
            mats = []
            for j in range(number):
                h = first + j
                differ = cum[:, h : h + 1] - cum_t[h : h + 1, :]
                decay = jnp.exp(jnp.where(mask, differ, -1e30))
                mats.append((decay * scores).astype(BF))
                d_scores = d_scores + d_mats[j * SIZE : (j + 1) * SIZE, :] * decay
            left = mats[0] if number == 1 else jnp.concatenate(mats, axis=0)
            parts.append(t_dot(left, dy_split))
        intra = parts[0] if len(parts) == 1 else jnp.concatenate(parts, axis=1)
        d_scores = d_scores.astype(BF)
        before = s.entering[c]
        after_b = after.astype(BF)
        dy_in = (dy * from_state).astype(BF)
        xt_f = xt.astype(F32)
        ended = (xt_f * to_end).astype(BF)
        from_later = dot(b_mat, after_b) * to_end
        d_xt = intra + from_later
        d_c = dot(d_scores, b_mat) + dot_t(dy_in, before)
        d_b = t_dot(d_scores, c_mat) + dot_t(ended, after_b)
        across = carry * jnp.sum(before.astype(F32) * after, axis=0, keepdims=True)
        fresh = carry * after + t_dot(c_mat, dy_in)
        pairs = head_sum(dy_b.astype(F32) * (y - skip_all * x) - xt_f * intra, inner, heads, width, 2)
        sums = head_sum(
            jnp.concatenate([xt_f * from_later, x * d_xt, jnp.broadcast_to(across, (8, inner))], axis=0), inner, heads, width
        )
        seg_col, seg_row = m[:, 0:1], segrow[0:1, rows]
        d_log = (
            masked_sum(later_ones(seg_col, seg_row), pairs, 2)
            + masked_sum(earlier_ones(seg_col, seg_row), sums[0:SIZE], 2)
            + sums[2 * SIZE : 2 * SIZE + 1]
        )
        d_raw = (sums[SIZE : 2 * SIZE] - rate * d_log) * sigmoid(raw_step)
        s.rd[rows, :] = d_raw.astype(BF)
        d_x = dy * skip_all + d_xt * dt_all
        s.d_pre_v[rows, :] = d_x * (sig_v * (1.0 + pre_v * (1.0 - sig_v)))
        d_st = jnp.concatenate([d_b, d_c], axis=1)
        s.d_pre_s[rows, :] = d_st * (sig_s * (1.0 + pre_s * (1.0 - sig_s)))
        total = lambda v: jnp.sum(v, axis=0, keepdims=True)
        return fresh, (total(dy * x), total(d_raw), total(d_log * log_decay))

    def body(i, sums):
        after = s.state[...]
        for k in range(group):
            after, more = chunk(z.count - 1 - (i * group + k), after)
            sums = tuple(u + v for u, v in zip(sums, more))
        s.state[...] = after
        return sums

    zero = lambda wide: jnp.zeros((1, wide), F32)
    skip, bias, decay = lax.fori_loop(0, z.count // group, body, (zero(inner), zero(heads), zero(heads)))
    s.narrow[layer, taps + 2 : taps + 3, :] = skip
    s.narrow[layer, taps + 3 : taps + 4, 0:heads] = bias
    s.narrow[layer, taps + 4 : taps + 5, 0:heads] = decay

    def conv_body(c, sums):
        rows = pl.ds(pl.multiple_of(c * SIZE, SIZE), SIZE)
        window = pl.ds(pl.multiple_of(c * SIZE, SIZE), SIZE + 8)
        m = meta[window, :]
        more = []
        for src, w_ref, value_ref, dst in ((s.d_pre_v, a.conv_weight, s.value, s.rv), (s.d_pre_s, a.state_conv_weight, s.raw, s.rs)):
            win = src[window, :]
            value = value_ref[rows, :].astype(F32)
            now = win[0:SIZE, :]
            total = w_ref[layer, 0:1, :] * now
            lines = [jnp.sum(now * value, axis=0, keepdims=True)]
            for k in range(1, taps):
                moved = win[k : k + SIZE, :] * m[k : k + SIZE, k : k + 1]
                total = total + w_ref[layer, k : k + 1, :] * moved
                lines.append(jnp.sum(moved * value, axis=0, keepdims=True))
            lines.append(jnp.sum(now, axis=0, keepdims=True))
            dst[rows, :] = total.astype(BF)
            more.extend(lines)
        return tuple(u + v for u, v in zip(sums, more))

    lines = lax.fori_loop(0, z.count, conv_body, (zero(inner),) * (taps + 1) + (zero(z.both),) * (taps + 1))
    for k in range(taps + 1):
        s.narrow[layer, k : k + 1, :] = lines[k]
        s.wide[layer, k : k + 1, :] = lines[taps + 1 + k]


def norm_backward(total, resid, grad, gain):
    scale = row_scale_of(resid)
    weighted = total * gain
    inner = jnp.sum(weighted * resid, axis=1, keepdims=True)
    gain_grad = jnp.sum(total * resid * scale, axis=0, keepdims=True)
    return grad + scale * weighted - resid * (scale * scale * scale * inner / resid.shape[1]), gain_grad


def exchange(src, got, send, recv, place, number, axis):
    copies = [remote(src, got.at[r], send.at[r], recv.at[r], place ^ r, axis) for r in range(1, number)]
    for copy in copies:
        copy.start()
    return copies


def collected(own, got, copies):
    total = own
    for r, copy in enumerate(copies, 1):
        copy.wait_recv()
        total = total + got[r]
    return total


def backward_kernel(ex, z, names_in, names_out, names_scratch, *refs):
    count_in, count_out = len(names_in), len(names_out)
    a = SimpleNamespace(**dict(zip(names_in, refs)))
    o = SimpleNamespace(**dict(zip(names_out, refs[count_in:])))
    s = SimpleNamespace(**dict(zip(names_scratch, refs[count_in + count_out :])))
    me, row = lax.axis_index(AXIS), lax.axis_index(DATA)
    n, across, taps, heads = ex.size, z.across, z.taps, z.heads
    share = z.depth // across
    cells = z.depth // (n * across)
    padded = padded_cells(z, n)
    greet([me ^ r for r in range(1, n)], [row ^ r for r in range(1, across)])
    saved = list(saved_shapes(z))

    def start_loads(layer, late):
        found = weight_loads(s, a, layer, 0) if late else []
        for i, k in enumerate(saved):
            if late == (i == 0):
                found.append(pltpu.make_async_copy(getattr(a, k).at[layer], getattr(s, k), s.save_sem.at[layer, i]))
        for copy in found:
            copy.start()
        return found

    loads = start_loads(LAYERS - 1, False) + start_loads(LAYERS - 1, True)
    size = z.rows // CHUNKS
    s.row_buf[...] = a.sent[...]
    s.grad[...] = a.cotangent[...]
    gather = Gather(ex, z.rows, s.row_buf, s.sent_all, s.gather_send.at[LAYERS - 1], s.gather_recv.at[LAYERS - 1])
    gather.start(*range(CHUNKS))
    tile = a.mean[...]
    for ref in (s.narrow, s.wide, s.gain):
        ref[...] = jnp.zeros_like(ref)
    s.d_pre_v[z.tokens :, :] = jnp.zeros((8, z.inner), F32)
    s.d_pre_s[z.tokens :, :] = jnp.zeros((8, z.both), F32)
    if padded != cells:
        s.state_part[...] = jnp.zeros_like(s.state_part)
    narrow_copies, outs, older = [None] * LAYERS, [], None

    def finish(piece, k, layer):
        s.done[k] = piece.last()
        target = o.g_out.at[layer] if k == 0 else o.g_inner.at[layer, k - 1]
        copy = pltpu.make_async_copy(s.done.at[k], target, s.done_sem.at[layer, k])
        copy.start()
        return copy

    cell_links, cell_sums = [], {}
    cell_rows = LAYERS * across * padded
    state_steps = reduce_steps_of(
        ex, cell_rows, s.state_part, s.state_pair, s.state_stage, s.state_got,
        (s.cell_pair_send, s.cell_pair_recv, s.cell_link_send, s.cell_link_recv), lambda g, own: None, cell_sums.__setitem__, cell_links,
    )
    for layer in range(LAYERS - 1, -1, -1):
        s.mean_own[layer] = tile
        means = []
        for r in range(1, n):
            means.append(
                remote(s.mean_own.at[layer], s.mean_all.at[layer, me], s.mean_send.at[layer, r], s.mean_recv.at[layer, r], me ^ r)
            )
            means[-1].start()
        s.mean_all[layer, me] = tile
        step_rows(z, a, s, layer, 0)
        if layer + 1 == LAYERS:
            build_meta(z.count, a.segments, s.column, s.meta, s.segrow)

        pieces = [
            Piece(
                across, own, s.piece_stage.at[k], s.piece_got.at[layer, k], s.piece_send.at[layer, k], s.piece_recv.at[layer, k]
            )
            for k, own in enumerate((s.own_out, s.own_inner.at[0], s.own_inner.at[1]))
        ]

        def visit(g, layer=layer, means=means, loads=loads, older=older, pieces=pieces):
            if g == 0:
                for copy in loads:
                    copy.wait()
            if g == sum(ex.links):
                for i in range(across):
                    s.own_out[i] = t_dot(s.scaled[...], s.sent_all[:, i * share : (i + 1) * share]).astype(BF)
                pieces[0].phase(0)
            here = group_rows(ex, g, z.rows)
            first = (me ^ g) // 2 * 2
            for r in (g, g ^ 1):
                if r:
                    means[r - 1].wait_recv()
            mean = jnp.concatenate([column_of(s.mean_all[layer, first]), column_of(s.mean_all[layer, first + 1])], axis=0)
            at = slice(layer, layer + 1)
            grad_scaled = dot_t(s.sent_all[here, :], s.wout[0])
            gate, y = s.gate[here, :], s.y[here, :]
            gate_sig = sigmoid(gate)
            silu_gate = gate * gate_sig
            gated = y * silu_gate
            s.narrow[layer, taps + 1 : taps + 2, :] += jnp.sum(grad_scaled * gated, axis=0, keepdims=True)
            grad_gated = grad_scaled * a.gate_gain[at, :] + (2.0 / z.inner_all) * mean * gated
            s.rg[here, :] = (grad_gated * y * (gate_sig * (1.0 + gate * (1.0 - gate_sig)))).astype(BF)
            s.dy[here, :] = grad_gated * silu_gate
            if g == ex.links[-1] and older is not None:
                older[2].phase(1)
                for k in range(2):
                    for j in range(2, len(older[k].order)):
                        older[k].phase(j)
                outs.append(finish(older[0], 0, layer + 1))

        sent = gather.run(visit)
        if older is not None:
            outs.append(finish(older[1], 1, layer + 1))
        for i in range(across):
            s.own_inner[0, i] = t_dot(s.normed[:, i * share : (i + 1) * share], s.rg[...]).astype(BF)
        pieces[1].phase(0)
        mix_backward(z, layer, s, a, s.meta, s.segrow)
        for copy in sent + means:
            copy.wait_send()
        loads = start_loads(layer - 1, False) if layer else []
        if older is not None:
            for k in range(2, len(older[2].order)):
                older[2].phase(k)
            outs.append(finish(older[2], 2, layer + 1))
        pieces[0].phase(1)
        narrow_copies[layer] = exchange(
            s.narrow.at[layer], s.narrow_got.at[layer], s.narrow_send.at[layer], s.narrow_recv.at[layer], row, across, DATA
        )

        def value_grads(pieces=pieces):
            for i in range(across):
                s.own_inner[1, i] = t_dot(s.normed[:, i * share : (i + 1) * share], s.rv[...]).astype(BF)
            pieces[2].phase(0)

        def state_grads(layer=layer):
            for i in range(across):
                here = slice(i * share, (i + 1) * share)
                state = t_dot(s.normed[:, here], s.rs[...])
                for j in range(n):
                    to = ((j * LAYERS + layer) * across + i) * padded
                    s.state_part[to : to + cells, :] = state[j * cells : (j + 1) * cells, :].astype(BF)
                s.step_part[layer, i, 0:heads, :] = t_dot(s.rd[...], s.normed[:, here])

        if layer == 0:
            value_grads()

        def idle(t, layer=layer, pieces=pieces, value_grads=value_grads, state_grads=state_grads):
            if t == 1:
                if layer:
                    value_grads()
                else:
                    state_grads()
            elif t == 2 and layer:
                state_grads()
            elif t == 3:
                pieces[1].phase(1)
            if t >= 2 and not layer:
                next(state_steps)

        def produce(g, own, layer=layer):
            if own:
                return
            here = group_rows(ex, g, z.rows)
            total = dot_t(s.rg[here, :], s.win[0, 0]) + dot_t(s.rv[here, :], s.win[0, 1])
            total = total + dot_t(s.rs[here, :], s.wst[0]) + dot(s.rd[here, :], s.wstep[0].astype(BF))
            s.part[here, :] = total.astype(BF)

        after = Gather(ex, z.rows, s.row_buf, s.sent_all, s.gather_send.at[layer - 1], s.gather_recv.at[layer - 1]) if layer else None
        found = []

        def final(q, value, layer=layer, after=after, found=found):
            rows = slice(q * size, (q + 1) * size)
            resid = a.resids[layer - 1, rows, :] if layer else a.residual[rows, :]
            fresh, gain_grad = norm_backward(value, resid, s.grad[rows, :], a.norm_gain[layer : layer + 1, :])
            mean = None
            if layer:
                mixed, gate = a.mixeds[layer - 1, rows, :], a.gates[layer - 1, rows, :]
                s.row_buf[rows, :] = (gate * fresh).astype(BF)
                after.start(q)
                s.grad[rows, :] = fresh
                mean = -0.5 * gate * gate * jnp.sum(mixed * fresh, axis=1, keepdims=True)
            else:
                o.input_grad[rows, :] = fresh
            found.append((q, gain_grad, mean))

        links = []
        reduce_rows(
            ex, z.rows, s.part, s.pair, s.stage, s.got,
            (s.pair_send.at[layer], s.pair_recv.at[layer], s.link_send.at[layer], s.link_recv.at[layer]), produce, final, links, idle=idle,
        )
        found.sort(key=lambda item: item[0])
        gain_grad = sum(item[1] for item in found)
        eighth = z.depth // 8
        for k in range(8):
            s.gain[layer, k : k + 1, :] = gain_grad[:, k * eighth : (k + 1) * eighth]
        for copy in links:
            copy.wait_send()
        if layer:
            tile = tile_of(jnp.concatenate([item[2] for item in found], axis=0))
            loads = loads + start_loads(layer - 1, True)
            gather = after
            older = pieces
    gains = exchange(s.gain, s.gain_got, s.gain_send, s.gain_recv, me, n, AXIS)
    wides = exchange(s.wide, s.wide_got, s.wide_send, s.wide_recv, me, n, AXIS)
    for _ in state_steps:
        pass
    state = jnp.concatenate([cell_sums[q] for q in range(CHUNKS)], axis=0)
    s.gain_mid[...] = collected(s.gain[...], s.gain_got, gains)
    s.wide_mid[...] = collected(s.wide[...], s.wide_got, wides)
    gains_two = exchange(s.gain_mid, s.gain_two, s.gain_send_two, s.gain_recv_two, row, across, DATA)
    wides_two = exchange(s.wide_mid, s.wide_two, s.wide_send_two, s.wide_recv_two, row, across, DATA)
    for layer in range(LAYERS):
        for i in range(across):
            at = (layer * across + i) * padded
            s.cell_own[i, layer * padded : (layer + 1) * padded, :] = state[at : at + padded, :].astype(BF)
            s.step_own[i, layer * 16 : layer * 16 + 8, :] = s.step_part[layer, i].astype(BF)
    cell = Piece(across, s.cell_own, s.cell_stage, s.cell_got, s.cell_send, s.cell_recv)
    step = Piece(across, s.step_own, s.step_stage, s.step_got, s.step_send, s.step_recv)
    cell.phase(0)
    step.phase(0)
    for copy in outs:
        copy.wait()
    for j in range(2, len(pieces[0].order)):
        pieces[0].phase(j)
    last = [finish(pieces[0], 0, 0)]
    pieces[2].phase(1)
    for k in range(1, len(cell.order)):
        cell.phase(k)
        step.phase(k)
    for j in range(2, len(pieces[1].order)):
        pieces[1].phase(j)
    last.append(finish(pieces[1], 1, 0))
    for layer in range(LAYERS):
        o.narrow[layer] = collected(s.narrow[layer], s.narrow_got.at[layer], narrow_copies[layer])
    o.gain[...] = collected(s.gain_mid[...], s.gain_two, gains_two)
    o.wide[...] = collected(s.wide_mid[...], s.wide_two, wides_two)
    state, steps = cell.last(), step.last()
    for layer in range(LAYERS):
        o.g_state[layer] = state[layer * padded : layer * padded + cells, :]
        o.g_step[layer] = steps[layer * 16 : layer * 16 + 8, :]
    for j in range(2, len(pieces[2].order)):
        pieces[2].phase(j)
    last.append(finish(pieces[2], 2, 0))
    for copy in cell_links + gains + wides + gains_two + wides_two + [c for copies in narrow_copies for c in copies]:
        copy.wait_send()
    for copy in last:
        copy.wait()


def padded_cells(z, n):
    cells = z.depth // (n * z.across)
    return -(-cells // 16) * 16


def piece_slots(across):
    order = [1 << b for b in range(across.bit_length() - 1)]
    return len(reduce_steps(order)), len(arrival_slots(order))


def backward_pass(ex, z, forward, residual, cotangent, segments, w):
    n, across = ex.size, z.across
    share = z.depth // across
    if share != z.inner:
        raise ValueError(share)
    saved = saved_shapes(z)
    rows = (z.rows, z.depth)
    inputs = dict(
        residual=(residual, True), cotangent=(cotangent, True), sent=(forward.sent, True), mean=(forward.mean, True),
        resids=(forward.resids, True), mixeds=(forward.mixeds, True), gates=(forward.gates, True),
        segments=(segments, True), **small_inputs(w),
    )
    for k in saved:
        inputs[k] = (getattr(forward, k), False)
    cells, padded = z.depth // (n * across), padded_cells(z, n)
    narrow, wide, gain = (LAYERS, 16, z.inner), (LAYERS, 8, z.both), (LAYERS, 8, z.depth // 8)
    outputs = dict(
        input_grad=(rows, F32, True),
        g_inner=((LAYERS, 2, share, z.inner), F32, False), g_out=((LAYERS, z.inner, share), F32, False),
        g_state=((LAYERS, cells, z.both), F32, True), g_step=((LAYERS, 8, share), F32, True),
        narrow=(narrow, F32, True), wide=(wide, F32, True), gain=(gain, F32, True),
    )
    scratch = {k: pltpu.VMEM(shape, kind) for k, (shape, kind) in saved.items()}
    scratch.update(weight_scratch(z, 1))
    scratch.update(meta_scratch(z))
    scratch.update(reduce_scratch(ex, z.rows, z.depth))
    slots = n // 2
    stages, arrivals = piece_slots(across)
    cell_rows = LAYERS * across * padded
    state = {"state_" + k: v for k, v in reduce_scratch(ex, cell_rows, z.both).items()}
    scratch.update(
        state_part=pltpu.VMEM((n * cell_rows, z.both), BF), **state,
        sent_all=pltpu.VMEM((z.tokens, z.depth), BF), part=pltpu.VMEM((z.tokens, z.depth), BF), row_buf=pltpu.VMEM(rows, BF),
        dy=pltpu.VMEM((z.tokens, z.inner), F32), rg=pltpu.VMEM((z.tokens, z.inner), BF), rv=pltpu.VMEM((z.tokens, z.inner), BF),
        rs=pltpu.VMEM((z.tokens, z.both), BF), rd=pltpu.VMEM((z.tokens, z.heads), BF), state=pltpu.VMEM((z.half, z.inner), F32),
        d_pre_v=pltpu.VMEM((z.tokens + 8, z.inner), F32), d_pre_s=pltpu.VMEM((z.tokens + 8, z.both), F32),
        mean_own=pltpu.VMEM((LAYERS, 8, z.rows), F32), mean_all=pltpu.VMEM((LAYERS, n, 8, z.rows), F32),
        mean_send=dma(LAYERS, n), mean_recv=dma(LAYERS, n), save_sem=dma(LAYERS, len(saved)),
        own_out=pltpu.VMEM((across, z.inner, share), BF), own_inner=pltpu.VMEM((2, across, share, z.inner), BF),
        piece_stage=pltpu.VMEM((3, stages, share, z.inner), BF), piece_got=pltpu.VMEM((LAYERS, 3, arrivals, share, z.inner), BF),
        piece_send=dma(LAYERS, 3, stages), piece_recv=dma(LAYERS, 3, arrivals),
        done=pltpu.VMEM((3, share, z.inner), F32), done_sem=dma(LAYERS, 3),
        narrow=pltpu.VMEM(narrow, F32), narrow_got=pltpu.VMEM((LAYERS, across) + narrow[1:], F32),
        narrow_send=dma(LAYERS, across), narrow_recv=dma(LAYERS, across),
        wide=pltpu.VMEM(wide, F32), wide_mid=pltpu.VMEM(wide, F32),
        wide_got=pltpu.VMEM((n,) + wide, F32), wide_two=pltpu.VMEM((across,) + wide, F32),
        gain=pltpu.VMEM(gain, F32), gain_mid=pltpu.VMEM(gain, F32),
        gain_got=pltpu.VMEM((n,) + gain, F32), gain_two=pltpu.VMEM((across,) + gain, F32),
        wide_send=dma(n), wide_recv=dma(n), gain_send=dma(n), gain_recv=dma(n),
        wide_send_two=dma(across), wide_recv_two=dma(across), gain_send_two=dma(across), gain_recv_two=dma(across),
        step_part=pltpu.VMEM((LAYERS, across, 8, share), F32), step_own=pltpu.VMEM((across, LAYERS * 16, share), BF),
        step_stage=pltpu.VMEM((stages, LAYERS * 16, share), BF), step_got=pltpu.VMEM((arrivals, LAYERS * 16, share), BF),
        step_send=dma(stages), step_recv=dma(arrivals),
        cell_own=pltpu.VMEM((across, LAYERS * padded, z.both), BF),
        cell_stage=pltpu.VMEM((stages, LAYERS * padded, z.both), BF), cell_got=pltpu.VMEM((arrivals, LAYERS * padded, z.both), BF),
        cell_send=dma(stages), cell_recv=dma(arrivals),
        cell_pair_send=dma(slots), cell_pair_recv=dma(slots), cell_link_send=dma(CHUNKS * slots),
        cell_link_recv=dma(CHUNKS * (slots - 1)), grad=pltpu.VMEM(rows, F32),
        gather_send=dma(LAYERS, CHUNKS, n), gather_recv=dma(LAYERS, CHUNKS, n),
        pair_send=dma(LAYERS, slots), pair_recv=dma(LAYERS, slots),
        link_send=dma(LAYERS, CHUNKS * slots), link_recv=dma(LAYERS, CHUNKS * (slots - 1)),
    )
    return run_kernel(backward_kernel, ex, z, inputs, outputs, scratch, 1, "backward")


def final_kernel(z, n, *refs):
    block, grad, inner, out, state, step, narrow, wide, gain = refs[:9]
    (o_block, o_grad, o_norm, o_inner, o_state, o_step, o_bias, o_decay, o_skip, o_conv, o_cbias, o_sconv, o_sbias, o_gate, o_out) = refs[9:]
    o_block[...] = block[...]
    o_grad[...] = grad[...]
    o_inner[...] = inner[...]
    o_out[...] = out[...]

    @pl.when(pl.program_id(0) == 0)
    def _():
        taps, heads = z.taps, z.heads
        o_state[...] = state[...]
        cells, eighth = o_norm.shape[1], gain.shape[2]
        per = eighth // cells
        device = lax.axis_index(DATA) * n + lax.axis_index(AXIS)
        pick = lax.broadcasted_iota(jnp.int32, (eighth, cells), 0)
        pick = (pick == lax.broadcasted_iota(jnp.int32, (eighth, cells), 1) + (device % per) * cells).astype(F32)
        line = lax.broadcasted_iota(jnp.int32, (8, eighth), 0) == device // per
        ones = head_sum_matrix(z.inner, heads, z.width).astype(F32)
        for layer in range(LAYERS):
            at = slice(layer, layer + 1)
            row = jnp.sum(jnp.where(line, gain[layer], 0.0), axis=0, keepdims=True)
            o_norm[at, :] = exact(jnp.broadcast_to(row, (8, eighth)), pick)[0:1, :]
            lines = narrow[layer]
            for h in range(heads):
                o_step[h, at, :] = step[layer, h : h + 1, :]
            skip = jnp.broadcast_to(lines[taps + 2 : taps + 3, :], (8, z.inner))
            o_skip[at, :] = exact(skip, ones)[0:1, :]
            o_bias[at, :] = lines[taps + 3 : taps + 4, 0:heads]
            o_decay[at, :] = lines[taps + 4 : taps + 5, 0:heads]
            o_conv[layer] = lines[0:taps, :]
            o_cbias[at, :] = lines[taps : taps + 1, :]
            o_gate[at, :] = lines[taps + 1 : taps + 2, :]
            o_sconv[layer] = wide[layer, 0:taps, :]
            o_sbias[at, :] = wide[layer, taps : taps + 1, :]


def final_pass(ex, z, block_output, b):
    share, both, heads, taps, inner = z.depth // z.across, z.both, z.heads, z.taps, z.inner
    cells = z.depth // (ex.size * z.across)
    steps = 2 if z.rows % 16 == 0 and share % 16 == 0 and inner % 16 == 0 else 1
    whole = lambda shape: pl.BlockSpec(shape, lambda i: (0,) * len(shape))
    rows = pl.BlockSpec((z.rows // steps, z.depth), lambda i: (i, 0))
    inner_spec = pl.BlockSpec((LAYERS, 2, share // steps, inner), lambda i: (0, 0, i, 0))
    out_spec = pl.BlockSpec((LAYERS, inner // steps, share), lambda i: (0, i, 0))
    arrays = (block_output, b.input_grad, b.g_inner, b.g_out, b.g_state, b.g_step, b.narrow, b.wide, b.gain)
    small = [
        (LAYERS, cells, both), (heads, LAYERS, share), (LAYERS, heads), (LAYERS, heads), (LAYERS, heads), (LAYERS, taps, inner),
        (LAYERS, inner), (LAYERS, taps, both), (LAYERS, both), (LAYERS, inner),
    ]
    shapes = [(z.rows, z.depth), (z.rows, z.depth), (LAYERS, cells), b.g_inner.shape] + small + [b.g_out.shape]
    return pl.pallas_call(
        functools.partial(final_kernel, z, ex.size),
        grid=(steps,),
        out_shape=tuple(jax.ShapeDtypeStruct(shape, F32) for shape in shapes),
        in_specs=[rows, rows, inner_spec, out_spec] + [whole(v.shape) for v in arrays[4:]],
        out_specs=tuple([rows, rows, whole((LAYERS, cells)), inner_spec] + [whole(shape) for shape in small] + [out_spec]),
        compiler_params=pltpu.CompilerParams(vmem_limit_bytes=VM),
        cost_estimate=cost_of(1 << 20),
        name="final",
    )(*arrays)


def sizes_of(ex, across, residual, segments, w):
    inner = w.inner_weight.shape[3]
    return Sizes(
        segments.shape[1], residual.shape[0], residual.shape[1], inner, w.step_weight.shape[2], w.state_weight.shape[2],
        w.conv_weight.shape[1], inner * ex.size, across,
    )


def shards(ex, across, residual, cotangent, segments, *weights):
    w = Weights(*weights)
    z = sizes_of(ex, across, residual, segments, w)
    w = w._replace(step_weight=jnp.transpose(w.step_weight, (2, 0, 1)))
    f = forward_pass(ex, z, residual, cotangent, segments, w)
    b = backward_pass(ex, z, f, residual, cotangent, segments, w)
    made = list(final_pass(ex, z, f.block_output, b))
    made[5] = jnp.transpose(made[5], (1, 2, 0))
    return tuple(made)


def solution(mesh):
    ex = Cube(mesh.shape[AXIS])
    both, rest = (DATA, AXIS), None
    return jax.shard_map(
        functools.partial(shards, ex, mesh.shape[DATA]),
        mesh=mesh,
        in_specs=(
            P(both, rest),
            P(both, rest),
            P(DATA, rest),
            P(),
            P(rest, rest, rest, AXIS),
            P(),
            P(rest, rest, AXIS),
            P(rest, AXIS),
            P(rest, AXIS),
            P(rest, AXIS),
            P(rest, rest, AXIS),
            P(rest, AXIS),
            P(),
            P(),
            P(rest, AXIS),
            P(rest, AXIS, rest),
        ),
        out_specs=(
            P(both, rest),
            P(both, rest),
            P(rest, both),
            P(rest, rest, DATA, AXIS),
            P(rest, both, rest),
            P(rest, DATA, AXIS),
            P(rest, AXIS),
            P(rest, AXIS),
            P(rest, AXIS),
            P(rest, rest, AXIS),
            P(rest, AXIS),
            P(),
            P(),
            P(rest, AXIS),
            P(rest, AXIS, DATA),
        ),
        check_vma=False,
    )
```
